32 devices in a mesh: dp: 4 (over y, x), row: 4 (over z), col: 2 (over core).
Axes of the slice: x: 2, y: 2, z: 4, core: 2. Of those that a mesh axis runs over, the one named last changes fastest.
Arguments:
- block_input: bfloat16 [192, 197, 384], P(('dp', 'row', 'col')), may hold values from -6 to 6
- first_norm_scale: float32 [384], P('row'), may hold values from 0.5 to 1.5
- first_norm_bias: float32 [384], P('row'), may hold values from -1.5 to 1.5
- attn_weight: bfloat16 [6, 384, 256], P('col', 'row'), may hold values from -1.2247449 to 1.2247449
- qv_bias: float32 [2, 384], P(None, 'col'), may hold values from -2.5 to 2.5
- out_bias: float32 [384], P('row'), may hold values from -2.5 to 2.5
- second_norm_scale: float32 [384], P('row'), may hold values from 0.5 to 1.5
- second_norm_bias: float32 [384], P('row'), may hold values from -1.5 to 1.5
- up_weight: bfloat16 [384, 1536], P('row', 'col'), may hold values from -0.3125 to 0.3125
- up_bias: float32 [1536], P('col'), may hold values from -2.5 to 2.5
- down_weight: bfloat16 [384, 1536], P('row', 'col'), may hold values from -0.15625 to 0.15625
- down_bias: float32 [384], P('row'), may hold values from -2.5 to 2.5
- cotangent: bfloat16 [192, 197, 384], P(('dp', 'row', 'col')), may hold values from -6 to 6
Outputs:
- block_output: bfloat16 [192, 197, 384], P(('dp', 'row', 'col'))
- d_x: float32 [192, 197, 384], P(('dp', 'row', 'col'))
- d_ln1_gain: float32 [384], P('row')
- d_ln1_shift: float32 [384], P('row')
- d_attn_weight: float32 [6, 384, 256], P('col', 'row')
- d_qv_bias: float32 [2, 384], P(None, 'col')
- d_out_bias: float32 [384], P('row')
- d_ln2_gain: float32 [384], P('row')
- d_ln2_shift: float32 [384], P('row')
- d_up_weight: float32 [384, 1536], P('row', 'col')
- d_up_bias: float32 [1536], P('col')
- d_down_weight: float32 [384, 1536], P('row', 'col')
- d_down_bias: float32 [384], P('row')
The draws below stay inside these ranges and needn't reach their ends.
All inputs are finite; a program needn't handle non-finite values.
Results may differ from the reference program's by a relative error of at most 0.013.
Values may be sent and summed in bfloat16 or wider, within the bound.
A program may use at most 448 MiB of HBM per device.

```python
import math
import jax
import jax.numpy as jnp
from jax import lax

D = 384
HEADS = 6
FF = 1536
SEQ = 197
HD = 64
IMAGES = 192


def draw_attn_weight(key, part):
    raw = jnp.clip(jax.random.normal(key, (HEADS, D, 4 * HD), jnp.float32), -6.0, 6.0)
    column = jnp.arange(4 * HD)
    factor = jnp.where(column >= 3 * HD, 4.0, 1.0) / math.sqrt(D)
    return (raw * factor).astype(jnp.bfloat16)


def steps_of(own_key, extent, shards, low, high):
    factor_of = 1.0
    for dim, blocks in shards:
        steps = jax.random.uniform(jax.random.fold_in(jax.random.fold_in(own_key, 6), dim), (blocks,), jnp.float32, low / len(shards), high / len(shards))
        factor_of = factor_of * jnp.repeat(jnp.exp(steps), extent[dim] // blocks).reshape((-1,) + (1,) * (len(extent) - 1 - dim))
    return factor_of


def normal_values(own_key, dims, scale, most, pieces=(), kind=jnp.bfloat16):
    loudness = steps_of(own_key, dims, pieces, -0.22, 0.18) if pieces else 1.0
    drawn = jax.random.normal(own_key, dims, jnp.float32) * scale * loudness
    return jnp.minimum(jnp.maximum(drawn, -most), most).astype(kind)


def setup_inputs(seed: int = 0) -> dict:
    key_of = jax.random.split(jax.random.key(seed), 14)
    block_input = normal_values(key_of[0], (IMAGES, SEQ, D), 1.0, 6.0, ((0, 32),))
    first_norm_scale = jnp.clip(1.0 + 0.1 * jax.random.normal(key_of[1], (D,), jnp.float32), 0.5, 1.5)
    first_norm_bias = normal_values(key_of[2], (D,), 0.3, 1.5, ((0, 4),), jnp.float32)
    attn_weight = draw_attn_weight(jax.random.fold_in(key_of[13], 71), 0)
    qv_bias = normal_values(key_of[4], (2, D), 0.5, 2.5, ((1, 2),), jnp.float32)
    out_bias = normal_values(key_of[5], (D,), 0.5, 2.5, ((0, 4),), jnp.float32)
    second_norm_scale = jnp.clip(1.0 + 0.1 * jax.random.normal(key_of[6], (D,), jnp.float32), 0.5, 1.5)
    second_norm_bias = normal_values(key_of[7], (D,), 0.3, 1.5, ((0, 4),), jnp.float32)
    up_weight = normal_values(key_of[8], (D, FF), D ** -0.5, 0.3125, ((0, 4), (1, 2)))
    up_bias = normal_values(key_of[9], (FF,), 0.5, 2.5, ((0, 2),), jnp.float32)
    down_weight = normal_values(key_of[10], (D, FF), FF ** -0.5, 0.15625, ((0, 4), (1, 2)))
    down_bias = normal_values(key_of[11], (D,), 0.5, 2.5, ((0, 4),), jnp.float32)
    cotangent = normal_values(key_of[12], (IMAGES, SEQ, D), 1.0, 6.0, ((0, 32),))
    return dict(block_input=block_input, first_norm_scale=first_norm_scale, first_norm_bias=first_norm_bias, attn_weight=attn_weight, qv_bias=qv_bias, out_bias=out_bias, second_norm_scale=second_norm_scale, second_norm_bias=second_norm_bias, up_weight=up_weight, up_bias=up_bias, down_weight=down_weight, down_bias=down_bias, cotangent=cotangent)


EPS = 1e-06
ROOT_HALF = 0.7071067811865476
INV_ROOT_TWO_PI = 0.3989422804014327

def gelu_parts(u):
    cdf = 0.5 * (1.0 + jax.scipy.special.erf(u * ROOT_HALF))
    return (u * cdf, cdf + u * jnp.exp(-0.5 * u * u) * INV_ROOT_TWO_PI)

def layer_norm_forward(input_value, scale_factor, offset_bias):
    row_average = lax.optimization_barrier(jnp.mean(input_value, -1, keepdims=True))
    centered_input = input_value - row_average
    var = lax.optimization_barrier(jnp.mean(centered_input * centered_input, -1, keepdims=True))
    inverse_deviation = lax.rsqrt(var + EPS)
    normalized_input = centered_input * inverse_deviation
    return (normalized_input, inverse_deviation, (normalized_input * scale_factor + offset_bias).astype(jnp.bfloat16))

def layer_norm_backward(incoming_gradient, normalized_input, inverse_deviation, scale_factor):
    normalized_gradient = incoming_gradient * scale_factor
    return inverse_deviation * (normalized_gradient - lax.optimization_barrier(jnp.mean(normalized_gradient, -1, keepdims=True)) - normalized_input * lax.optimization_barrier(jnp.mean(normalized_gradient * normalized_input, -1, keepdims=True)))

def matmul(left, weight):
    flat = left.reshape(-1, left.shape[-1])
    out = jnp.dot(flat, weight, preferred_element_type=jnp.float32)
    return out.reshape(left.shape[:-1] + (weight.shape[-1],))

def weight_grad(left, incoming_gradient):
    flat_left = left.reshape(-1, left.shape[-1])
    flat_grad = incoming_gradient.reshape(-1, incoming_gradient.shape[-1])
    return jnp.dot(flat_left.T, flat_grad, preferred_element_type=jnp.float32)

def scores_of(query, keys, scale):
    return jnp.einsum('bqhd,bkhd->bhqk', query.astype(jnp.float32), keys.astype(jnp.float32)) * scale

def attend(query, keys, values, scale):
    scores = scores_of(query, keys, scale)
    top = lax.optimization_barrier(jnp.max(scores, -1, keepdims=True))
    lse = top + jnp.log(lax.optimization_barrier(jnp.sum(jnp.exp(scores - top), -1, keepdims=True)))
    probs = jnp.exp(scores - lse).astype(jnp.bfloat16)
    out = jnp.einsum('bhqk,bkhd->bqhd', probs.astype(jnp.float32), values.astype(jnp.float32))
    return (out.astype(jnp.bfloat16), lse)

def attend_back(query, keys, values, lse, dout, scale):
    scores = scores_of(query, keys, scale)
    probs = jnp.exp(scores - lse)
    probs_b = probs.astype(jnp.bfloat16)
    dvals = jnp.einsum('bhqk,bqhd->bkhd', probs_b.astype(jnp.float32), dout.astype(jnp.float32))
    dprob = jnp.einsum('bqhd,bkhd->bhqk', dout.astype(jnp.float32), values.astype(jnp.float32))
    delta = lax.optimization_barrier(jnp.sum(probs * dprob, -1, keepdims=True))
    dsb = (probs * (dprob - delta)).astype(jnp.bfloat16).astype(jnp.float32)
    dquery = jnp.einsum('bhqk,bkhd->bqhd', dsb, keys.astype(jnp.float32)) * scale
    dkeys = jnp.einsum('bhqk,bqhd->bkhd', dsb, query.astype(jnp.float32)) * scale
    return (dquery.astype(jnp.bfloat16), dkeys.astype(jnp.bfloat16), dvals.astype(jnp.bfloat16))

def reference(block_input, first_norm_scale, first_norm_bias, attn_weight, qv_bias, out_bias, second_norm_scale, second_norm_bias, up_weight, up_bias, down_weight, down_bias, cotangent):
    images = block_input.shape[0]
    block = math.gcd(images, 16)
    nblocks = images // block
    scale = 1.0 / math.sqrt(HD)
    qkv_flat = attn_weight[:, :, :3 * HD].reshape(HEADS, D, 3, HD).transpose(1, 2, 0, 3).reshape(D, 3 * D)
    out_weight = attn_weight[:, :, 3 * HD:].transpose(0, 2, 1).reshape(D, D)
    down_t = down_weight.T
    bias_three = jnp.stack([qv_bias[0], jnp.zeros_like(qv_bias[0]), qv_bias[1]])

    def one_block(carry, inputs):
        x_b, gradient_block = inputs
        count = x_b.shape[0]
        input_as_float = x_b.astype(jnp.float32)
        first_normalized_input, first_inverse_deviation, first_activation = layer_norm_forward(input_as_float, first_norm_scale, first_norm_bias)
        qkv = matmul(first_activation, qkv_flat).reshape(count, SEQ, 3, D) + bias_three
        query = qkv[:, :, 0].astype(jnp.bfloat16).reshape(count, SEQ, HEADS, HD)
        keys = qkv[:, :, 1].astype(jnp.bfloat16).reshape(count, SEQ, HEADS, HD)
        values = qkv[:, :, 2].astype(jnp.bfloat16).reshape(count, SEQ, HEADS, HD)
        attn, lse = attend(query, keys, values, scale)
        attn_flat = attn.reshape(count, SEQ, D)
        hidden_input = input_as_float + matmul(attn_flat, out_weight) + out_bias
        second_normalized_input, second_inverse_deviation, second_activation = layer_norm_forward(hidden_input, second_norm_scale, second_norm_bias)
        pre = matmul(second_activation, up_weight) + up_bias
        act, slope = gelu_parts(pre)
        act_b = act.astype(jnp.bfloat16)
        out_b = (hidden_input + matmul(act_b, down_t) + down_bias).astype(jnp.bfloat16)
        g_down_w = weight_grad(gradient_block, act_b)
        g_down_b = lax.optimization_barrier(jnp.sum(gradient_block.astype(jnp.float32), (0, 1)))
        dpre = (matmul(gradient_block, down_weight) * slope).astype(jnp.bfloat16)
        g_up_w = weight_grad(second_activation, dpre)
        g_up_b = lax.optimization_barrier(jnp.sum(dpre.astype(jnp.float32), (0, 1)))
        second_activation_grad = matmul(dpre, up_weight.T)
        second_norm_scale_grad = lax.optimization_barrier(jnp.sum(second_activation_grad * second_normalized_input, (0, 1)))
        g_ln2_s = lax.optimization_barrier(jnp.sum(second_activation_grad, (0, 1)))
        hidden_gradient = gradient_block.astype(jnp.float32) + layer_norm_backward(second_activation_grad, second_normalized_input, second_inverse_deviation, second_norm_scale)
        dhb = hidden_gradient.astype(jnp.bfloat16)
        g_out_w = weight_grad(attn_flat, dhb)
        g_out_b = lax.optimization_barrier(jnp.sum(dhb.astype(jnp.float32), (0, 1)))
        dout = matmul(dhb, out_weight.T).astype(jnp.bfloat16).reshape(count, SEQ, HEADS, HD)
        dquery, dkeys, dvals = attend_back(query, keys, values, lse, dout, scale)
        dqkv = jnp.stack([dquery, dkeys, dvals], 2).reshape(count, SEQ, 3 * D)
        g_qkv_w = weight_grad(first_activation, dqkv)
        bias_sums = lax.optimization_barrier(jnp.sum(dqkv.astype(jnp.float32), (0, 1))).reshape(3, D)
        g_qv_b = jnp.stack([bias_sums[0], bias_sums[2]])
        first_activation_grad = matmul(dqkv, qkv_flat.T)
        first_norm_scale_grad = lax.optimization_barrier(jnp.sum(first_activation_grad * first_normalized_input, (0, 1)))
        g_ln1_s = lax.optimization_barrier(jnp.sum(first_activation_grad, (0, 1)))
        input_gradient_block = hidden_gradient + layer_norm_backward(first_activation_grad, first_normalized_input, first_inverse_deviation, first_norm_scale)
        terms = (first_norm_scale_grad, g_ln1_s, g_qkv_w, g_qv_b, g_out_w, g_out_b, second_norm_scale_grad, g_ln2_s, g_up_w, g_up_b, g_down_w, g_down_b)
        carry = tuple((total + term for total, term in zip(carry, terms)))
        return (carry, (out_b, input_gradient_block))
    init = (jnp.zeros((D,), jnp.float32), jnp.zeros((D,), jnp.float32), jnp.zeros((D, 3 * D), jnp.float32), jnp.zeros((2, D), jnp.float32), jnp.zeros((D, D), jnp.float32), jnp.zeros((D,), jnp.float32), jnp.zeros((D,), jnp.float32), jnp.zeros((D,), jnp.float32), jnp.zeros((D, FF), jnp.float32), jnp.zeros((FF,), jnp.float32), jnp.zeros((D, FF), jnp.float32), jnp.zeros((D,), jnp.float32))
    blocks_x = block_input.reshape(nblocks, block, SEQ, D)
    blocks_g = cotangent.reshape(nblocks, block, SEQ, D)
    grads, (outs, dxs) = lax.scan(one_block, init, (blocks_x, blocks_g))
    y_out = outs.reshape(images, SEQ, D)
    output_input_gradient = dxs.reshape(images, SEQ, D)
    packed_qkv = grads[2].reshape(D, 3, HEADS, HD).transpose(2, 0, 1, 3).reshape(HEADS, D, 3 * HD)
    packed_out = grads[4].reshape(HEADS, HD, D).transpose(0, 2, 1)
    d_attn = jnp.concatenate([packed_qkv, packed_out], 2)
    return (y_out, output_input_gradient, grads[0], grads[1], d_attn, grads[3], grads[5], grads[6], grads[7], grads[8], grads[9], grads[10], grads[11])
```

```python
import functools
import math

import jax
import jax.numpy as jnp
from jax import lax
from jax.experimental import pallas as pl
from jax.experimental.pallas import tpu as pltpu
from jax.sharding import PartitionSpec as P

EPS = 1e-06
ROOT_HALF = 0.7071067811865476
INV_ROOT_TWO_PI = 0.3989422804014327
LOG2E = 1.4426950408889634
F32, BF16 = jnp.float32, jnp.bfloat16


def mm(a, b, ca, cb):
    return lax.dot_general(a, b, (((ca,), (cb,)), ((), ())), preferred_element_type=F32)


def norm_parts(v):
    mean = jnp.mean(v, -1, keepdims=True)
    cen = v - mean
    rstd = lax.rsqrt(jnp.mean(cen * cen, -1, keepdims=True) + EPS)
    return cen * rstd, rstd


def norm_back(g, gain, xhat, rstd):
    gx = g * gain
    return rstd * (gx - jnp.mean(gx, -1, keepdims=True) - xhat * jnp.mean(gx * xhat, -1, keepdims=True))


def gelu_parts(u):
    cdf = 0.5 * (1.0 + lax.erf(u * ROOT_HALF))
    return u * cdf, cdf + u * jnp.exp(-0.5 * u * u) * INV_ROOT_TWO_PI


def kernel(cfg, x_hbm, c_hbm, wa, wup, wdn, g1, b1, qvb, ob, g2, b2, ub, db,
           y_out, dx_out, dg1, db1, dwa, dqvb, dob, dg2, db2, dup, dub, ddn, ddb,
           xin, cin, cb, xh1, a1, qkv, pt, o, h, xh2, rs1, rs2, a2, wot, bias3, gb, du, yacc, dacc,
           dhb, dout, dqkv, a1t, a2t, ct, dht, sems):
    NI, SEQ, SP, D, H, HD, FF, FC = cfg
    T = NI * SP
    E = HD
    cx = pltpu.make_async_copy(x_hbm, xin, sems.at[0])
    cc = pltpu.make_async_copy(c_hbm, cin, sems.at[1])
    cx.start()
    cc.start()
    xh1[:, SP - 16:, :] = jnp.zeros((NI, 16, D), F32)
    h[:, SP - 16:, :] = jnp.zeros((NI, 16, D), F32)
    yacc[:, SP - 16:, :] = jnp.zeros((NI, 16, D), F32)
    rs1[:, SP - 16:, :] = jnp.zeros((NI, 16, 1), F32)
    wot[...] = jnp.concatenate([wa[hh][:, 3 * E:] for hh in range(H)], axis=1)
    for hh in range(H):
        bias3[hh] = jnp.concatenate(
            [qvb[0:1, hh * E:(hh + 1) * E], jnp.zeros((1, E), F32),
             qvb[1:2, hh * E:(hh + 1) * E], jnp.zeros((1, E), F32)], axis=1)
    cx.wait()
    cc.wait()

    key_ok = lax.broadcasted_iota(jnp.int32, (SP, SP), 0) < SEQ

    def fwd(i, carry):
        xf = xin[i].astype(F32)
        xh, rstd = norm_parts(xf)
        xh1[i, :SEQ] = xh
        rs1[i, :SEQ] = rstd
        h[i, :SEQ] = xf
        yacc[i, :SEQ] = cin[i].astype(F32)
        cb[i] = yacc[i].astype(BF16)
        a = (xh1[i] * g1[...] + b1[...]).astype(BF16)
        a1[i] = a
        outs = []
        for hh in range(H):
            t = (mm(a, wa[hh], 1, 0) + bias3[hh]).astype(BF16)
            qkv[i, hh] = t
            q, k, v = t[:, :E], t[:, E:2 * E], t[:, 2 * E:3 * E]
            s = mm(k, q, 1, 1) * (LOG2E / math.sqrt(E))
            s = jnp.where(key_ok, s, -1e30)
            top = jnp.max(s, 0, keepdims=True)
            e = jnp.exp2(s - top)
            p = (e * (1.0 / jnp.sum(e, 0, keepdims=True))).astype(BF16)
            pt[i, hh] = p
            outs.append(mm(p, v, 0, 0).astype(BF16))
        oo = jnp.concatenate(outs, axis=1)
        o[i] = oo
        hh_ = h[i] + mm(oo, wot[...], 1, 1) + ob[...]
        h[i] = hh_
        xh, rstd = norm_parts(hh_)
        xh2[i] = xh
        rs2[i] = rstd
        a2[i] = (xh * g2[...] + b2[...]).astype(BF16)
        yacc[i] = hh_ + db[...]
        dacc[i] = jnp.zeros((SP, D), F32)
        return carry

    lax.fori_loop(0, NI, fwd, 0)
    a2t[...] = a2[...].reshape(T, D).T
    ct[...] = cb[...].reshape(T, D).T
    a1t[...] = a1[...].reshape(T, D).T

    NH = FF // wup.shape[2]
    FH = wup.shape[2]
    per = FH // FC

    def ff(f, carry):
        half, s = f // per, lax.rem(f, per)
        cols = pl.ds(pl.multiple_of(s * FC, FC), FC)
        w1, w2 = wup[half, :, cols], wdn[half, :, cols]
        bias = ub[pl.ds(half, 1), cols]

        def one(i, tot):
            u = mm(a2[i], w1, 1, 0) + bias
            act, slope = gelu_parts(u)
            gbi = act.astype(BF16)
            d = mm(cb[i], w2, 1, 0) * slope
            dui = d.astype(BF16)
            gb[i] = gbi
            du[i] = dui
            yacc[i] += mm(gbi, w2, 1, 1)
            dacc[i] += mm(dui, w1, 1, 1)
            return tot + jnp.sum(d, 0, keepdims=True)

        tot = lax.fori_loop(0, NI, one, jnp.zeros((1, FC), F32))
        dub[pl.ds(half, 1), cols] = tot
        ddn[half, :, cols] = mm(ct[...], gb[...].reshape(T, FC), 1, 0)
        dup[half, :, cols] = mm(a2t[...], du[...].reshape(T, FC), 1, 0)
        return carry

    lax.fori_loop(0, NH * per, ff, 0)

    def mid(i, carry):
        s_db, s_g, s_b, s_ob = carry
        y_out[i] = yacc[i][:SEQ].astype(BF16)
        c = cb[i].astype(F32)
        da = dacc[i]
        xh = xh2[i]
        dh = c + norm_back(da, g2[...], xh, rs2[i])
        h[i] = dh
        db_ = dh.astype(BF16)
        dhb[i] = db_
        dd = mm(db_, wot[...], 1, 0).astype(BF16)
        for hh in range(H):
            dout[i, hh] = dd[:, hh * E:(hh + 1) * E]
        dacc[i] = jnp.zeros((SP, D), F32)
        add = lambda t, v: t + jnp.sum(v, 0, keepdims=True)
        return add(s_db, c), add(s_g, da * xh), add(s_b, da), add(s_ob, dh)

    z = jnp.zeros((1, D), F32)
    s_db, s_g, s_b, s_ob = lax.fori_loop(0, NI, mid, (z, z, z, z))
    ddb[...] = s_db
    dg2[...] = s_g
    db2[...] = s_b
    dob[...] = s_ob
    dht[...] = dhb[...].reshape(T, D).T
    dwo = mm(dht[...], o[...].reshape(T, D), 1, 0)

    scale = 1.0 / math.sqrt(E)

    def back(hh, carry):
        def one(i, tot):
            t = qkv[i, hh]
            q, k, v = t[:, :E], t[:, E:2 * E], t[:, 2 * E:3 * E]
            p = pt[i, hh]
            do = dout[i, hh]
            pf = p.astype(F32)
            dp = mm(v, do, 1, 1)
            delta = jnp.sum(pf * dp, 0, keepdims=True)
            ds = (pf * (dp - delta)).astype(BF16)
            dk = mm(ds, q, 1, 0) * scale
            dv = mm(p, do, 1, 0)
            dq = mm(ds, k, 0, 0) * scale
            dd = jnp.concatenate([dq, dk, dv, jnp.zeros((SP, E), F32)], axis=1)
            db_ = dd.astype(BF16)
            dqkv[i] = db_
            dacc[i] += mm(db_, wa[hh], 1, 1)
            return tot + jnp.sum(dd, 0, keepdims=True)

        tot = lax.fori_loop(0, NI, one, jnp.zeros((1, 4 * E), F32))
        dqvb[hh] = tot
        dwa[hh] = mm(a1t[...], dqkv[...].reshape(T, 4 * E), 1, 0)
        return carry

    lax.fori_loop(0, H, back, 0)
    for hh in range(H):
        dwa[hh, :, 3 * E:] = dwo[:, hh * E:(hh + 1) * E]

    def last(i, carry):
        s_g, s_b = carry
        da = dacc[i]
        xh = xh1[i]
        dx = h[i] + norm_back(da, g1[...], xh, rs1[i])
        dx_out[i] = dx[:SEQ]
        add = lambda t, v: t + jnp.sum(v, 0, keepdims=True)
        return add(s_g, da * xh), add(s_b, da)

    s_g, s_b = lax.fori_loop(0, NI, last, (z, z))
    dg1[...] = s_g
    db1[...] = s_b


def compute(x, c, wa, wup, wdn, g1, b1, qvb, ob, g2, b2, ub, db, fc=768):
    NI, SEQ, D = x.shape
    H, _, W4 = wa.shape
    HD = W4 // 4
    C, _, FH = wup.shape
    FF = C * FH
    SP = -(-SEQ // 16) * 16
    T = NI * SP
    cfg = (NI, SEQ, SP, D, H, HD, FF, fc)
    V = pl.BlockSpec(memory_space=pltpu.VMEM)
    A = pl.BlockSpec(memory_space=pl.ANY)
    sd = jax.ShapeDtypeStruct
    vm = pltpu.VMEM
    return pl.pallas_call(
        functools.partial(kernel, cfg),
        out_shape=(sd((NI, SEQ, D), BF16), sd((NI, SEQ, D), F32), sd((1, D), F32), sd((1, D), F32),
                   sd((H, D, W4), F32), sd((H, 1, W4), F32), sd((1, D), F32), sd((1, D), F32), sd((1, D), F32),
                   sd((C, D, FH), F32), sd((C, FH), F32), sd((C, D, FH), F32), sd((1, D), F32)),
        in_specs=[A, A] + [V] * 11,
        out_specs=[V] * 13,
        scratch_shapes=[
            vm((NI, SEQ, D), BF16), vm((NI, SEQ, D), BF16), vm((NI, SP, D), BF16), vm((NI, SP, D), F32),
            vm((NI, SP, D), BF16), vm((NI, H, SP, 4 * HD), BF16), vm((NI, H, SP, SP), BF16), vm((NI, SP, D), BF16),
            vm((NI, SP, D), F32), vm((NI, SP, D), F32), vm((NI, SP, 1), F32), vm((NI, SP, 1), F32),
            vm((NI, SP, D), BF16), vm((D, D), BF16), vm((H, 1, 4 * HD), F32), vm((NI, SP, fc), BF16), vm((NI, SP, fc), BF16),
            vm((NI, SP, D), F32), vm((NI, SP, D), F32), vm((NI, SP, D), BF16), vm((NI, H, SP, HD), BF16),
            vm((NI, SP, 4 * HD), BF16), vm((D, T), BF16), vm((D, T), BF16), vm((D, T), BF16), vm((D, T), BF16),
            pltpu.SemaphoreType.DMA((2,)),
        ],
        compiler_params=pltpu.CompilerParams(vmem_limit_bytes=67043328),
    )(x, c, wa, wup, wdn, g1, b1, qvb, ob, g2, b2, ub, db)


def local(x, g1, b1, aw, qvb, ob, g2, b2, up, ub, dn, db, c):
    gr = lambda v, ax: lax.all_gather(v, "row", axis=ax, tiled=True)
    vec = jnp.stack([g1, b1, ob, g2, b2, db])
    vec = gr(vec, 1)
    g1, b1, ob, g2, b2, db = [vec[i:i + 1] for i in range(6)]
    rows = aw.shape[1]
    wa = lax.all_gather(gr(aw, 1), "col", axis=0, tiled=True)
    wup = lax.all_gather(gr(up, 0), "col", axis=0)
    wdn = lax.all_gather(gr(dn, 0), "col", axis=0)
    qvb_ = lax.all_gather(qvb, "col", axis=1, tiled=True)
    ub_ = lax.all_gather(ub, "col", axis=0)
    y, dx, dg1, db1, dwa, dqvb, dob, dg2, db2, dup, dub, ddn, ddb = compute(
        x, c, wa, wup, wdn, g1, b1, qvb_, ob, g2, b2, ub_, db, fc=up.shape[1])

    def scatter(g, cdim, rdim):
        g = g.astype(BF16)
        g = lax.psum_scatter(g, "row", scatter_dimension=rdim, tiled=True)
        g = lax.psum_scatter(g, "col", scatter_dimension=cdim, tiled=True)
        return lax.psum(g, "dp").astype(F32)

    dwa = scatter(dwa, 0, 1)
    dup = scatter(dup, 0, 1)[0]
    ddn = scatter(ddn, 0, 1)[0]
    hd = aw.shape[2] // 4
    small = lax.psum(jnp.concatenate([dg1[0], db1[0], dob[0], dg2[0], db2[0], ddb[0], dqvb[:, 0, :hd].reshape(-1),
                                      dqvb[:, 0, 2 * hd:3 * hd].reshape(-1), dub.reshape(-1)]), ("dp", "row", "col"))
    d = g1.shape[1]
    r, k = lax.axis_index("row"), lax.axis_index("col")
    rp = [lax.dynamic_slice(small, (i * d + r * rows,), (rows,)) for i in range(6)]
    qc = qvb.shape[1]
    dq = [lax.dynamic_slice(small, ((6 + i) * d + k * qc,), (qc,)) for i in range(2)]
    du = lax.dynamic_slice(small, (8 * d + k * ub.shape[0],), (ub.shape[0],))
    return y, dx, rp[0], rp[1], dwa, jnp.stack(dq), rp[2], rp[3], rp[4], dup, du, ddn, rp[5]


def solution(mesh):
    placed = (
        P(("dp", "row", "col"), None, None),
        P("row"),
        P("row"),
        P("col", "row", None),
        P(None, "col"),
        P("row"),
        P("row"),
        P("row"),
        P("row", "col"),
        P("col"),
        P("row", "col"),
        P("row"),
        P(("dp", "row", "col"), None, None),
    )
    return jax.shard_map(
        local,
        mesh=mesh,
        in_specs=placed,
        out_specs=(
            P(("dp", "row", "col"), None, None),
            P(("dp", "row", "col"), None, None),
            P("row"),
            P("row"),
            P("col", "row", None),
            P(None, "col"),
            P("row"),
            P("row"),
            P("row"),
            P("row", "col"),
            P("col"),
            P("row", "col"),
            P("row"),
        ),
        check_vma=False,
    )
```

```python
import functools
import math

import jax
import jax.numpy as jnp
from jax import lax
from jax.experimental import pallas as pl
from jax.experimental.pallas import tpu as pltpu
from jax.sharding import PartitionSpec as P

EPS = 1e-06
ROOT_HALF = 0.7071067811865476
INV_ROOT_TWO_PI = 0.3989422804014327
LOG2E = 1.4426950408889634
F32, BF16 = jnp.float32, jnp.bfloat16
MESH = pl.DeviceIdType.MESH


def mm(a, b, ca, cb):
    return lax.dot_general(a, b, (((ca,), (cb,)), ((), ())), preferred_element_type=F32)


def norm_parts(v):
    mean = jnp.mean(v, -1, keepdims=True)
    cen = v - mean
    rstd = lax.rsqrt(jnp.mean(cen * cen, -1, keepdims=True) + EPS)
    return cen * rstd, rstd


def norm_back(g, gain, xhat, rstd):
    gx = g * gain
    return rstd * (gx - jnp.mean(gx, -1, keepdims=True) - xhat * jnp.mean(gx * xhat, -1, keepdims=True))


def gelu_parts(u):
    w = u * ROOT_HALF
    cdf = 0.5 + 0.5 * lax.erf(w)
    bell = jnp.exp2((w * w) * -LOG2E)
    return u * cdf, cdf + (w * bell) * (INV_ROOT_TWO_PI / ROOT_HALF)


def rsum(v):
    return jnp.sum(v, 0, keepdims=True)


class Shift:
    def __init__(self, axis, n):
        self.axis, self.n, self.me = axis, n, lax.axis_index(axis)

    def up(self, k):
        return lax.rem(self.me + k, self.n)

    def down(self, k):
        return lax.rem(self.me + self.n - k, self.n)

    def ks(self):
        return range(1, self.n)


def remote(src, dst, ssem, rsem, axis, to):
    return pltpu.make_async_remote_copy(
        src_ref=src, dst_ref=dst, send_sem=ssem, recv_sem=rsem, device_id={axis: to}, device_id_type=MESH)


class Reduce:
    def __init__(self, cfg, ax, bufs, sems):
        self.rows, self.split = cfg
        self.dp, self.row, self.col = ax
        (self.send_c, self.recv_c, self.send_p, self.recv_p, self.send_z, self.recv_z, self.fin) = bufs
        self.sems = sems
        self.np = self.send_p.shape[0]
        self.c, self.p, self.z, self.a = [], [], [], []

    def put_c(self, k, a, v):
        self.send_c[k - 1, a] = v.astype(BF16)

    def start_c(self, k):
        self.c.append(remote(self.send_c.at[k - 1], self.recv_c.at[k - 1], self.sems.at[0, k], self.sems.at[1, k],
                             self.col.axis, self.col.up(k)))
        self.c[-1].start()

    def wait_c(self):
        for cp in self.c:
            cp.wait_recv()

    def put_p(self, a, v):
        sr, sl = self.split
        pr, pl_ = self.send_p.shape[-2:]
        for k in self.col.ks():
            v = v + self.recv_c[k - 1, a].astype(F32)
        for r in range(self.row.n):
            for qr in range(sr):
                for ql in range(sl):
                    lo = r * self.rows + qr * pr
                    piece = v[lo:lo + pr, ql * pl_:(ql + 1) * pl_].astype(BF16)
                    self.send_p[qr * sl + ql, r, a] = piece
                    if self.np == 1:
                        self.recv_p[self.dp.me, r, a] = piece

    def start_p(self):
        for k in self.dp.ks():
            to = self.dp.up(k)
            self.p.append(remote(self.send_p.at[to if self.np > 1 else 0], self.recv_p.at[self.dp.me],
                                 self.sems.at[2, k], self.sems.at[3, k], self.dp.axis, to))
            self.p[-1].start()

    def start_z(self):
        for cp in self.p:
            cp.wait_recv()
        if self.np > 1:
            t = self.send_p[self.dp.me].astype(F32)
            for k in self.dp.ks():
                t = t + self.recv_p[self.dp.up(k)].astype(F32)
        else:
            t = self.recv_p[0].astype(F32)
            for q in range(1, self.dp.n):
                t = t + self.recv_p[q].astype(F32)
        self.send_z[...] = t.astype(BF16)
        for k in self.row.ks():
            to = self.row.up(k)
            self.z.append(remote(self.send_z.at[to], self.recv_z.at[self.row.me], self.sems.at[4, k], self.sems.at[5, k],
                                 self.row.axis, to))
            self.z[-1].start()

    def start_a(self):
        for cp in self.z:
            cp.wait_recv()
        t = self.send_z[self.row.me].astype(F32)
        for k in self.row.ks():
            t = t + self.recv_z[self.row.up(k)].astype(F32)
        me = self.dp.me if self.np > 1 else 0
        self.fin[me] = t.astype(BF16)
        if self.np > 1:
            for k in self.dp.ks():
                self.a.append(remote(self.fin.at[me], self.fin.at[me], self.sems.at[6, k], self.sems.at[7, k],
                                     self.dp.axis, self.dp.up(k)))
                self.a[-1].start()

    def finish(self, put):
        sr, sl = self.split
        pr, pl_ = self.send_p.shape[-2:]
        for cp in self.a:
            cp.wait_recv()
        for a in range(self.fin.shape[1]):
            for qr in range(sr):
                for ql in range(sl):
                    put(a, slice(qr * pr, (qr + 1) * pr), slice(ql * pl_, (ql + 1) * pl_),
                        self.fin[qr * sl + ql, a].astype(F32))
        for cp in self.c + self.p + self.z + self.a:
            cp.wait_send()


def kernel(cfg, *refs):
    (DP, R, C, NI, SEQ, SP, D, Hc, E, FH, rows, split) = cfg
    (x_hbm, g1_h, b1_h, aw_h, qvb_h, ob_h, g2_h, b2_h, up_h, ub_h, dn_h, db_h, c_hbm) = refs[:13]
    (y_o, dx_o, dg1_o, db1_o, daw_o, dqvb_o, dob_o, dg2_o, db2_o, dup_o, dub_o, ddn_o, ddb_o) = refs[13:26]
    (wa, wup, wdn, vall, qvall, uball, vec, bias3, xin, cin, cb, xh1, rs1, a1, qkv, pt, o, h, xh2, rs2, a2, wot, gb, du,
     yacc, dacc, dout, dqkv, a2t, ct, dwo, dxb, dubs, dqvs,
     f1, f2, f3, f4, f5, f6, f7, t1, t2, t3, t4, t5, t6, t7, so_f, so_t,
     sgs, sgc, sgp, sgz, sgr,
     lsem, osem, wz, wp, wc, fsem, tsem, vsem, gsem) = refs[26:]
    H, T, W4 = C * Hc, NI * SP, 4 * E
    dp, row, col = Shift("dp", DP), Shift("row", R), Shift("col", C)
    d, r, c = dp.me, row.me, col.me
    sr, sl = split
    np_ = sr * sl
    part = np_ > 1

    loads = [pltpu.make_async_copy(x_hbm, xin, lsem.at[0]), pltpu.make_async_copy(c_hbm, cin, lsem.at[1])]
    own = pl.ds(pl.multiple_of(r * rows, rows), rows)
    heads = pl.ds(c * Hc, Hc)
    wloads = [pltpu.make_async_copy(aw_h, wa.at[heads, own, :], lsem.at[10]),
              pltpu.make_async_copy(up_h, wup.at[c, own, :], lsem.at[11]),
              pltpu.make_async_copy(dn_h, wdn.at[c, own, :], lsem.at[12])]
    for cp in loads + wloads:
        cp.start()
    for i, v in enumerate([g1_h, b1_h, ob_h, g2_h, b2_h, db_h]):
        vall[r, i:i + 1, 0:rows] = v[...].reshape(1, rows)
    qvall[c] = qvb_h[...]
    uball[c] = ub_h[...].reshape(1, FH)

    barrier = pltpu.get_barrier_semaphore()
    for ax in (dp, row, col):
        for k in ax.ks():
            pl.semaphore_signal(barrier, inc=1, device_id={ax.axis: ax.up(k)}, device_id_type=MESH)

    xh1[:, SP - 16:, :] = jnp.zeros((NI, 16, D), F32)
    h[:, SP - 16:, :] = jnp.zeros((NI, 16, D), F32)
    yacc[:, SP - 16:, :] = jnp.zeros((NI, 16, D), F32)
    rs1[:, SP - 16:, :] = jnp.zeros((NI, 16, 1), F32)
    sgs[...] = jnp.zeros(sgs.shape, F32)
    loads[0].wait()

    def norm1(i, carry):
        xf = xin[i].astype(F32)
        xh, rstd = norm_parts(xf)
        xh1[i, :SEQ] = xh
        rs1[i, :SEQ] = rstd
        h[i, :SEQ] = xf
        return carry

    lax.fori_loop(0, NI, norm1, 0)
    pl.semaphore_wait(barrier, (DP - 1) + (R - 1) + (C - 1))

    def block(ref, hh, rr, q):
        pr, pw = rows // sr, ref.shape[2] // sl
        return ref.at[hh, pl.ds(pl.multiple_of(rr * rows + (q // sl) * pr, pr), pr),
                      pl.ds(pl.multiple_of(lax.rem(q, sl) * pw, pw), pw)]

    def shard(ref, q):
        pr, pw = rows // sr, ref.shape[-1] // sl
        cut = (pl.ds(pl.multiple_of((q // sl) * pr, pr), pr), pl.ds(pl.multiple_of(lax.rem(q, sl) * pw, pw), pw))
        return ref.at[(slice(None),) + cut] if len(ref.shape) == 3 else ref.at[cut]

    piece = d if part else 0
    weights = [(aw_h, wa, heads), (up_h, wup, c), (dn_h, wdn, c)]

    def gather_z(i):
        src, dst, hh = weights[i]
        out = []
        for k in row.ks():
            out.append(remote(shard(src, piece), block(dst, hh, r, piece), wz.at[0, i, k], wz.at[1, i, k], "row", row.up(k)))
            out[-1].start()
        return out

    def gather_p(i, zs):
        _, dst, hh = weights[i]
        out = []
        for cp, k in zip(zs, row.ks()):
            cp.wait_recv()
            if part:
                for kd in dp.ks():
                    b = block(dst, hh, row.down(k), piece)
                    out.append(remote(b, b, wp.at[0, i, k, kd], wp.at[1, i, k, kd], "dp", dp.up(kd)))
                    out[-1].start()
        return out

    def gather_c(i, ps):
        _, dst, hh = weights[i]
        for cp in ps:
            cp.wait_recv()
        wloads[i].wait()
        out = []
        for k in col.ks():
            out.append(remote(dst.at[hh], dst.at[hh], wc.at[0, i, k], wc.at[1, i, k], "col", col.up(k)))
            out[-1].start()
        return out

    z0 = gather_z(0)
    vz = [remote(vall.at[r], vall.at[r], vsem.at[0, k], vsem.at[1, k], "row", row.up(k)) for k in row.ks()]
    vc = [remote(qvall.at[c], qvall.at[c], vsem.at[2, k], vsem.at[3, k], "col", col.up(k)) for k in col.ks()]
    vc += [remote(uball.at[c], uball.at[c], vsem.at[4, k], vsem.at[5, k], "col", col.up(k)) for k in col.ks()]
    for cp in vz + vc:
        cp.start()
    loads[1].wait()

    def prep(i, carry):
        yacc[i, :SEQ] = cin[i].astype(F32)
        cb[i] = yacc[i].astype(BF16)
        return carry

    lax.fori_loop(0, NI, prep, 0)
    p0 = gather_p(0, z0)
    z1, z2 = gather_z(1), gather_z(2)
    for cp in vz + vc:
        cp.wait_recv()
    vec[...] = jnp.concatenate([vall[rr][:, :rows] for rr in range(R)], axis=1)
    g1, b1, ob, g2, b2, db = (vec[i:i + 1, :] for i in range(6))
    for hh in range(H):
        qb = qvall[hh // Hc][:, (hh % Hc) * E:(hh % Hc + 1) * E]
        zz = jnp.zeros((1, E), F32)
        bias3[hh] = jnp.concatenate([qb[0:1], zz, qb[1:2], zz], axis=1)
    ct[...] = cb[...].reshape(T, D).T
    c0 = gather_c(0, p0)
    for cp in c0:
        cp.wait_recv()
    wot[...] = jnp.concatenate([wa[hh][:, 3 * E:] for hh in range(H)], axis=1)

    key_ok = lax.broadcasted_iota(jnp.int32, (SP, SP), 0) < SEQ

    def fwd(i, carry):
        a = (xh1[i] * vec[0:1, :] + vec[1:2, :]).astype(BF16)
        a1[i] = a
        outs = []
        for hh in range(H):
            t = (mm(a, wa[hh], 1, 0) + bias3[hh]).astype(BF16)
            qkv[i, hh] = t
            q, k, v = t[:, :E], t[:, E:2 * E], t[:, 2 * E:3 * E]
            s = mm(k, q, 1, 1) * (LOG2E / math.sqrt(E))
            s = jnp.where(key_ok, s, -1e30)
            top = jnp.max(s, 0, keepdims=True)
            e = jnp.exp2(s - top)
            p = (e * (1.0 / rsum(e))).astype(BF16)
            pt[i, hh] = p
            outs.append(mm(p, v, 0, 0).astype(BF16))
        oo = jnp.concatenate(outs, axis=1)
        o[i] = oo
        hid = h[i] + mm(oo, wot[...], 1, 1) + vec[2:3, :]
        h[i] = hid
        xh, rstd = norm_parts(hid)
        xh2[i] = xh
        rs2[i] = rstd
        a2[i] = (xh * vec[3:4, :] + vec[4:5, :]).astype(BF16)
        yacc[i] = hid + vec[5:6, :]
        dacc[i] = jnp.zeros((SP, D), F32)
        return carry

    mid1, mid2 = (NI + 2) // 3, (2 * NI + 2) // 3
    lax.fori_loop(0, mid1, fwd, 0)
    p1, p2 = gather_p(1, z1), gather_p(2, z2)
    lax.fori_loop(mid1, mid2, fwd, 0)
    c1, c2 = gather_c(1, p1), gather_c(2, p2)
    lax.fori_loop(mid2, NI, fwd, 0)
    a2t[...] = a2[...].reshape(T, D).T
    for cp in c1 + c2:
        cp.wait_recv()

    redf = Reduce((rows, split), (dp, row, col), (f1, f2, f3, f4, f5, f6, f7), fsem)
    redt = Reduce((rows, split), (dp, row, col), (t1, t2, t3, t4, t5, t6, t7), tsem)

    def ff(half):
        w1, w2 = wup[half], wdn[half]
        bias = uball[half]

        def one(i, tot):
            u = mm(a2[i], w1, 1, 0) + bias
            act, slope = gelu_parts(u)
            gbi = act.astype(BF16)
            dd = mm(cb[i], w2, 1, 0) * slope
            dui = dd.astype(BF16)
            gb[i] = gbi
            du[i] = dui
            yacc[i] += mm(gbi, w2, 1, 1)
            dacc[i] += mm(dui, w1, 1, 1)
            return tot + rsum(dd)

        dubs[half] = lax.fori_loop(0, NI, one, jnp.zeros((1, FH), F32))
        return (mm(a2t[...], du[...].reshape(T, FH), 1, 0), mm(ct[...], gb[...].reshape(T, FH), 1, 0))

    for k in col.ks():
        for a, v in enumerate(ff(col.up(k))):
            redf.put_c(k, a, v)
        redf.start_c(k)
    mine = ff(c)
    redf.wait_c()
    for a, v in enumerate(mine):
        redf.put_p(a, v)
    redf.start_p()

    def mid(i, carry):
        s_db, s_g, s_b, s_ob = carry
        xin[i] = yacc[i][:SEQ].astype(BF16)
        cf = cb[i].astype(F32)
        da = dacc[i]
        xh = xh2[i]
        dh = cf + norm_back(da, vec[3:4, :], xh, rs2[i])
        h[i] = dh
        db_ = dh.astype(BF16)
        a2[i] = db_
        dd = mm(db_, wot[...], 1, 0).astype(BF16)
        for hh in range(H):
            dout[i, hh] = dd[:, hh * E:(hh + 1) * E]
        dacc[i] = jnp.zeros((SP, D), F32)
        return s_db + rsum(cf), s_g + rsum(da * xh), s_b + rsum(da), s_ob + rsum(dh)

    z = jnp.zeros((1, D), F32)
    s_db, s_g2, s_b2, s_ob = lax.fori_loop(0, NI, mid, (z, z, z, z))
    y_cp = pltpu.make_async_copy(xin, y_o, osem.at[0])
    y_cp.start()
    ct[...] = a2[...].reshape(T, D).T
    a2t[...] = a1[...].reshape(T, D).T
    dwo_all = mm(ct[...], o[...].reshape(T, D), 1, 0)
    for hh in range(H):
        dwo[hh] = dwo_all[:, hh * E:(hh + 1) * E]

    scale = 1.0 / math.sqrt(E)

    def back(hh):
        def one(i, tot):
            t = qkv[i, hh]
            q, k, v = t[:, :E], t[:, E:2 * E], t[:, 2 * E:3 * E]
            p = pt[i, hh]
            do = dout[i, hh]
            pf = p.astype(F32)
            dpr = mm(v, do, 1, 1)
            delta = rsum(pf * dpr)
            ds = (pf * (dpr - delta)).astype(BF16)
            dk = mm(ds, q, 1, 0) * scale
            dv = mm(p, do, 1, 0)
            dq = mm(ds, k, 0, 0) * scale
            dd = jnp.concatenate([dq, dk, dv, jnp.zeros((SP, E), F32)], axis=1)
            db_ = dd.astype(BF16)
            dqkv[i] = db_
            dacc[i] += mm(db_, wa[hh], 1, 1)
            return tot + rsum(dd)

        dqvs[hh] = lax.fori_loop(0, NI, one, jnp.zeros((1, W4), F32), unroll=True)
        g = mm(a2t[...], dqkv[...].reshape(T, W4), 1, 0)
        return jnp.concatenate([g[:, :3 * E], dwo[hh]], axis=1)

    for k in col.ks():
        def other(j, carry):
            redt.put_c(k, j, back(col.up(k) * Hc + j))
            return carry

        lax.fori_loop(0, Hc, other, 0)
        redt.start_c(k)
    redf.start_z()
    redt.wait_c()

    def mine_(j, carry):
        redt.put_p(j, back(c * Hc + j))
        return carry

    lax.fori_loop(0, Hc, mine_, 0)
    redt.start_p()
    redf.start_a()

    def last(i, carry):
        s_g, s_b = carry
        da = dacc[i]
        xh = xh1[i]
        dx = h[i] + norm_back(da, vec[0:1, :], xh, rs1[i])
        dxb[i] = dx[:SEQ]
        return s_g + rsum(da * xh), s_b + rsum(da)

    s_g1, s_b1 = lax.fori_loop(0, NI, last, (z, z))
    dx_cp = pltpu.make_async_copy(dxb, dx_o, osem.at[1])
    dx_cp.start()

    six = jnp.concatenate([s_g1, s_b1, s_ob, s_g2, s_b2, s_db], axis=0)
    nf = FH // 128
    for cc in range(C):
        tail = [jnp.concatenate([dqvs[cc * Hc + j][:, :E], dqvs[cc * Hc + j][:, 2 * E:3 * E]], axis=1) for j in range(Hc)]
        tail += [dubs[cc][:, j * 128:(j + 1) * 128] for j in range(nf)]
        tail = jnp.concatenate(tail, axis=0)
        for rr in range(R):
            sgs[cc, rr, 0:6, 0:rows] = six[:, rr * rows:(rr + 1) * rows]
            sgs[cc, rr, 6:6 + Hc + nf, 0:2 * E] = tail
    sgc[c] = sgs[c]
    gc = [remote(sgs.at[col.up(k)], sgc.at[c], gsem.at[0, k], gsem.at[1, k], "col", col.up(k)) for k in col.ks()]
    for cp in gc:
        cp.start()
    for cp in gc:
        cp.wait_recv()
    s = sgc[0]
    for k in range(1, C):
        s = s + sgc[k]
    sgp[d] = s
    gp = [remote(sgp.at[d], sgp.at[d], gsem.at[2, k], gsem.at[3, k], "dp", dp.up(k)) for k in dp.ks()]
    for cp in gp:
        cp.start()
    redt.start_z()
    for cp in gp:
        cp.wait_recv()
    s = sgp[0]
    for k in range(1, DP):
        s = s + sgp[k]
    sgz[...] = s
    sgr[r] = sgz[r]
    gz = [remote(sgz.at[row.up(k)], sgr.at[r], gsem.at[4, k], gsem.at[5, k], "row", row.up(k)) for k in row.ks()]
    for cp in gz:
        cp.start()

    def put_f(a, rs, ls, v):
        so_f[a, rs, ls] = v

    redf.finish(put_f)
    outs = [y_cp, dx_cp, pltpu.make_async_copy(so_f.at[0], dup_o, osem.at[2]), pltpu.make_async_copy(so_f.at[1], ddn_o, osem.at[3])]
    for cp in outs[2:]:
        cp.start()
    redt.start_a()
    for cp in gz:
        cp.wait_recv()
    s = sgr[0]
    for k in range(1, R):
        s = s + sgr[k]
    for j in range(Hc):
        dqvb_o[0:1, j * E:(j + 1) * E] = s[6 + j:7 + j, :E]
        dqvb_o[1:2, j * E:(j + 1) * E] = s[6 + j:7 + j, E:2 * E]
    for i, ref in enumerate([dg1_o, db1_o, dob_o, dg2_o, db2_o, ddb_o]):
        ref[...] = s[i:i + 1, :rows].reshape(rows)
    for j in range(nf):
        dub_o[pl.ds(j * 128, 128)] = s[6 + Hc + j:7 + Hc + j, :].reshape(128)

    def put_t(a, rs, ls, v):
        so_t[a, rs, ls] = v

    redt.finish(put_t)
    outs.append(pltpu.make_async_copy(so_t, daw_o, osem.at[11]))
    outs[-1].start()
    for cp in gc + gp + gz + vz + vc + z0 + z1 + z2 + p0 + p1 + p2 + c0 + c1 + c2:
        cp.wait_send()
    for cp in outs:
        cp.wait()


def pick_split(n, rows, widths):
    for sr in range(1, n + 1):
        if n % sr == 0 and rows % (16 * sr) == 0 and all(w % (128 * (n // sr)) == 0 for w in widths):
            return sr, n // sr
    return 1, 1


def local(sizes, x, g1, b1, aw, qvb, ob, g2, b2, up, ub, dn, db, c):
    DP, R, C = sizes
    NI, SEQ, D = x.shape
    Hc, rows, W4 = aw.shape
    E, FH = W4 // 4, up.shape[1]
    H, SP = C * Hc, -(-SEQ // 16) * 16
    T = NI * SP
    split = pick_split(DP, rows, (W4, FH))
    np_ = split[0] * split[1]
    pr, pw, pf = rows // split[0], W4 // split[1], FH // split[1]
    sd, vm = jax.ShapeDtypeStruct, pltpu.VMEM
    dma = pltpu.SemaphoreType.DMA
    nf = FH // 128
    S = -(-(6 + Hc + nf) // 8) * 8
    cfg = (DP, R, C, NI, SEQ, SP, D, Hc, E, FH, rows, split)

    def red(A, L, pl_):
        return [vm((C - 1, A, D, L), BF16)] * 2 + [vm((np_, R, A, pr, pl_), BF16), vm((DP, R, A, pr, pl_), BF16),
                vm((R, A, pr, pl_), BF16), vm((R, A, pr, pl_), BF16), vm((np_, A, pr, pl_), BF16)]

    scratch = [
        vm((H, D, W4), BF16), vm((C, D, FH), BF16), vm((C, D, FH), BF16), vm((R, 8, 128), F32),
        vm((C, 2, Hc * E), F32), vm((C, 1, FH), F32), vm((8, D), F32), vm((H, 1, W4), F32),
        vm((NI, SEQ, D), BF16), vm((NI, SEQ, D), BF16), vm((NI, SP, D), BF16), vm((NI, SP, D), F32), vm((NI, SP, 1), F32),
        vm((NI, SP, D), BF16), vm((NI, H, SP, W4), BF16), vm((NI, H, SP, SP), BF16), vm((NI, SP, D), BF16),
        vm((NI, SP, D), F32), vm((NI, SP, D), F32), vm((NI, SP, 1), F32), vm((NI, SP, D), BF16), vm((D, D), BF16),
        vm((NI, SP, FH), BF16), vm((NI, SP, FH), BF16), vm((NI, SP, D), F32), vm((NI, SP, D), F32),
        vm((NI, H, SP, E), BF16), vm((NI, SP, W4), BF16), vm((D, T), BF16), vm((D, T), BF16), vm((H, D, E), F32), vm((NI, SEQ, D), F32), vm((C, 1, FH), F32), vm((H, 1, W4), F32),
        *red(2, FH, pf), *red(Hc, W4, pw),
        vm((2, rows, FH), F32), vm((Hc, rows, W4), F32),
        vm((C, R, S, 128), F32), vm((C, R, S, 128), F32), vm((DP, R, S, 128), F32), vm((R, S, 128), F32),
        vm((R, S, 128), F32),
        dma((13,)), dma((12 + nf,)), dma((2, 3, R)), dma((2, 3, R, DP)), dma((2, 3, C)),
        dma((8, max(DP, R, C))), dma((8, max(DP, R, C))), dma((6, max(R, C))), dma((6, max(DP, R, C))),
    ]
    any_ = pl.BlockSpec(memory_space=pl.ANY)
    vm_ = pl.BlockSpec(memory_space=pltpu.VMEM)
    v = lambda a: sd(a.shape, F32)
    return tuple(pl.pallas_call(
        functools.partial(kernel, cfg),
        out_shape=(sd(x.shape, BF16), v(x), v(g1), v(b1), v(aw), v(qvb), v(ob), v(g2), v(b2), v(up), v(ub), v(dn), v(db)),
        in_specs=[any_, vm_, vm_, any_, vm_, vm_, vm_, vm_, any_, vm_, any_, vm_, any_],
        out_specs=[any_, any_, vm_, vm_, any_, vm_, vm_, vm_, vm_, any_, vm_, any_, vm_],
        scratch_shapes=scratch,
        compiler_params=pltpu.CompilerParams(vmem_limit_bytes=67043328, collective_id=0, has_side_effects=True),
    )(x, g1, b1, aw, qvb, ob, g2, b2, up, ub, dn, db, c))


def solution(mesh):
    sizes = tuple(mesh.shape[a] for a in ("dp", "row", "col"))
    placed = (
        P(("dp", "row", "col"), None, None),
        P("row"),
        P("row"),
        P("col", "row", None),
        P(None, "col"),
        P("row"),
        P("row"),
        P("row"),
        P("row", "col"),
        P("col"),
        P("row", "col"),
        P("row"),
        P(("dp", "row", "col"), None, None),
    )
    return jax.shard_map(
        functools.partial(local, sizes),
        mesh=mesh,
        in_specs=placed,
        out_specs=(
            P(("dp", "row", "col"), None, None),
            P(("dp", "row", "col"), None, None),
            P("row"),
            P("row"),
            P("col", "row", None),
            P(None, "col"),
            P("row"),
            P("row"),
            P("row"),
            P("row", "col"),
            P("col"),
            P("row", "col"),
            P("row"),
        ),
        check_vma=False,
    )
```

```python
import functools
import math

import jax
import jax.numpy as jnp
from jax import lax
from jax.experimental import pallas as pl
from jax.experimental.pallas import tpu as pltpu
from jax.sharding import PartitionSpec as P

EPS = 1e-06
ROOT_HALF = 0.7071067811865476
INV_ROOT_TWO_PI = 0.3989422804014327
LOG2E = 1.4426950408889634
F32, BF16 = jnp.float32, jnp.bfloat16
MESH = pl.DeviceIdType.MESH


def mm(a, b, ca, cb):
    return lax.dot_general(a, b, (((ca,), (cb,)), ((), ())), preferred_element_type=F32)


def norm_parts(v):
    mean = jnp.mean(v, -1, keepdims=True)
    cen = v - mean
    rstd = lax.rsqrt(jnp.mean(cen * cen, -1, keepdims=True) + EPS)
    return cen * rstd, rstd


def norm_back(g, gain, xhat, rstd):
    gx = g * gain
    return rstd * (gx - jnp.mean(gx, -1, keepdims=True) - xhat * jnp.mean(gx * xhat, -1, keepdims=True))


def gelu_parts(u):
    w = u * ROOT_HALF
    cdf = 0.5 + 0.5 * lax.erf(w)
    bell = jnp.exp2((w * w) * -LOG2E)
    return u * cdf, cdf + (w * bell) * (INV_ROOT_TWO_PI / ROOT_HALF)


SKIP = set()


def loop(lo, hi, body, init, **kw):
    return init if body.__name__ in SKIP else lax.fori_loop(lo, hi, body, init, **kw)


def rsum(v):
    return jnp.sum(v, 0, keepdims=True)


class Shift:
    def __init__(self, axis, n):
        self.axis, self.n, self.me = axis, n, lax.axis_index(axis)

    def up(self, k):
        return lax.rem(self.me + k, self.n)

    def down(self, k):
        return lax.rem(self.me + self.n - k, self.n)

    def ks(self):
        return range(1, self.n)


def remote(src, dst, ssem, rsem, axis, to):
    return pltpu.make_async_remote_copy(
        src_ref=src, dst_ref=dst, send_sem=ssem, recv_sem=rsem, device_id={axis: to}, device_id_type=MESH)


class Reduce:
    def __init__(self, cfg, ax, bufs, sems):
        self.rows, self.split = cfg
        self.dp, self.row, self.col = ax
        (self.sb, self.rc, self.rp, self.sz, self.rz, self.fin) = bufs
        self.sems = sems
        self.np = self.fin.shape[0]
        self.p, self.z, self.a = [], [], []

    def put(self, slot, a, v):
        sr, sl = self.split
        pr, pw = self.fin.shape[-2:]
        for r in range(self.row.n):
            for qr in range(sr):
                for ql in range(sl):
                    lo = r * self.rows + qr * pr
                    self.sb[slot, qr * sl + ql, r, a] = v[lo:lo + pr, ql * pw:(ql + 1) * pw].astype(BF16)

    def c(self, k):
        return remote(self.sb.at[k - 1], self.rc.at[k - 1], self.sems.at[0, k], self.sems.at[1, k], self.col.axis, self.col.up(k))

    def start_p(self):
        own = self.col.n - 1
        if own:
            t = self.sb[own].astype(F32)
            for k in self.col.ks():
                self.c(k).wait_recv()
                t = t + self.rc[k - 1].astype(F32)
            self.sb[own] = t.astype(BF16)
        if self.np == 1:
            self.rp[self.dp.me] = self.sb[own, 0]
        for k in self.dp.ks():
            to = self.dp.up(k)
            self.p.append(remote(self.sb.at[own, to if self.np > 1 else 0], self.rp.at[self.dp.me],
                                 self.sems.at[2, k], self.sems.at[3, k], self.dp.axis, to))
            self.p[-1].start()

    def start_z(self):
        for cp in self.p:
            cp.wait_recv()
        if self.np > 1:
            t = self.sb[self.col.n - 1, self.dp.me].astype(F32)
            for k in self.dp.ks():
                t = t + self.rp[self.dp.up(k)].astype(F32)
        else:
            t = self.rp[0].astype(F32)
            for q in range(1, self.dp.n):
                t = t + self.rp[q].astype(F32)
        self.sz[...] = t.astype(BF16)
        for k in self.row.ks():
            to = self.row.up(k)
            self.z.append(remote(self.sz.at[to], self.rz.at[self.row.me], self.sems.at[4, k], self.sems.at[5, k],
                                 self.row.axis, to))
            self.z[-1].start()

    def start_a(self):
        for cp in self.z:
            cp.wait_recv()
        t = self.sz[self.row.me].astype(F32)
        for k in self.row.ks():
            t = t + self.rz[self.row.up(k)].astype(F32)
        me = self.dp.me if self.np > 1 else 0
        self.fin[me] = t.astype(BF16)
        if self.np > 1:
            for k in self.dp.ks():
                self.a.append(remote(self.fin.at[me], self.fin.at[me], self.sems.at[6, k], self.sems.at[7, k],
                                     self.dp.axis, self.dp.up(k)))
                self.a[-1].start()

    def finish(self):
        for cp in self.a:
            cp.wait_recv()

    def drain(self):
        for k in self.col.ks():
            self.c(k).wait_send()
        for cp in self.p + self.z + self.a:
            cp.wait_send()


def kernel(cfg, *refs):
    (DP, R, C, NI, SEQ, SP, D, Hc, E, FH, rows, split, chunks) = cfg
    (x_hbm, g1_h, b1_h, aw_h, qvb_h, ob_h, g2_h, b2_h, up_h, ub_h, dn_h, db_h, c_hbm) = refs[:13]
    nc = len(chunks)
    (y_o, dx_o, ft_o, sg_o), ff_o = refs[13:17], refs[17:17 + nc]
    refs = refs[17 + nc:]
    fbuf = [refs[6 * i:6 * i + 6] for i in range(nc)]
    tbuf = [refs[6 * (nc + j):6 * (nc + j) + 6] for j in range(Hc)]
    (wa, wup, wdn, vall, qvall, uball, vec, bias3, xin, cin, cb, xh1, rs1, a1, qkv, pt, o, h, xh2, rs2, a2, wot, wotp,
     gb, du, yacc, dacc, dout, a2t, ct, a1t, dwo, dxb, dubs, dqvs,
     sgs, sgc, sgp, sgz, sgr, sgf,
     lsem, osem, wz, wp, wc, rsem, vsem, gsem) = refs[6 * (nc + Hc):]
    H, T, W4 = C * Hc, NI * SP, 4 * E
    dp, row, col = Shift("dp", DP), Shift("row", R), Shift("col", C)
    d, r, c = dp.me, row.me, col.me
    sr, sl = split
    np_ = sr * sl
    part = np_ > 1

    loads = [pltpu.make_async_copy(x_hbm, xin, lsem.at[0]), pltpu.make_async_copy(c_hbm, cin, lsem.at[1])]
    own = pl.ds(pl.multiple_of(r * rows, rows), rows)
    heads = pl.ds(c * Hc, Hc)
    wloads = [pltpu.make_async_copy(aw_h, wa.at[heads, own, :], lsem.at[10]),
              pltpu.make_async_copy(up_h, wup.at[c, own, :], lsem.at[11]),
              pltpu.make_async_copy(dn_h, wdn.at[c, own, :], lsem.at[12])]
    for cp in loads + wloads:
        cp.start()
    for i, v in enumerate([g1_h, b1_h, ob_h, g2_h, b2_h, db_h]):
        vall[r, i:i + 1, 0:rows] = v[...].reshape(1, rows)
    qvall[c] = qvb_h[...]
    uball[c] = ub_h[...].reshape(1, FH)

    barrier = pltpu.get_barrier_semaphore()
    for ax in (dp, row, col):
        for k in ax.ks():
            pl.semaphore_signal(barrier, inc=1, device_id={ax.axis: ax.up(k)}, device_id_type=MESH)

    xh1[:, SP - 16:, :] = jnp.zeros((NI, 16, D), F32)
    h[:, SP - 16:, :] = jnp.zeros((NI, 16, D), F32)
    yacc[:, SP - 16:, :] = jnp.zeros((NI, 16, D), F32)
    rs1[:, SP - 16:, :] = jnp.zeros((NI, 16, 1), F32)
    sgs[...] = jnp.zeros(sgs.shape, F32)
    loads[0].wait()

    def norm1(i, carry):
        xf = xin[i].astype(F32)
        xh, rstd = norm_parts(xf)
        xh1[i, :SEQ] = xh
        rs1[i, :SEQ] = rstd
        h[i, :SEQ] = xf
        return carry

    loop(0, NI, norm1, 0)
    pl.semaphore_wait(barrier, (DP - 1) + (R - 1) + (C - 1))

    piece = d if part else 0
    off = lax.rem(c * Hc, 2)
    order = [lax.rem(off + e, Hc) for e in range(Hc)]
    units = [(aw_h.at[j], wa.at[c * Hc + j]) for j in order]
    for lo, w in chunks:
        cut = (slice(None), pl.ds(lo, w))
        units += [(up_h.at[cut], wup.at[(c,) + cut]), (dn_h.at[cut], wdn.at[(c,) + cut])]

    def cut_of(ref, rr, q):
        pr, pw = rows // sr, ref.shape[1] // sl
        return ref.at[pl.ds(pl.multiple_of(rr * rows + (q // sl) * pr, pr), pr),
                      pl.ds(pl.multiple_of(lax.rem(q, sl) * pw, pw), pw)]

    def gather_z(u):
        src, dst = units[u]
        out = [remote(cut_of(src, 0, piece), cut_of(dst, r, piece), wz.at[0, u, k], wz.at[1, u, k], "row", row.up(k))
               for k in row.ks()]
        for cp in out:
            cp.start()
        return out

    def gather_p(u, zs):
        dst, out = units[u][1], []
        for cp, k in zip(zs, row.ks()):
            cp.wait_recv()
            if part:
                for kd in dp.ks():
                    b = cut_of(dst, row.down(k), piece)
                    out.append(remote(b, b, wp.at[0, u, k, kd], wp.at[1, u, k, kd], "dp", dp.up(kd)))
                    out[-1].start()
        return out

    def gather_c(u, ps):
        dst, out = units[u][1], []
        for cp in ps:
            cp.wait_recv()
        for k in col.ks():
            out.append(remote(dst, dst, wc.at[0, u, k], wc.at[1, u, k], "col", col.up(k)))
            out[-1].start()
        return out

    U = len(units)
    zs, ps, cs = [None] * U, [None] * U, [None] * U
    for u in range(Hc):
        zs[u] = gather_z(u)
    vz = [remote(vall.at[r], vall.at[r], vsem.at[0, k], vsem.at[1, k], "row", row.up(k)) for k in row.ks()]
    vc = [remote(qvall.at[c], qvall.at[c], vsem.at[2, k], vsem.at[3, k], "col", col.up(k)) for k in col.ks()]
    vc += [remote(uball.at[c], uball.at[c], vsem.at[4, k], vsem.at[5, k], "col", col.up(k)) for k in col.ks()]
    for cp in vz + vc:
        cp.start()
    loads[1].wait()

    def prep(i, carry):
        yacc[i, :SEQ] = cin[i].astype(F32)
        cb[i] = yacc[i].astype(BF16)
        return carry

    loop(0, NI, prep, 0)
    for u in range(Hc):
        ps[u] = gather_p(u, zs[u])
    for u in range(Hc, U):
        zs[u] = gather_z(u)
    for cp in vz + vc:
        cp.wait_recv()
    vec[...] = jnp.concatenate([vall[rr][:, :rows] for rr in range(R)], axis=1)
    for hh in range(H):
        qb = qvall[hh // Hc][:, (hh % Hc) * E:(hh % Hc + 1) * E]
        zz = jnp.zeros((1, E), F32)
        bias3[hh] = jnp.concatenate([zz, qb[0:1], qb[1:2], zz], axis=1)

    def act1(i, carry):
        a1[i] = (xh1[i] * vec[0:1, :] + vec[1:2, :]).astype(BF16)
        return carry

    loop(0, NI, act1, 0)
    ct[...] = cb[...].reshape(T, D).T
    for cp in wloads:
        cp.wait()
    first = min(2, Hc)
    for u in range(first):
        cs[u] = gather_c(u, ps[u])

    live = SEQ // 16 * 16
    key_ok = lax.broadcasted_iota(jnp.int32, (SP - live, SP), 0) < SEQ - live

    def attend(t):
        k, q, v = t[:, :E], t[:, E:2 * E], t[:, 2 * E:3 * E]
        s = mm(k, q, 1, 1)
        s = jnp.concatenate([s[:live], jnp.where(key_ok, s[live:], -1e30)], axis=0)
        top = jnp.max(s, 0, keepdims=True)
        e = jnp.exp2((s - top) * (LOG2E / math.sqrt(E)))
        p = (e * (1.0 / rsum(e))).astype(BF16)
        return p, mm(p, v, 0, 0).astype(BF16)

    def fwd(it, carry):
        pr = lax.rem((c * Hc + 1) // 2 + it, H // 2)
        a = a1[...].reshape(T, D)
        ts = []
        for hh in (2 * pr, 2 * pr + 1):
            w = wa[hh]
            w = jnp.concatenate([w[:, E:2 * E], w[:, :E], w[:, 2 * E:]], axis=1)
            t = (mm(a, w, 1, 0) + bias3[hh]).astype(BF16)
            qkv[hh] = t.reshape(NI, SP, W4)
            ts.append(t)
        for i in range(NI):
            outs = []
            for t, hh in zip(ts, (2 * pr, 2 * pr + 1)):
                p, oh = attend(t[i * SP:(i + 1) * SP])
                pt[hh, i] = p
                outs.append(oh)
            o[i, :, pl.ds(pl.multiple_of(pr * 2 * E, 2 * E), 2 * E)] = jnp.concatenate(outs, axis=1)
        return carry

    loop(0, 1, fwd, 0)
    for u in range(first, Hc):
        cs[u] = gather_c(u, ps[u])
    a1t[:D] = a1[...].reshape(T, D).T
    a1t[D:] = jnp.ones((16, T), BF16)
    a2t[D:] = jnp.ones((16, T), BF16)
    for u in range(Hc, Hc + 2):
        ps[u] = gather_p(u, zs[u])
    for u in range(Hc):
        for cp in cs[u]:
            cp.wait_recv()
    loop(1, H // 2, fwd, 0)
    for u in range(Hc + 2, U):
        ps[u] = gather_p(u, zs[u])
    wot[...] = jnp.concatenate([wa[hh][:, 3 * E:] for hh in range(H)], axis=1)
    for hh in range(H):
        wotp[:, hh * 2 * E:(hh + 1) * 2 * E] = jnp.concatenate([wa[hh][:, 3 * E:], jnp.zeros((D, E), BF16)], axis=1)

    G = math.gcd(NI, 3)
    GT = G * SP

    def proj(i, carry):
        im = pl.ds(i * G, G)
        back3 = lambda v: v.reshape(G, SP, D)
        hid = h[im].reshape(GT, D) + mm(o[im].reshape(GT, D), wot[...], 1, 1) + vec[2:3, :]
        h[im] = back3(hid)
        xh, rstd = norm_parts(hid)
        xh2[im] = back3(xh)
        rs2[im] = rstd.reshape(G, SP, 1)
        a2[im] = back3((xh * vec[3:4, :] + vec[4:5, :]).astype(BF16))
        yacc[im] = back3(hid + vec[5:6, :])
        return carry

    loop(0, NI // G, proj, 0)
    a2t[:D] = a2[...].reshape(T, D).T

    ax = (dp, row, col)
    redf = [Reduce((rows, split), ax, fbuf[i], rsem.at[i]) for i in range(nc)]
    redt = [Reduce((rows, split), ax, tbuf[j], rsem.at[nc + j]) for j in range(Hc)]

    def ff(half, lo, w, first):
        w1, w2 = wup[half, :, lo:lo + w], wdn[half, :, lo:lo + w]
        bias = uball[half, :, lo:lo + w]

        def ffone(i, carry):
            im = pl.ds(i * G, G)
            u = mm(a2[im].reshape(GT, D), w1, 1, 0) + bias
            act, slope = gelu_parts(u)
            gbi = act.astype(BF16)
            dui = (mm(cb[im].reshape(GT, D), w2, 1, 0) * slope).astype(BF16)
            gb[im, :, :w] = gbi.reshape(G, SP, w)
            du[im, :, :w] = dui.reshape(G, SP, w)
            yacc[im] += mm(gbi, w2, 1, 1).reshape(G, SP, D)
            dd = mm(dui, w1, 1, 1).reshape(G, SP, D)
            dacc[im] = dd if first else dacc[im] + dd
            return carry

        loop(0, NI // G, ffone, 0)
        gu = mm(a2t[...], du[:, :, :w].reshape(T, w), 1, 0)
        dubs[half, :, lo:lo + w] = gu[D:D + 1]
        return gu[:D], mm(ct[...], gb[:, :, :w].reshape(T, w), 1, 0)

    for i, (lo, w) in enumerate(chunks):
        if i == 0:
            for u in (Hc, Hc + 1):
                cs[u] = gather_c(u, ps[u])
        for a, v in enumerate(ff(c, lo, w, i == 0)):
            redf[i].put(C - 1, a, v)
        if i == 0:
            for u in range(Hc + 2, U):
                cs[u] = gather_c(u, ps[u])
        else:
            redf[i - 1].start_p()
        for u in (Hc + 2 * i, Hc + 2 * i + 1):
            for cp in cs[u]:
                cp.wait_recv()
        for k in col.ks():
            for a, v in enumerate(ff(col.up(k), lo, w, False)):
                redf[i].put(k - 1, a, v)
            redf[i].c(k).start()

    def mid(i, carry):
        s_db, s_g, s_b, s_ob = carry
        im = pl.ds(i * G, G)
        for j in range(G):
            xin[i * G + j] = yacc[i * G + j][:SEQ].astype(BF16)
        cf = cb[im].reshape(GT, D).astype(F32)
        da = dacc[im].reshape(GT, D)
        xh = xh2[im].reshape(GT, D)
        dh = cf + norm_back(da, vec[3:4, :], xh, rs2[im].reshape(GT, 1))
        h[im] = dh.reshape(G, SP, D)
        db_ = dh.astype(BF16)
        a2[im] = db_.reshape(G, SP, D)
        dd = mm(db_, wotp[...], 1, 0).astype(BF16)
        for hh in range(H):
            dout[hh, im] = dd[:, hh * 2 * E:(hh + 1) * 2 * E].reshape(G, SP, 2 * E)
        return s_db + rsum(cf), s_g + rsum(da * xh), s_b + rsum(da), s_ob + rsum(dh)

    z = jnp.zeros((1, D), F32)
    s_db, s_g2, s_b2, s_ob = loop(0, NI // G, mid, (z, z, z, z))
    y_cp = pltpu.make_async_copy(xin, y_o, osem.at[0])
    y_cp.start()
    ct[...] = a2[...].reshape(T, D).T
    dwo_all = mm(ct[...], o[...].reshape(T, D), 1, 0)
    for hh in range(H):
        dwo[hh] = jnp.concatenate([jnp.zeros((D, E), F32), dwo_all[:, hh * E:(hh + 1) * E]], axis=1)
    redf[nc - 1].start_p()

    low = lax.broadcasted_iota(jnp.int32, (SP, 2 * E), 1) < E

    def back(hh):
        if "back" not in SKIP:
            for i in range(NI):
                kq, v = qkv[hh, i, :, :2 * E], qkv[hh, i, :, 2 * E:]
                p = pt[hh, i]
                do = dout[hh, i]
                pf = p.astype(F32)
                dpr = mm(v * (1.0 / math.sqrt(E)), do, 1, 1)
                delta = rsum(pf * dpr)
                ds = (pf * (dpr - delta)).astype(BF16)
                dk = mm(ds, kq, 1, 0)
                dq = mm(ds, kq, 0, 0)
                dv = mm(p, do, 1, 0)
                qkv[hh, i, :, :2 * E] = jnp.where(low, dq, dk).astype(BF16)
                qkv[hh, i, :, 2 * E:] = dv.astype(BF16)
        g = mm(a1t[...], qkv[hh].reshape(T, W4), 1, 0)
        dqvs[hh] = g[D:D + 1]
        return jnp.concatenate([g[:D, :2 * E], g[:D, 2 * E:] + dwo[hh]], axis=1)

    steps = [lambda: redf[0].start_z(),
             lambda: (redf[0].start_a(), redf[-1].start_z() if nc > 1 else None, redt[0].start_z()),
             lambda: (redf[-1].start_a() if nc > 1 else None, redt[0].start_a(), redt[1].start_z())]
    for j in range(Hc):
        def pair(s, carry):
            redt[j].put(s, 0, back(lax.rem(c + 1 + s, C) * Hc + j))

            @pl.when(s < C - 1)
            def _():
                redt[j].c(s + 1).start()

            return carry

        lax.fori_loop(0, C, pair, 0)
        redt[j].start_p()
        if j < len(steps):
            steps[j]()

    def last(i, carry):
        s_g, s_b = carry
        im = pl.ds(i * G, G)
        da = mm(qkv[0, im].reshape(GT, W4), wa[0], 1, 1)
        for hh in range(1, H):
            da = da + mm(qkv[hh, im].reshape(GT, W4), wa[hh], 1, 1)
        xh = xh1[im].reshape(GT, D)
        dx = h[im].reshape(GT, D) + norm_back(da, vec[0:1, :], xh, rs1[im].reshape(GT, 1))
        for j in range(G):
            dxb[i * G + j] = dx[j * SP:j * SP + SEQ]
        return s_g + rsum(da * xh), s_b + rsum(da)

    s_g1, s_b1 = loop(0, NI // G, last, (z, z))
    dx_cp = pltpu.make_async_copy(dxb, dx_o, osem.at[1])
    dx_cp.start()

    six = jnp.concatenate([s_g1, s_b1, s_ob, s_g2, s_b2, s_db], axis=0)
    nf = FH // 128
    for cc in range(C):
        tail = [jnp.concatenate([dqvs[cc * Hc + j][:, :E], dqvs[cc * Hc + j][:, 2 * E:3 * E]], axis=1) for j in range(Hc)]
        tail += [dubs[cc][:, j * 128:(j + 1) * 128] for j in range(nf)]
        tail = jnp.concatenate(tail, axis=0)
        for rr in range(R):
            sgs[cc, rr, 0:6, 0:rows] = six[:, rr * rows:(rr + 1) * rows]
            sgs[cc, rr, 6:6 + Hc + nf, 0:128] = tail
    sgc[c] = sgs[c]
    gc = [remote(sgs.at[col.up(k)], sgc.at[c], gsem.at[0, k], gsem.at[1, k], "col", col.up(k)) for k in col.ks()]
    for cp in gc:
        cp.start()
    for cp in gc:
        cp.wait_recv()
    s = sgc[0]
    for k in range(1, C):
        s = s + sgc[k]
    sgp[d] = s
    gp = [remote(sgp.at[d], sgp.at[d], gsem.at[2, k], gsem.at[3, k], "dp", dp.up(k)) for k in dp.ks()]
    for cp in gp:
        cp.start()
    redt[Hc - 1].start_z()
    for cp in gp:
        cp.wait_recv()
    s = sgp[0]
    for k in range(1, DP):
        s = s + sgp[k]
    sgz[...] = s
    sgr[r] = sgz[r]
    gz = [remote(sgz.at[row.up(k)], sgr.at[r], gsem.at[4, k], gsem.at[5, k], "row", row.up(k)) for k in row.ks()]
    for cp in gz:
        cp.start()

    outs = [y_cp, dx_cp]
    if Hc > 1:
        redt[Hc - 2].start_a()
    for i in range(nc):
        redf[i].finish()
        outs.append(pltpu.make_async_copy(redf[i].fin, ff_o[i], osem.at[2 + i]))
        outs[-1].start()
    redt[Hc - 1].start_a()
    for cp in gz:
        cp.wait_recv()
    s = sgr[0]
    for k in range(1, R):
        s = s + sgr[k]
    sgf[...] = s
    outs.append(pltpu.make_async_copy(sgf, sg_o, osem.at[2 + nc]))
    outs[-1].start()
    for j in range(Hc):
        redt[j].finish()
        outs.append(pltpu.make_async_copy(redt[j].fin, ft_o.at[j], osem.at[3 + nc + j]))
        outs[-1].start()
    for red in redf + redt:
        red.drain()
    for cp in sum([x for x in zs + ps + cs if x], []):
        cp.wait_send()
    for cp in gc + gp + gz + vz + vc:
        cp.wait_send()
    for cp in outs:
        cp.wait()


def finish_kernel(cfg, *refs):
    rows, Hc, E, nf, (sr, sl), chunks = cfg
    nc = len(chunks)
    (y_i, dx_i, ft_i, sg_i), ff_i, refs = refs[:4], refs[4:4 + nc], refs[4 + nc:]
    (y_o, dx_o, dg1_o, db1_o, daw_o, dqvb_o, dob_o, dg2_o, db2_o, dup_o, dub_o, ddn_o, ddb_o) = refs[:13]
    (ybuf, xbuf, ft, sg, wf, wt, isem, osem), ff = refs[13:21], refs[21:]
    n = ybuf.shape[0]
    small = [pltpu.make_async_copy(i, v, isem.at[2 * n + k]) for k, (i, v) in enumerate(((sg_i, sg), (ft_i, ft), *zip(ff_i, ff)))]
    ins = [pltpu.make_async_copy(dx_i.at[k], xbuf.at[k], isem.at[k]) for k in range(n)]
    ins += [pltpu.make_async_copy(y_i.at[k], ybuf.at[k], isem.at[n + k]) for k in range(n)]
    outs = [pltpu.make_async_copy(xbuf.at[k], dx_o.at[k], osem.at[k]) for k in range(n)]
    outs += [pltpu.make_async_copy(ybuf.at[k], y_o.at[k], osem.at[n + k]) for k in range(n)]
    for cp in small + ins:
        cp.start()
    small[0].wait()
    s = sg[...]
    for i, ref in enumerate([dg1_o, db1_o, dob_o, dg2_o, db2_o, ddb_o]):
        ref[...] = s[i:i + 1, :rows].reshape(rows)
    for j in range(nf):
        dub_o[pl.ds(j * 128, 128)] = s[6 + Hc + j:7 + Hc + j, :128].reshape(128)
    for j in range(Hc):
        dqvb_o[0:1, j * E:(j + 1) * E] = s[6 + j:7 + j, :E]
        dqvb_o[1:2, j * E:(j + 1) * E] = s[6 + j:7 + j, E:2 * E]

    def lay(src, a, ref, lo):
        pr, pw = src.shape[-2:]
        for qr in range(sr):
            for ql in range(sl):
                ref[pl.ds(qr * pr, pr), pl.ds(lo + ql * pw, pw)] = src[qr * sl + ql, a].astype(F32)

    small[1].wait()
    for j in range(Hc):
        lay(ft.at[j], 0, wt.at[j], 0)
    for i, (lo, w) in enumerate(chunks):
        small[2 + i].wait()
        for a in range(2):
            lay(ff[i], a, wf.at[a], lo)
    big = [pltpu.make_async_copy(b, o, osem.at[2 * n + k]) for k, (b, o) in enumerate(((wf.at[0], dup_o), (wf.at[1], ddn_o), (wt, daw_o)))]
    for o in big:
        o.start()
    outs += big
    for i, o in zip(ins, outs):
        i.wait()
        o.start()
    for o in outs:
        o.wait()


def pick_split(n, rows, widths):
    for sr in range(1, n + 1):
        if n % sr == 0 and rows % (16 * sr) == 0 and all(w % (128 * (n // sr)) == 0 for w in widths):
            return sr, n // sr
    return 1, 1


def local(sizes, x, g1, b1, aw, qvb, ob, g2, b2, up, ub, dn, db, c):
    DP, R, C = sizes
    NI, SEQ, D = x.shape
    Hc, rows, W4 = aw.shape
    E, FH = W4 // 4, up.shape[1]
    H, SP = C * Hc, -(-SEQ // 16) * 16
    T = NI * SP
    chunks = ((0, FH - 256), (FH - 256, 256)) if FH % 256 == 0 and FH > 256 else ((0, FH),)
    nc, wmax = len(chunks), max(w for _, w in chunks)
    split = pick_split(DP, rows, (W4,) + tuple(w for _, w in chunks))
    np_ = split[0] * split[1]
    pr, pw = rows // split[0], W4 // split[1]
    sd, vm = jax.ShapeDtypeStruct, pltpu.VMEM
    dma = pltpu.SemaphoreType.DMA
    nf, VW = FH // 128, -(-rows // 128) * 128
    S = -(-(6 + Hc + nf) // 8) * 8
    cfg = (DP, R, C, NI, SEQ, SP, D, Hc, E, FH, rows, split, chunks)

    def red(A, L):
        pw = L // split[1]
        return [vm((C, np_, R, A, pr, pw), BF16), vm((max(C - 1, 1), np_, R, A, pr, pw), BF16), vm((DP, R, A, pr, pw), BF16),
                vm((R, A, pr, pw), BF16), vm((R, A, pr, pw), BF16), vm((np_, A, pr, pw), BF16)]

    scratch = sum([red(2, w) for _, w in chunks] + [red(1, W4)] * Hc, []) + [
        vm((H, D, W4), BF16), vm((C, D, FH), BF16), vm((C, D, FH), BF16), vm((R, 8, VW), F32),
        vm((C, 2, Hc * E), F32), vm((C, 1, FH), F32), vm((8, D), F32), vm((H, 1, W4), F32),
        vm((NI, SEQ, D), BF16), vm((NI, SEQ, D), BF16), vm((NI, SP, D), BF16), vm((NI, SP, D), F32), vm((NI, SP, 1), F32),
        vm((NI, SP, D), BF16), vm((H, NI, SP, W4), BF16), vm((H, NI, SP, SP), BF16), vm((NI, SP, D), BF16),
        vm((NI, SP, D), F32), vm((NI, SP, D), F32), vm((NI, SP, 1), F32), vm((NI, SP, D), BF16), vm((D, D), BF16),
        vm((D, 2 * D), BF16),
        vm((NI, SP, wmax), BF16), vm((NI, SP, wmax), BF16), vm((NI, SP, D), F32), vm((NI, SP, D), F32),
        vm((H, NI, SP, 2 * E), BF16), vm((D + 16, T), BF16), vm((D, T), BF16), vm((D + 16, T), BF16),
        vm((H, D, 2 * E), F32), vm((NI, SEQ, D), F32), vm((C, 1, FH), F32), vm((H, 1, W4), F32),
        vm((C, R, S, VW), F32), vm((C, R, S, VW), F32), vm((DP, R, S, VW), F32), vm((R, S, VW), F32),
        vm((R, S, VW), F32), vm((S, VW), F32),
        dma((13,)), dma((3 + nc + Hc,)), dma((2, Hc + 2 * nc, R)), dma((2, Hc + 2 * nc, R, DP)), dma((2, Hc + 2 * nc, C)),
        dma((nc + Hc, 8, max(DP, R, C))), dma((6, max(R, C))), dma((6, max(DP, R, C))),
    ]
    any_ = pl.BlockSpec(memory_space=pl.ANY)
    vm_ = pl.BlockSpec(memory_space=pltpu.VMEM)
    v = lambda a: sd(a.shape, F32)
    y, dx, ft, sg, *ff = pl.pallas_call(
        functools.partial(kernel, cfg),
        out_shape=(sd(x.shape, BF16), v(x), sd((Hc, np_, 1, pr, pw), BF16), sd((S, VW), F32),
                   *[sd((np_, 2, pr, w // split[1]), BF16) for _, w in chunks]),
        in_specs=[any_, vm_, vm_, any_, vm_, vm_, vm_, vm_, any_, vm_, any_, vm_, any_],
        out_specs=[any_] * (4 + nc),
        scratch_shapes=scratch,
        compiler_params=pltpu.CompilerParams(vmem_limit_bytes=67043328, collective_id=0, has_side_effects=True),
    )(x, g1, b1, aw, qvb, ob, g2, b2, up, ub, dn, db, c)
    return tuple(pl.pallas_call(
        functools.partial(finish_kernel, (rows, Hc, E, nf, split, chunks)),
        out_shape=(sd(x.shape, BF16), v(x), v(g1), v(b1), v(aw), v(qvb), v(ob), v(g2), v(b2), v(up), v(ub), v(dn), v(db)),
        in_specs=[any_] * (4 + nc),
        out_specs=[any_, any_, vm_, vm_, any_, vm_, vm_, vm_, vm_, any_, vm_, any_, vm_],
        scratch_shapes=[vm(x.shape, BF16), vm(x.shape, F32), vm(ft.shape, BF16), vm(sg.shape, F32),
                        vm((2, rows, FH), F32), vm(aw.shape, F32), dma((2 * NI + 2 + nc,)), dma((2 * NI + 3,)),
                        *[vm(f.shape, BF16) for f in ff]],
        compiler_params=pltpu.CompilerParams(vmem_limit_bytes=67043328),
    )(y, dx, ft, sg, *ff))


def solution(mesh):
    sizes = tuple(mesh.shape[a] for a in ("dp", "row", "col"))
    placed = (
        P(("dp", "row", "col"), None, None),
        P("row"),
        P("row"),
        P("col", "row", None),
        P(None, "col"),
        P("row"),
        P("row"),
        P("row"),
        P("row", "col"),
        P("col"),
        P("row", "col"),
        P("row"),
        P(("dp", "row", "col"), None, None),
    )
    return jax.shard_map(
        functools.partial(local, sizes),
        mesh=mesh,
        in_specs=placed,
        out_specs=(
            P(("dp", "row", "col"), None, None),
            P(("dp", "row", "col"), None, None),
            P("row"),
            P("row"),
            P("col", "row", None),
            P(None, "col"),
            P("row"),
            P("row"),
            P("row"),
            P("row", "col"),
            P("col"),
            P("row", "col"),
            P("row"),
        ),
        check_vma=False,
    )
```

```python
import functools
import math

import jax
import jax.numpy as jnp
from jax import lax
from jax.experimental import pallas as pl
from jax.experimental.pallas import tpu as pltpu
from jax.sharding import PartitionSpec as P

EPS = 1e-06
ROOT_HALF = 0.7071067811865476
INV_ROOT_TWO_PI = 0.3989422804014327
LOG2E = 1.4426950408889634
F32, BF16 = jnp.float32, jnp.bfloat16
MESH = pl.DeviceIdType.MESH


def mm(a, b, ca, cb):
    return lax.dot_general(a, b, (((ca,), (cb,)), ((), ())), preferred_element_type=F32)


def norm_parts(v):
    mean = jnp.mean(v, -1, keepdims=True)
    cen = v - mean
    rstd = lax.rsqrt(jnp.mean(cen * cen, -1, keepdims=True) + EPS)
    return cen * rstd, rstd


def norm_back(g, gain, xhat, rstd):
    gx = g * gain
    return rstd * (gx - jnp.mean(gx, -1, keepdims=True) - xhat * jnp.mean(gx * xhat, -1, keepdims=True))


def gelu_parts(u):
    w = u * ROOT_HALF
    cdf = 0.5 + 0.5 * lax.erf(w)
    bell = jnp.exp2((w * w) * -LOG2E)
    return u * cdf, cdf + (w * bell) * (INV_ROOT_TWO_PI / ROOT_HALF)


SKIP = set()


def loop(lo, hi, body, init, **kw):
    return init if body.__name__ in SKIP else lax.fori_loop(lo, hi, body, init, **kw)


def rsum(v):
    return jnp.sum(v, 0, keepdims=True)


def fold(v):
    t = v[:8]
    for lo in range(8, v.shape[0], 8):
        t = t + v[lo:lo + 8]
    return t


class Shift:
    def __init__(self, axis, n):
        self.axis, self.n, self.me = axis, n, lax.axis_index(axis)

    def up(self, k):
        return lax.rem(self.me + k, self.n)

    def down(self, k):
        return lax.rem(self.me + self.n - k, self.n)

    def ks(self):
        return range(1, self.n)


def remote(src, dst, ssem, rsem, axis, to):
    return pltpu.make_async_remote_copy(
        src_ref=src, dst_ref=dst, send_sem=ssem, recv_sem=rsem, device_id={axis: to}, device_id_type=MESH)


def settle(sem, region):
    pltpu.make_async_copy(region, region, sem).wait()


class Reduce:
    def __init__(self, cfg, ax, bufs, sems, halve):
        self.rows, self.split = cfg
        self.dp, self.row, self.col = ax
        (self.sb, self.rc, self.rp, self.sz, self.rz, self.fin) = bufs
        self.sems = sems
        self.np = self.fin.shape[0]
        self.halve = halve and self.np == 4
        self.own = self.col.n - 1

    def put(self, slot, a, v):
        sr, sl = self.split
        pr, pw = self.fin.shape[-2:]
        for r in range(self.row.n):
            for qr in range(sr):
                for ql in range(sl):
                    lo = r * self.rows + qr * pr
                    self.sb[slot, qr * sl + ql, a, r] = v[lo:lo + pr, ql * pw:(ql + 1) * pw].astype(BF16)

    def copy(self, src, dst, stage, ax, to):
        return remote(src, dst, self.sems.at[0, stage], self.sems.at[1, stage], ax.axis, to)

    def c(self, k):
        return self.copy(self.sb.at[k - 1], self.rc.at[k - 1], 0, self.col, self.col.up(k))

    def wait(self, side, stage):
        n, m = self.dp.n - 1, self.row.n - 1
        live = (self.own, n, self.halve, m, n and self.np > 1)[stage]
        if live:
            region = (lambda: self.rc, lambda: self.rp.at[0:2 if self.halve else n], lambda: self.rp.at[2],
                      lambda: self.rz.at[0:m], lambda: self.fin.at[0:n])[stage]
            settle(self.sems.at[side, stage], region())

    def halves(self, a):
        lo, hi = lax.rem(self.dp.me, 2), self.dp.me // 2
        if a % 2 == 0:
            return lo, hi, lambda x, y: x + 2 * y, self.dp.me + 1 - 2 * lo, self.dp.me + 2 - 4 * hi
        return hi, lo, lambda x, y: 2 * x + y, self.dp.me + 2 - 4 * hi, self.dp.me + 1 - 2 * lo

    def arrays(self):
        return range(self.fin.shape[1])

    def ps(self):
        if not self.halve:
            return [self.copy(self.sb.at[self.own, self.dp.up(k) if self.np > 1 else 0], self.rp.at[self.dp.me], 1,
                              self.dp, self.dp.up(k)) for k in self.dp.ks()]
        out = []
        for a in self.arrays():
            bit, _, at, to, _ = self.halves(a)
            for i in range(2):
                out.append(self.copy(self.sb.at[self.own, at(1 - bit, i), a], self.rp.at[i, a], 1, self.dp, to))
        return out

    def qs(self):
        out = []
        for a in self.arrays() if self.halve else ():
            bit, other, at, _, to = self.halves(a)
            out.append(self.copy(self.sb.at[self.own, at(bit, 1 - other), a], self.rp.at[2, a], 2, self.dp, to))
        return out

    def zs(self):
        return [self.copy(self.sz.at[self.row.up(k)], self.rz.at[self.row.me], 3, self.row, self.row.up(k))
                for k in self.row.ks()]

    def as_(self):
        if self.np == 1:
            return []
        mine = self.fin.at[self.dp.me]
        return [self.copy(mine, mine, 4, self.dp, self.dp.up(k)) for k in self.dp.ks()]

    def start_p(self):
        if self.own:
            self.wait(1, 0)
            t = self.sb[self.own].astype(F32)
            for k in self.col.ks():
                t = t + self.rc[k - 1].astype(F32)
            self.sb[self.own] = t.astype(BF16)
        if self.np == 1:
            self.rp[self.dp.me] = self.sb[self.own, 0]
        for cp in self.ps():
            cp.start()

    def start_q(self):
        if self.halve:
            self.wait(1, 1)
            for a in self.arrays():
                bit, other, at, _, _ = self.halves(a)
                q = at(bit, 1 - other)
                t = self.sb[self.own, q, a].astype(F32) + self.rp[1 - other, a].astype(F32)
                self.sb[self.own, q, a] = t.astype(BF16)
            for cp in self.qs():
                cp.start()

    def start_z(self):
        self.wait(1, 2 if self.halve else 1)
        for a in self.arrays():
            if self.halve:
                _, other, _, _, _ = self.halves(a)
                t = self.sb[self.own, self.dp.me, a].astype(F32) + self.rp[other, a].astype(F32) + self.rp[2, a].astype(F32)
            elif self.np > 1:
                t = self.sb[self.own, self.dp.me, a].astype(F32)
                for k in self.dp.ks():
                    t = t + self.rp[self.dp.up(k), a].astype(F32)
            else:
                t = self.rp[0, a].astype(F32)
                for q in range(1, self.dp.n):
                    t = t + self.rp[q, a].astype(F32)
            self.sz[:, a] = t.astype(BF16)
        for cp in self.zs():
            cp.start()

    def start_a(self):
        self.wait(1, 3)
        t = self.sz[self.row.me].astype(F32)
        for k in self.row.ks():
            t = t + self.rz[self.row.up(k)].astype(F32)
        self.fin[self.dp.me if self.np > 1 else 0] = t.astype(BF16)
        for cp in self.as_():
            cp.start()

    def finish(self):
        self.wait(1, 4)

    def drain(self):
        for stage in range(5):
            self.wait(0, stage)


def kernel(cfg, *refs):
    (DP, R, C, NI, SEQ, SP, D, Hc, E, FH, rows, split, chunks) = cfg
    (x_hbm, g1_h, b1_h, aw_h, qvb_h, ob_h, g2_h, b2_h, up_h, ub_h, dn_h, db_h, c_hbm) = refs[:13]
    nc = len(chunks)
    (y_o, dx_o, ft_o, sg_o), ff_o = refs[13:17], refs[17:17 + nc]
    refs = refs[17 + nc:]
    fbuf = [refs[6 * i:6 * i + 6] for i in range(nc)]
    tbuf = [refs[6 * (nc + j):6 * (nc + j) + 6] for j in range(Hc)]
    (wa, wup, wdn, vall, qvall, uball, vec, bias3, xin, cin, cb, xh1, rs1, a1, qkv, pt, o, h, xh2, rs2, a2, wot, wotp,
     gb, du, yacc, dacc, dout, a2t, ct, a1t, dwo, dxb, dubs, dqvs,
     sgs, sgc, sgp, sgz, sgr, sgf,
     lsem, osem, wsem, csem, rsem, vsem) = refs[6 * (nc + Hc):]
    H, T, W4 = C * Hc, NI * SP, 4 * E
    dp, row, col = Shift("dp", DP), Shift("row", R), Shift("col", C)
    d, r, c = dp.me, row.me, col.me
    sr, sl = split
    np_ = sr * sl
    part = np_ > 1

    loads = [pltpu.make_async_copy(x_hbm, xin, lsem.at[0]), pltpu.make_async_copy(c_hbm, cin, lsem.at[1])]
    own = pl.ds(pl.multiple_of(r * rows, rows), rows)
    heads = pl.ds(c * Hc, Hc)
    wloads = [pltpu.make_async_copy(aw_h, wa.at[heads, own, :], lsem.at[2]),
              pltpu.make_async_copy(up_h, wup.at[c, own, :], lsem.at[3]),
              pltpu.make_async_copy(dn_h, wdn.at[c, own, :], lsem.at[4])]
    for cp in loads + wloads:
        cp.start()
    for i, v in enumerate([g1_h, b1_h, ob_h, g2_h, b2_h, db_h]):
        vall[r, i:i + 1, 0:rows] = v[...].reshape(1, rows)
    qvall[c] = qvb_h[...]
    uball[c] = ub_h[...].reshape(1, FH)

    barrier = pltpu.get_barrier_semaphore()
    for ax in (dp, row, col):
        for k in ax.ks():
            pl.semaphore_signal(barrier, inc=1, device_id={ax.axis: ax.up(k)}, device_id_type=MESH)

    xh1[:, SP - 16:, :] = jnp.zeros((NI, 16, D), F32)
    h[:, SP - 16:, :] = jnp.zeros((NI, 16, D), F32)
    yacc[:, SP - 16:, :] = jnp.zeros((NI, 16, D), F32)
    rs1[:, SP - 16:, :] = jnp.zeros((NI, 16, 1), F32)
    sgs[...] = jnp.zeros(sgs.shape, F32)
    pl.semaphore_wait(barrier, (DP - 1) + (R - 1) + (C - 1))

    piece = d if part else 0
    off = lax.rem(c * Hc, 2)
    order = [lax.rem(off + e, Hc) for e in range(Hc)]
    units = [[(aw_h.at[j], wa.at[c * Hc + j])] for j in order]
    for lo, w in chunks:
        cut = (slice(None), pl.ds(lo, w))
        units.append([(up_h.at[cut], wup.at[(c,) + cut]), (dn_h.at[cut], wdn.at[(c,) + cut])])

    def cut_of(ref, rr, q):
        pr, pw = rows // sr, ref.shape[1] // sl
        return ref.at[pl.ds(pl.multiple_of(rr * rows + (q // sl) * pr, pr), pr),
                      pl.ds(pl.multiple_of(lax.rem(q, sl) * pw, pw), pw)]

    def gather_z(u):
        return [remote(cut_of(src, 0, piece), cut_of(dst, r, piece), wsem.at[0, 0, u], wsem.at[1, 0, u], "row", row.up(k))
                for src, dst in units[u] for k in row.ks()]

    def gather_p(u):
        out = []
        for _, dst in units[u] if part else ():
            for k in row.ks():
                b = cut_of(dst, row.down(k), piece)
                out += [remote(b, b, wsem.at[0, 1, u], wsem.at[1, 1, u], "dp", dp.up(kd)) for kd in dp.ks()]
        return out

    def gather_c(u):
        at = u if u < Hc else Hc + 2 * (u - Hc)
        return [remote(dst, dst, csem.at[0, at + i, k - 1], csem.at[1, at + i, k - 1], "col", col.up(k))
                for i, (_, dst) in enumerate(units[u]) for k in col.ks()]

    def settle_z(side, u):
        sb = (tbuf[u] if u < Hc else fbuf[u - Hc])[0]
        if R > 1:
            settle(wsem.at[side, 0, u], sb.at[0, 0, :, 0:R - 1])

    def settle_p(side, u):
        sb = (tbuf[u] if u < Hc else fbuf[u - Hc])[0]
        if R > 1 and part:
            settle(wsem.at[side, 1, u], sb.at[0, 0:DP - 1, :, 0:R - 1])

    def settle_c(side, u):
        for cp in gather_c(u):
            cp.wait_recv() if side else cp.wait_send()

    def begin(copies):
        for cp in copies:
            cp.start()

    U = Hc + nc
    for u in range(Hc):
        begin(gather_z(u))
    vz = [remote(vall.at[r], vall.at[r], vsem.at[0, 0], vsem.at[1, 0], "row", row.up(k)) for k in row.ks()]
    vc = [remote(qvall.at[c], qvall.at[c], vsem.at[0, 1], vsem.at[1, 1], "col", col.up(k)) for k in col.ks()]
    vc += [remote(uball.at[c], uball.at[c], vsem.at[0, 2], vsem.at[1, 2], "col", col.up(k)) for k in col.ks()]

    def settle_v(side):
        if R > 1:
            settle(vsem.at[side, 0], vall.at[0:R - 1])
        if C > 1:
            settle(vsem.at[side, 1], qvall.at[0:C - 1])
            settle(vsem.at[side, 2], uball.at[0:C - 1])

    def settle_g(side, stage):
        n, ref = ((C - 1, sgc), (DP - 1, sgp), (R - 1, sgr))[stage]
        if n:
            settle(vsem.at[side, 3 + stage], ref.at[0:n])

    begin(vz + vc)
    loads[0].wait()

    def norm1(i, carry):
        xf = xin[i].astype(F32)
        xh, rstd = norm_parts(xf)
        xh1[i, :SEQ] = xh
        rs1[i, :SEQ] = rstd
        h[i, :SEQ] = xf
        return carry

    loop(0, NI, norm1, 0)
    for u in range(Hc):
        settle_z(1, u)
        begin(gather_p(u))
    for u in range(Hc, U):
        begin(gather_z(u))
    loads[1].wait()

    def prep(i, carry):
        yacc[i, :SEQ] = cin[i].astype(F32)
        cb[i] = yacc[i].astype(BF16)
        return carry

    loop(0, NI, prep, 0)
    settle_v(1)
    vec[...] = jnp.concatenate([vall[rr][:, :rows] for rr in range(R)], axis=1)
    for hh in range(H):
        qb = qvall[hh // Hc][:, (hh % Hc) * E:(hh % Hc + 1) * E]
        zz = jnp.zeros((1, E), F32)
        bias3[hh] = jnp.concatenate([zz, qb[0:1], qb[1:2], zz], axis=1)

    def act1(i, carry):
        a1[i] = (xh1[i] * vec[0:1, :] + vec[1:2, :]).astype(BF16)
        return carry

    loop(0, NI, act1, 0)
    for cp in wloads:
        cp.wait()
    first = min(2, Hc)
    for u in range(first):
        settle_p(1, u)
        begin(gather_c(u))

    live = SEQ // 16 * 16
    key_ok = lax.broadcasted_iota(jnp.int32, (SP - live, SP), 0) < SEQ - live

    def logits(t):
        return mm(t[:, :E], t[:, E:2 * E], 1, 1)

    def attend(s, t):
        s = jnp.concatenate([s[:live], jnp.where(key_ok, s[live:], -1e30)], axis=0)
        top = jnp.max(s, 0, keepdims=True)
        e = jnp.exp2((s - top) * (LOG2E / math.sqrt(E)))
        return (e * (1.0 / rsum(e))).astype(BF16)

    def weigh(p, t):
        return mm(p, t[:, 2 * E:3 * E], 0, 0).astype(BF16)

    def fwd(it, carry):
        pr = lax.rem((c * Hc + 1) // 2 + it, H // 2)
        a = a1[...].reshape(T, D)
        ts = []
        for hh in (2 * pr, 2 * pr + 1):
            w = wa[hh]
            w = jnp.concatenate([w[:, E:2 * E], w[:, :E], w[:, 2 * E:]], axis=1)
            t = (mm(a, w, 1, 0) + bias3[hh]).astype(BF16)
            qkv[hh] = t.reshape(NI, SP, W4)
            ts.append(t)
        todo = [(i, j, ts[j][i * SP:(i + 1) * SP]) for i in range(NI) for j in range(2)]
        ahead, probs, outs = [logits(todo[0][2])], [], []

        def out(n):
            i, j, t = todo[n]
            outs.append(weigh(probs[n], t))
            if j == 1:
                o[i, :, pl.ds(pl.multiple_of(pr * 2 * E, 2 * E), 2 * E)] = jnp.concatenate(outs[-2:], axis=1)

        for n, (i, j, t) in enumerate(todo):
            if n + 1 < len(todo):
                ahead.append(logits(todo[n + 1][2]))
            probs.append(attend(ahead[n], t))
            pt[2 * pr + j, i] = probs[n]
            if n:
                out(n - 1)
        out(len(todo) - 1)
        return carry

    loop(0, 1, fwd, 0)
    for u in range(first, Hc):
        settle_p(1, u)
        begin(gather_c(u))
    for u in range(Hc, U):
        settle_z(1, u)
        begin(gather_p(u))
    ct[...] = cb[...].reshape(T, D).T
    a1t[:D] = a1[...].reshape(T, D).T
    a1t[D:] = jnp.ones((16, T), BF16)
    a2t[D:] = jnp.ones((16, T), BF16)
    for u in range(Hc):
        settle_c(1, u)
    loop(1, H // 2, fwd, 0)
    wot[...] = jnp.concatenate([wa[hh][:, 3 * E:] for hh in range(H)], axis=1)
    for hh in range(H):
        wotp[:, hh * 2 * E:(hh + 1) * 2 * E] = jnp.concatenate([wa[hh][:, 3 * E:], jnp.zeros((D, E), BF16)], axis=1)
    settle_p(1, Hc)
    begin(gather_c(Hc))

    G = 2 if NI % 2 == 0 else 1
    GT, B = G * SP, 16
    tiles = [(lo, min(B, SP - lo)) for lo in range(0, SP, B)]

    if "proj" not in SKIP:
        ms = [mm(o[0], wot[...], 1, 1)]
        for i in range(NI):
            if i + 1 < NI:
                ms.append(mm(o[i + 1], wot[...], 1, 1))
            for lo, n in tiles:
                rs = slice(lo, lo + n)
                hid = h[i, rs] + ms[i][rs] + vec[2:3, :]
                h[i, rs] = hid
                xh, rstd = norm_parts(hid)
                xh2[i, rs] = xh
                rs2[i, rs] = rstd
                a2[i, rs] = (xh * vec[3:4, :] + vec[4:5, :]).astype(BF16)
                yacc[i, rs] = hid + vec[5:6, :]
    a2t[:D] = a2[...].reshape(T, D).T

    ax = (dp, row, col)
    redf = [Reduce((rows, split), ax, fbuf[i], rsem.at[i], True) for i in range(nc)]
    redt = [Reduce((rows, split), ax, tbuf[j], rsem.at[nc + j], False) for j in range(Hc)]

    plan = {("f", 2): [(0, "q")], "mid": [(1, "q"), (2, "p"), (0, "z")], (1, 0): [(1, "z"), (2, "q")],
            (1, 1): [(0, "a")], (2, 0): [(2, "z")], (2, 1): [(3, "z")], "last": [(4, "z"), (1, "a")],
            "end": [(5, "z"), (2, "a"), (3, "a")], "end2": [(4, "a")], "end3": [(5, "a")]}
    reds = redf + redt
    if (nc, Hc, C) != (3, 3, 2):
        plan = {"mid": [(nc - 1, "p")], "last": [(u, "q") for u in range(nc + Hc)] + [(u, "z") for u in range(nc + Hc)],
                "end": [(u, "a") for u in range(nc + Hc)]}

    def step(at):
        for u, what in plan.get(at, ()):
            getattr(reds[u], "start_" + what)()

    def ff(half, lo, w, first):
        w1, w2 = wup.at[half, :, lo:lo + w], wdn.at[half, :, lo:lo + w]
        bias = uball[half, :, lo:lo + w]

        halves = [(k, min(256, w - k)) for k in range(0, w, 256)]
        todo = [(slice(i, i + G), k, m) for i in range(0, NI, G) for k, m in halves]

        def dots(n):
            im, k, m = todo[n]
            return (mm(a2[im].reshape(GT, D), w1[:, k:k + m], 1, 0), mm(cb[im].reshape(GT, D), w2[:, k:k + m], 1, 0))

        def down(im):
            yacc[im] += mm(gb[im, :, :w].reshape(GT, w), w2[...], 1, 1).reshape(G, SP, D)
            dd = mm(du[im, :, :w].reshape(GT, w), w1[...], 1, 1).reshape(G, SP, D)
            dacc[im] = dd if first else dacc[im] + dd

        if "ffone" not in SKIP:
            ahead = [dots(0)]
            for n, (im, k, m) in enumerate(todo):
                if n + 1 < len(todo):
                    ahead.append(dots(n + 1))
                u, dd = ahead[n]
                act, slope = gelu_parts(u + bias[:, k:k + m])
                gb[im, :, k:k + m] = act.astype(BF16).reshape(G, SP, m)
                du[im, :, k:k + m] = (dd * slope).astype(BF16).reshape(G, SP, m)
                if k == 0 and n:
                    down(todo[n - 1][0])
            down(todo[-1][0])
        gu = mm(a2t[...], du[:, :, :w].reshape(T, w), 1, 0)
        dubs[half, :, lo:lo + w] = gu[D:D + 1]
        return gu[:D], mm(ct[...], gb[:, :, :w].reshape(T, w), 1, 0)

    for i, (lo, w) in enumerate(chunks):
        for a, v in enumerate(ff(c, lo, w, i == 0)):
            redf[i].put(C - 1, a, v)
        if i:
            redf[i - 1].start_p()
        step(("f", i))
        if i + 1 < nc:
            settle_p(1, Hc + i + 1)
            begin(gather_c(Hc + i + 1))
        settle_c(1, Hc + i)
        for k in col.ks():
            for a, v in enumerate(ff(col.up(k), lo, w, False)):
                redf[i].put(k - 1, a, v)
            redf[i].c(k).start()

    z = jnp.zeros((8, D), F32)
    def dout_of(i):
        dd = mm(a2[i], wotp[...], 1, 0).astype(BF16)
        for hh in range(H):
            dout[hh, i] = dd[:, hh * 2 * E:(hh + 1) * 2 * E]

    sums = [z, z, z, z]
    for i in range(NI):
        xin[i] = yacc[i][:SEQ].astype(BF16)
        for lo, n in tiles:
            rs = slice(lo, lo + n)
            cf = cb[i, rs].astype(F32)
            da = dacc[i, rs]
            xh = xh2[i, rs]
            dh = cf + norm_back(da, vec[3:4, :], xh, rs2[i, rs])
            h[i, rs] = dh
            a2[i, rs] = dh.astype(BF16)
            sums = [t + fold(v) for t, v in zip(sums, (cf, da * xh, da, dh))]
        if i:
            dout_of(i - 1)
    dout_of(NI - 1)
    s_db, s_g2, s_b2, s_ob = (rsum(v) for v in sums)
    y_cp = pltpu.make_async_copy(xin, y_o, osem.at[0])
    y_cp.start()
    step("mid")
    ct[...] = a2[...].reshape(T, D).T
    dwo_all = mm(ct[...], o[...].reshape(T, D), 1, 0)
    for hh in range(H):
        dwo[hh] = jnp.concatenate([jnp.zeros((D, E), F32), dwo_all[:, hh * E:(hh + 1) * E]], axis=1)

    low = lax.broadcasted_iota(jnp.int32, (SP, 2 * E), 1) < E

    def back(hh):
        if "back" not in SKIP:
            def dprob(i):
                return mm(qkv[hh, i, :, 2 * E:] * (1.0 / math.sqrt(E)), dout[hh, i], 1, 1)

            def grads(i, p, ds):
                kq = qkv[hh, i, :, :2 * E]
                dv = mm(p, dout[hh, i], 1, 0)
                dk = mm(ds, kq, 1, 0)
                dq = mm(ds, kq, 0, 0)
                qkv[hh, i, :, :2 * E] = jnp.where(low, dq, dk).astype(BF16)
                qkv[hh, i, :, 2 * E:] = dv.astype(BF16)

            ahead, last_ = [dprob(0)], None
            for i in range(NI):
                if i + 1 < NI:
                    ahead.append(dprob(i + 1))
                dpr = ahead[i]
                p = pt[hh, i]
                pf = p.astype(F32)
                delta = rsum(pf * dpr)
                ds = (pf * (dpr - delta)).astype(BF16)
                if last_:
                    grads(*last_)
                last_ = (i, p, ds)
            grads(*last_)
        g = mm(a1t[...], qkv[hh].reshape(T, W4), 1, 0)
        dqvs[hh] = g[D:D + 1]
        return jnp.concatenate([g[:D, :2 * E], g[:D, 2 * E:] + dwo[hh]], axis=1)

    for j in range(Hc):
        def pair(s, carry):
            redt[j].put(s, 0, back(lax.rem(c + 1 + s, C) * Hc + j))

            @pl.when(s < C - 1)
            def _():
                redt[j].c(s + 1).start()
                step((j, 0))

            return carry

        lax.fori_loop(0, C, pair, 0)
        redt[j].start_p()
        step((j, 1))

    def da1(i):
        t = mm(qkv[0, i], wa[0], 1, 1)
        for hh in range(1, H):
            t = t + mm(qkv[hh, i], wa[hh], 1, 1)
        return t

    sums, ds = [z, z], [da1(0)]
    for i in range(NI):
        if i + 1 < NI:
            ds.append(da1(i + 1))
        for lo, n in tiles:
            rs = slice(lo, lo + n)
            da = ds[i][rs]
            xh = xh1[i, rs]
            dx = h[i, rs] + norm_back(da, vec[0:1, :], xh, rs1[i, rs])
            keep = min(n, SEQ - lo)
            dxb[i, lo:lo + keep] = dx[:keep]
            sums = [t + fold(v) for t, v in zip(sums, (da * xh, da))]
    s_g1, s_b1 = (rsum(v) for v in sums)
    dx_cp = pltpu.make_async_copy(dxb, dx_o, osem.at[1])
    dx_cp.start()

    six = jnp.concatenate([s_g1, s_b1, s_ob, s_g2, s_b2, s_db], axis=0)
    nf = FH // 128
    for cc in range(C):
        tail = [jnp.concatenate([dqvs[cc * Hc + j][:, :E], dqvs[cc * Hc + j][:, 2 * E:3 * E]], axis=1) for j in range(Hc)]
        tail += [dubs[cc][:, j * 128:(j + 1) * 128] for j in range(nf)]
        tail = jnp.concatenate(tail, axis=0)
        for rr in range(R):
            sgs[cc, rr, 0:6, 0:rows] = six[:, rr * rows:(rr + 1) * rows]
            sgs[cc, rr, 6:6 + Hc + nf, 0:128] = tail
    sgc[c] = sgs[c]
    gc = [remote(sgs.at[col.up(k)], sgc.at[c], vsem.at[0, 3], vsem.at[1, 3], "col", col.up(k)) for k in col.ks()]
    for cp in gc:
        cp.start()
    step("last")
    settle_g(1, 0)
    s = sgc[0]
    for k in range(1, C):
        s = s + sgc[k]
    sgp[d] = s
    gp = [remote(sgp.at[d], sgp.at[d], vsem.at[0, 4], vsem.at[1, 4], "dp", dp.up(k)) for k in dp.ks()]
    for cp in gp:
        cp.start()
    step("end")
    settle_g(1, 1)
    s = sgp[0]
    for k in range(1, DP):
        s = s + sgp[k]
    sgz[...] = s
    sgr[r] = sgz[r]
    gz = [remote(sgz.at[row.up(k)], sgr.at[r], vsem.at[0, 5], vsem.at[1, 5], "row", row.up(k)) for k in row.ks()]
    for cp in gz:
        cp.start()

    outs = [y_cp, dx_cp]
    step("end2")
    for i in range(nc):
        redf[i].finish()
        outs.append(pltpu.make_async_copy(redf[i].fin, ff_o[i], osem.at[3 + i]))
        outs[-1].start()
    step("end3")
    settle_g(1, 2)
    s = sgr[0]
    for k in range(1, R):
        s = s + sgr[k]
    sgf[...] = s
    outs.append(pltpu.make_async_copy(sgf, sg_o, osem.at[2]))
    outs[-1].start()
    for j in range(Hc):
        redt[j].finish()
        outs.append(pltpu.make_async_copy(redt[j].fin, ft_o.at[j], osem.at[3 + nc + j]))
        outs[-1].start()
    for red in redf + redt:
        red.drain()
    for u in range(U):
        settle_z(0, u)
        settle_p(0, u)
        settle_c(0, u)
    settle_v(0)
    for stage in range(3):
        settle_g(0, stage)
    for cp in outs:
        cp.wait()


def finish_kernel(cfg, *refs):
    rows, Hc, E, nf, (sr, sl), chunks = cfg
    nc = len(chunks)
    (y_i, dx_i, ft_i, sg_i), ff_i, refs = refs[:4], refs[4:4 + nc], refs[4 + nc:]
    (y_o, dx_o, dg1_o, db1_o, daw_o, dqvb_o, dob_o, dg2_o, db2_o, dup_o, dub_o, ddn_o, ddb_o) = refs[:13]
    (ybuf, xbuf, ft, sg, wf, wt, isem, osem), ff = refs[13:21], refs[21:]
    n = ybuf.shape[0]
    small = [pltpu.make_async_copy(i, v, isem.at[2 * n + k]) for k, (i, v) in enumerate(((sg_i, sg), (ft_i, ft), *zip(ff_i, ff)))]
    ins = [pltpu.make_async_copy(dx_i.at[k], xbuf.at[k], isem.at[k]) for k in range(n)]
    ins += [pltpu.make_async_copy(y_i.at[k], ybuf.at[k], isem.at[n + k]) for k in range(n)]
    outs = [pltpu.make_async_copy(xbuf.at[k], dx_o.at[k], osem.at[k]) for k in range(n)]
    outs += [pltpu.make_async_copy(ybuf.at[k], y_o.at[k], osem.at[n + k]) for k in range(n)]
    for cp in small + ins:
        cp.start()
    small[0].wait()
    s = sg[...]
    for i, ref in enumerate([dg1_o, db1_o, dob_o, dg2_o, db2_o, ddb_o]):
        ref[...] = s[i:i + 1, :rows].reshape(rows)
    for j in range(nf):
        dub_o[pl.ds(j * 128, 128)] = s[6 + Hc + j:7 + Hc + j, :128].reshape(128)
    for j in range(Hc):
        dqvb_o[0:1, j * E:(j + 1) * E] = s[6 + j:7 + j, :E]
        dqvb_o[1:2, j * E:(j + 1) * E] = s[6 + j:7 + j, E:2 * E]

    def lay(src, a, ref, lo):
        pr, pw = src.shape[-2:]
        for qr in range(sr):
            for ql in range(sl):
                ref[pl.ds(qr * pr, pr), pl.ds(lo + ql * pw, pw)] = src[qr * sl + ql, a].astype(F32)

    small[1].wait()
    for j in range(Hc):
        lay(ft.at[j], 0, wt.at[j], 0)
    for i, (lo, w) in enumerate(chunks):
        small[2 + i].wait()
        for a in range(2):
            lay(ff[i], a, wf.at[a], lo)
    big = [pltpu.make_async_copy(b, o, osem.at[2 * n + k]) for k, (b, o) in enumerate(((wf.at[0], dup_o), (wf.at[1], ddn_o), (wt, daw_o)))]
    for o in big:
        o.start()
    outs += big
    for i, o in zip(ins, outs):
        i.wait()
        o.start()
    for o in outs:
        o.wait()


def pick_split(n, rows, widths):
    for sr in range(1, n + 1):
        if n % sr == 0 and rows % (16 * sr) == 0 and all(w % (128 * (n // sr)) == 0 for w in widths):
            return sr, n // sr
    return 1, 1


def local(sizes, x, g1, b1, aw, qvb, ob, g2, b2, up, ub, dn, db, c):
    DP, R, C = sizes
    NI, SEQ, D = x.shape
    Hc, rows, W4 = aw.shape
    E, FH = W4 // 4, up.shape[1]
    H, SP = C * Hc, -(-SEQ // 16) * 16
    T = NI * SP
    chunks = tuple((lo, 256) for lo in range(0, FH, 256)) if FH % 256 == 0 else ((0, FH),)
    nc, wmax = len(chunks), max(w for _, w in chunks)
    split = pick_split(DP, rows, (W4,) + tuple(w for _, w in chunks))
    np_ = split[0] * split[1]
    pr, pw = rows // split[0], W4 // split[1]
    sd, vm = jax.ShapeDtypeStruct, pltpu.VMEM
    dma = pltpu.SemaphoreType.DMA
    nf, VW = FH // 128, -(-rows // 128) * 128
    S = -(-(6 + Hc + nf) // 8) * 8
    cfg = (DP, R, C, NI, SEQ, SP, D, Hc, E, FH, rows, split, chunks)

    def red(A, L):
        pw = L // split[1]
        return [vm((C, np_, A, R, pr, pw), BF16), vm((max(C - 1, 1), np_, A, R, pr, pw), BF16), vm((DP, A, R, pr, pw), BF16),
                vm((R, A, pr, pw), BF16), vm((R, A, pr, pw), BF16), vm((np_, A, pr, pw), BF16)]

    scratch = sum([red(2, w) for _, w in chunks] + [red(1, W4)] * Hc, []) + [
        vm((H, D, W4), BF16), vm((C, D, FH), BF16), vm((C, D, FH), BF16), vm((R, 8, VW), F32),
        vm((C, 2, Hc * E), F32), vm((C, 1, FH), F32), vm((8, D), F32), vm((H, 1, W4), F32),
        vm((NI, SEQ, D), BF16), vm((NI, SEQ, D), BF16), vm((NI, SP, D), BF16), vm((NI, SP, D), F32), vm((NI, SP, 1), F32),
        vm((NI, SP, D), BF16), vm((H, NI, SP, W4), BF16), vm((H, NI, SP, SP), BF16), vm((NI, SP, D), BF16),
        vm((NI, SP, D), F32), vm((NI, SP, D), F32), vm((NI, SP, 1), F32), vm((NI, SP, D), BF16), vm((D, D), BF16),
        vm((D, 2 * D), BF16),
        vm((NI, SP, wmax), BF16), vm((NI, SP, wmax), BF16), vm((NI, SP, D), F32), vm((NI, SP, D), F32),
        vm((H, NI, SP, 2 * E), BF16), vm((D + 16, T), BF16), vm((D, T), BF16), vm((D + 16, T), BF16),
        vm((H, D, 2 * E), F32), vm((NI, SEQ, D), F32), vm((C, 1, FH), F32), vm((H, 1, W4), F32),
        vm((C, R, S, VW), F32), vm((C, R, S, VW), F32), vm((DP, R, S, VW), F32), vm((R, S, VW), F32),
        vm((R, S, VW), F32), vm((S, VW), F32),
        dma((5,)), dma((3 + nc + Hc,)), dma((2, 2, Hc + nc)), dma((2, Hc + 2 * nc, max(C - 1, 1))), dma((nc + Hc, 2, 5)), dma((2, 6)),
    ]
    any_ = pl.BlockSpec(memory_space=pl.ANY)
    vm_ = pl.BlockSpec(memory_space=pltpu.VMEM)
    v = lambda a: sd(a.shape, F32)
    y, dx, ft, sg, *ff = pl.pallas_call(
        functools.partial(kernel, cfg),
        out_shape=(sd(x.shape, BF16), v(x), sd((Hc, np_, 1, pr, pw), BF16), sd((S, VW), F32),
                   *[sd((np_, 2, pr, w // split[1]), BF16) for _, w in chunks]),
        in_specs=[any_, vm_, vm_, any_, vm_, vm_, vm_, vm_, any_, vm_, any_, vm_, any_],
        out_specs=[any_] * (4 + nc),
        scratch_shapes=scratch,
        compiler_params=pltpu.CompilerParams(vmem_limit_bytes=67043328, collective_id=0, has_side_effects=True),
    )(x, g1, b1, aw, qvb, ob, g2, b2, up, ub, dn, db, c)
    return tuple(pl.pallas_call(
        functools.partial(finish_kernel, (rows, Hc, E, nf, split, chunks)),
        out_shape=(sd(x.shape, BF16), v(x), v(g1), v(b1), v(aw), v(qvb), v(ob), v(g2), v(b2), v(up), v(ub), v(dn), v(db)),
        in_specs=[any_] * (4 + nc),
        out_specs=[any_, any_, vm_, vm_, any_, vm_, vm_, vm_, vm_, any_, vm_, any_, vm_],
        scratch_shapes=[vm(x.shape, BF16), vm(x.shape, F32), vm(ft.shape, BF16), vm(sg.shape, F32),
                        vm((2, rows, FH), F32), vm(aw.shape, F32), dma((2 * NI + 2 + nc,)), dma((2 * NI + 3,)),
                        *[vm(f.shape, BF16) for f in ff]],
        compiler_params=pltpu.CompilerParams(vmem_limit_bytes=67043328),
    )(y, dx, ft, sg, *ff))


def solution(mesh):
    sizes = tuple(mesh.shape[a] for a in ("dp", "row", "col"))
    placed = (
        P(("dp", "row", "col"), None, None),
        P("row"),
        P("row"),
        P("col", "row", None),
        P(None, "col"),
        P("row"),
        P("row"),
        P("row"),
        P("row", "col"),
        P("col"),
        P("row", "col"),
        P("row"),
        P(("dp", "row", "col"), None, None),
    )
    return jax.shard_map(
        functools.partial(local, sizes),
        mesh=mesh,
        in_specs=placed,
        out_specs=(
            P(("dp", "row", "col"), None, None),
            P(("dp", "row", "col"), None, None),
            P("row"),
            P("row"),
            P("col", "row", None),
            P(None, "col"),
            P("row"),
            P("row"),
            P("row"),
            P("row", "col"),
            P("col"),
            P("row", "col"),
            P("row"),
        ),
        check_vma=False,
    )
```

```python
import functools
import math

import jax
import jax.numpy as jnp
from jax import lax
from jax.experimental import pallas as pl
from jax.experimental.pallas import tpu as pltpu
from jax.sharding import PartitionSpec as P

EPS = 1e-06
ROOT_HALF = 0.7071067811865476
INV_ROOT_TWO_PI = 0.3989422804014327
LOG2E = 1.4426950408889634
F32, BF16 = jnp.float32, jnp.bfloat16
MESH = pl.DeviceIdType.MESH


def mm(a, b, ca, cb):
    return lax.dot_general(a, b, (((ca,), (cb,)), ((), ())), preferred_element_type=F32)


def norm_parts(v):
    mean = jnp.mean(v, -1, keepdims=True)
    cen = v - mean
    rstd = lax.rsqrt(jnp.mean(cen * cen, -1, keepdims=True) + EPS)
    return cen * rstd, rstd


def norm_back(g, gain, xhat, rstd):
    gx = g * gain
    return rstd * (gx - jnp.mean(gx, -1, keepdims=True) - xhat * jnp.mean(gx * xhat, -1, keepdims=True))


def gelu_parts(u):
    w = u * ROOT_HALF
    cdf = 0.5 + 0.5 * lax.erf(w)
    bell = jnp.exp2((w * w) * -LOG2E)
    return u * cdf, cdf + (w * bell) * (INV_ROOT_TWO_PI / ROOT_HALF)


DEEP = (3, 2, 3)


def loop(lo, hi, body, init):
    return lax.fori_loop(lo, hi, body, init)


def rsum(v):
    return jnp.sum(v, 0, keepdims=True)


def fold(v):
    t = v[:8]
    for lo in range(8, v.shape[0], 8):
        t = t + v[lo:lo + 8]
    return t


class Shift:
    def __init__(self, axis, n):
        self.axis, self.n, self.me = axis, n, lax.axis_index(axis)

    def up(self, k):
        return lax.rem(self.me + k, self.n)

    def down(self, k):
        return lax.rem(self.me + self.n - k, self.n)

    def ks(self):
        return range(1, self.n)


def remote(src, dst, ssem, rsem, axis, to):
    return pltpu.make_async_remote_copy(
        src_ref=src, dst_ref=dst, send_sem=ssem, recv_sem=rsem, device_id={axis: to}, device_id_type=MESH)


def settle(sem, region):
    pltpu.make_async_copy(region, region, sem).wait()


class Reduce:
    def __init__(self, cfg, ax, bufs, sems, halve):
        self.rows, self.split = cfg
        self.dp, self.row, self.col = ax
        (self.sb, self.rc, self.rp, self.sz, self.rz, self.fin) = bufs
        self.sems = sems
        self.np = self.fin.shape[0]
        self.halve = halve and self.np == 4
        self.own = self.col.n - 1

    def put(self, slot, a, v):
        sr, sl = self.split
        pr, pw = self.fin.shape[-2:]
        for r in range(self.row.n):
            for qr in range(sr):
                for ql in range(sl):
                    lo = r * self.rows + qr * pr
                    self.sb[slot, qr * sl + ql, a, r] = v[lo:lo + pr, ql * pw:(ql + 1) * pw].astype(BF16)

    def copy(self, src, dst, stage, ax, to):
        return remote(src, dst, self.sems.at[0, stage], self.sems.at[1, stage], ax.axis, to)

    def c(self, k):
        return self.copy(self.sb.at[k - 1], self.rc.at[k - 1], 0, self.col, self.col.up(k))

    def wait(self, side, stage):
        n, m = self.dp.n - 1, self.row.n - 1
        live = (self.own, n, self.halve, m, n and self.np > 1)[stage]
        if live:
            region = (lambda: self.rc, lambda: self.rp.at[0:2 if self.halve else n], lambda: self.rp.at[2],
                      lambda: self.rz.at[0:m], lambda: self.fin.at[0:n])[stage]
            settle(self.sems.at[side, stage], region())

    def halves(self, a):
        lo, hi = lax.rem(self.dp.me, 2), self.dp.me // 2
        if a % 2 == 0:
            return lo, hi, lambda x, y: x + 2 * y, self.dp.me + 1 - 2 * lo, self.dp.me + 2 - 4 * hi
        return hi, lo, lambda x, y: 2 * x + y, self.dp.me + 2 - 4 * hi, self.dp.me + 1 - 2 * lo

    def arrays(self):
        return range(self.fin.shape[1])

    def ps(self):
        if not self.halve:
            return [self.copy(self.sb.at[self.own, self.dp.up(k) if self.np > 1 else 0], self.rp.at[self.dp.me], 1,
                              self.dp, self.dp.up(k)) for k in self.dp.ks()]
        out = []
        for a in self.arrays():
            bit, _, at, to, _ = self.halves(a)
            for i in range(2):
                out.append(self.copy(self.sb.at[self.own, at(1 - bit, i), a], self.rp.at[i, a], 1, self.dp, to))
        return out

    def qs(self):
        out = []
        for a in self.arrays() if self.halve else ():
            bit, other, at, _, to = self.halves(a)
            out.append(self.copy(self.sb.at[self.own, at(bit, 1 - other), a], self.rp.at[2, a], 2, self.dp, to))
        return out

    def zs(self):
        return [self.copy(self.sz.at[self.row.up(k)], self.rz.at[self.row.me], 3, self.row, self.row.up(k))
                for k in self.row.ks()]

    def as_(self):
        if self.np == 1:
            return []
        mine = self.fin.at[self.dp.me]
        return [self.copy(mine, mine, 4, self.dp, self.dp.up(k)) for k in self.dp.ks()]

    def start_p(self):
        if self.own:
            self.wait(1, 0)
            t = self.sb[self.own].astype(F32)
            for k in self.col.ks():
                t = t + self.rc[k - 1].astype(F32)
            self.sb[self.own] = t.astype(BF16)
        if self.np == 1:
            self.rp[self.dp.me] = self.sb[self.own, 0]
        for cp in self.ps():
            cp.start()

    def start_q(self):
        if self.halve:
            self.wait(1, 1)
            for a in self.arrays():
                bit, other, at, _, _ = self.halves(a)
                q = at(bit, 1 - other)
                t = self.sb[self.own, q, a].astype(F32) + self.rp[1 - other, a].astype(F32)
                self.sb[self.own, q, a] = t.astype(BF16)
            for cp in self.qs():
                cp.start()

    def start_z(self):
        self.wait(1, 2 if self.halve else 1)
        for a in self.arrays():
            if self.halve:
                _, other, _, _, _ = self.halves(a)
                t = self.sb[self.own, self.dp.me, a].astype(F32) + self.rp[other, a].astype(F32) + self.rp[2, a].astype(F32)
            elif self.np > 1:
                t = self.sb[self.own, self.dp.me, a].astype(F32)
                for k in self.dp.ks():
                    t = t + self.rp[self.dp.up(k), a].astype(F32)
            else:
                t = self.rp[0, a].astype(F32)
                for q in range(1, self.dp.n):
                    t = t + self.rp[q, a].astype(F32)
            self.sz[:, a] = t.astype(BF16)
        for cp in self.zs():
            cp.start()

    def start_a(self):
        self.wait(1, 3)
        t = self.sz[self.row.me].astype(F32)
        for k in self.row.ks():
            t = t + self.rz[self.row.up(k)].astype(F32)
        self.fin[self.dp.me if self.np > 1 else 0] = t.astype(BF16)
        for cp in self.as_():
            cp.start()

    def finish(self):
        self.wait(1, 4)

    def drain(self):
        for stage in range(5):
            self.wait(0, stage)


def kernel(cfg, *refs):
    (DP, R, C, NI, SEQ, SP, D, Hc, E, FH, rows, split, chunks) = cfg
    (x_hbm, g1_h, b1_h, aw_h, qvb_h, ob_h, g2_h, b2_h, up_h, ub_h, dn_h, db_h, c_hbm) = refs[:13]
    nc = len(chunks)
    (y_o, dx_o, ft_o, sg_o), ff_o = refs[13:17], refs[17:17 + nc]
    refs = refs[17 + nc:]
    fbuf = [refs[6 * i:6 * i + 6] for i in range(nc)]
    tbuf = [refs[6 * (nc + j):6 * (nc + j) + 6] for j in range(Hc)]
    (wa, wup, wdn, vall, qvall, uball, vec, bias3, xin, cin, cb, xh1, rs1, a1, qkv, pt, o, h, xh2, rs2, a2, wot, wotp,
     gb, du, yacc, dacc, dout, a2t, ct, a1t, dwo, dxb, dubs, dqvs,
     sgs, sgc, sgp, sgz, sgr, sgf,
     lsem, osem, wsem, csem, rsem, vsem) = refs[6 * (nc + Hc):]
    H, T, W4 = C * Hc, NI * SP, 4 * E
    dp, row, col = Shift("dp", DP), Shift("row", R), Shift("col", C)
    d, r, c = dp.me, row.me, col.me
    sr, sl = split
    np_ = sr * sl
    part = np_ > 1

    loads = [pltpu.make_async_copy(x_hbm, xin, lsem.at[0]), pltpu.make_async_copy(c_hbm, cin, lsem.at[1])]
    own = pl.ds(pl.multiple_of(r * rows, rows), rows)
    heads = pl.ds(c * Hc, Hc)
    wloads = [pltpu.make_async_copy(aw_h, wa.at[heads, own, :], lsem.at[2]),
              pltpu.make_async_copy(up_h, wup.at[c, own, :], lsem.at[3]),
              pltpu.make_async_copy(dn_h, wdn.at[c, own, :], lsem.at[4])]
    for cp in loads + wloads:
        cp.start()
    for i, v in enumerate([g1_h, b1_h, ob_h, g2_h, b2_h, db_h]):
        vall[r, i:i + 1, 0:rows] = v[...].reshape(1, rows)
    qvall[c] = qvb_h[...]
    uball[c] = ub_h[...].reshape(1, FH)

    barrier = pltpu.get_barrier_semaphore()
    for ax in (dp, row, col):
        for k in ax.ks():
            pl.semaphore_signal(barrier, inc=1, device_id={ax.axis: ax.up(k)}, device_id_type=MESH)

    xh1[:, SP - 16:, :] = jnp.zeros((NI, 16, D), F32)
    h[:, SP - 16:, :] = jnp.zeros((NI, 16, D), F32)
    yacc[:, SP - 16:, :] = jnp.zeros((NI, 16, D), F32)
    rs1[:, SP - 16:, :] = jnp.zeros((NI, 16, 1), F32)
    sgs[...] = jnp.zeros(sgs.shape, F32)
    pl.semaphore_wait(barrier, (DP - 1) + (R - 1) + (C - 1))

    piece = d if part else 0
    off = lax.rem(c * Hc, 2)
    order = [lax.rem(off + e, Hc) for e in range(Hc)]
    units = [[(aw_h.at[j], wa.at[c * Hc + j])] for j in order]
    for lo, w in chunks:
        cut = (slice(None), pl.ds(lo, w))
        units.append([(up_h.at[cut], wup.at[(c,) + cut]), (dn_h.at[cut], wdn.at[(c,) + cut])])

    def cut_of(ref, rr, q):
        pr, pw = rows // sr, ref.shape[1] // sl
        return ref.at[pl.ds(pl.multiple_of(rr * rows + (q // sl) * pr, pr), pr),
                      pl.ds(pl.multiple_of(lax.rem(q, sl) * pw, pw), pw)]

    def gather_z(u):
        return [remote(cut_of(src, 0, piece), cut_of(dst, r, piece), wsem.at[0, 0, u], wsem.at[1, 0, u], "row", row.up(k))
                for src, dst in units[u] for k in row.ks()]

    def gather_p(u):
        out = []
        for _, dst in units[u] if part else ():
            for k in row.ks():
                b = cut_of(dst, row.down(k), piece)
                out += [remote(b, b, wsem.at[0, 1, u], wsem.at[1, 1, u], "dp", dp.up(kd)) for kd in dp.ks()]
        return out

    def gather_c(u):
        at = u if u < Hc else Hc + 2 * (u - Hc)
        return [remote(dst, dst, csem.at[0, at + i, k - 1], csem.at[1, at + i, k - 1], "col", col.up(k))
                for i, (_, dst) in enumerate(units[u]) for k in col.ks()]

    def settle_z(side, u):
        sb = (tbuf[u] if u < Hc else fbuf[u - Hc])[0]
        if R > 1:
            settle(wsem.at[side, 0, u], sb.at[0, 0, :, 0:R - 1])

    def settle_p(side, u):
        sb = (tbuf[u] if u < Hc else fbuf[u - Hc])[0]
        if R > 1 and part:
            settle(wsem.at[side, 1, u], sb.at[0, 0:DP - 1, :, 0:R - 1])

    def settle_c(side, u):
        for cp in gather_c(u):
            cp.wait_recv() if side else cp.wait_send()

    def begin(copies):
        for cp in copies:
            cp.start()

    U = Hc + nc
    for u in range(Hc):
        begin(gather_z(u))
    vz = [remote(vall.at[r], vall.at[r], vsem.at[0, 0], vsem.at[1, 0], "row", row.up(k)) for k in row.ks()]
    vc = [remote(qvall.at[c], qvall.at[c], vsem.at[0, 1], vsem.at[1, 1], "col", col.up(k)) for k in col.ks()]
    vc += [remote(uball.at[c], uball.at[c], vsem.at[0, 2], vsem.at[1, 2], "col", col.up(k)) for k in col.ks()]

    def settle_v(side):
        if R > 1:
            settle(vsem.at[side, 0], vall.at[0:R - 1])
        if C > 1:
            settle(vsem.at[side, 1], qvall.at[0:C - 1])
            settle(vsem.at[side, 2], uball.at[0:C - 1])

    def settle_g(side, stage):
        n, ref = ((C - 1, sgc), (DP - 1, sgp), (R - 1, sgr))[stage]
        if n:
            settle(vsem.at[side, 3 + stage], ref.at[0:n])

    begin(vz + vc)
    loads[0].wait()

    def norm1(i, carry):
        xf = xin[i].astype(F32)
        xh, rstd = norm_parts(xf)
        xh1[i, :SEQ] = xh
        rs1[i, :SEQ] = rstd
        h[i, :SEQ] = xf
        return carry

    loop(0, NI, norm1, 0)
    for u in range(Hc):
        settle_z(1, u)
        begin(gather_p(u))
    for u in range(Hc, U):
        begin(gather_z(u))
    loads[1].wait()

    def prep(i, carry):
        yacc[i, :SEQ] = cin[i].astype(F32)
        cb[i] = yacc[i].astype(BF16)
        return carry

    loop(0, NI, prep, 0)
    settle_v(1)
    vec[...] = jnp.concatenate([vall[rr][:, :rows] for rr in range(R)], axis=1)
    for hh in range(H):
        qb = qvall[hh // Hc][:, (hh % Hc) * E:(hh % Hc + 1) * E]
        zz = jnp.zeros((1, E), F32)
        bias3[hh] = jnp.concatenate([zz, qb[0:1], qb[1:2], zz], axis=1)

    def act1(i, carry):
        a1[i] = (xh1[i] * vec[0:1, :] + vec[1:2, :]).astype(BF16)
        return carry

    loop(0, NI, act1, 0)
    for cp in wloads:
        cp.wait()
    first = min(2, Hc)
    for u in range(first):
        settle_p(1, u)
        begin(gather_c(u))

    live = SEQ // 16 * 16
    key_ok = lax.broadcasted_iota(jnp.int32, (SP - live, SP), 0) < SEQ - live

    def logits(t):
        return mm(t[:, :E], t[:, E:2 * E], 1, 1)

    def attend(s, t):
        s = jnp.concatenate([s[:live], jnp.where(key_ok, s[live:], -1e30)], axis=0)
        top = jnp.max(s, 0, keepdims=True)
        e = jnp.exp2((s - top) * (LOG2E / math.sqrt(E)))
        return (e * (1.0 / rsum(e))).astype(BF16)

    def weigh(p, t):
        return mm(t[:, 2 * E:].T[:E], p, 1, 0)

    def fwd(it, carry):
        pr = lax.rem((c * Hc + 1) // 2 + it, H // 2)
        todo = [(i, j) for i in range(NI) for j in range(2)]
        N, ts, vts, ahead, probs, outs = len(todo), [], [], [], [], []

        def project(n):
            i, j = todo[n]
            w = wa[2 * pr + j]
            w = jnp.concatenate([w[:, E:2 * E], w[:, :E], w[:, 2 * E:]], axis=1)
            t = (mm(a1[i], w, 1, 0) + bias3[2 * pr + j]).astype(BF16)
            qkv[2 * pr + j, i] = t
            ts.append(t)
            vts.append(t[:, 2 * E:].T[:E])

        def out(n):
            i, j = todo[n]
            outs.append(mm(vts[n], probs[n], 1, 0))
            if j == 1:
                o[i, :, pl.ds(pl.multiple_of(pr * 2 * E, 2 * E), 2 * E)] = jnp.concatenate(outs[-2:], axis=0).astype(BF16).T

        for n in range(-DEEP[0], N + 1):
            if 0 <= n + DEEP[0] < N:
                project(n + DEEP[0])
            if 0 <= n + DEEP[1] < N:
                ahead.append(logits(ts[n + DEEP[1]]))
            if 0 <= n < N:
                probs.append(attend(ahead[n], ts[n]))
                pt[2 * pr + todo[n][1], todo[n][0]] = probs[n]
            if n >= 1:
                out(n - 1)
        return carry

    loop(0, 1, fwd, 0)
    for u in range(first, Hc):
        settle_p(1, u)
        begin(gather_c(u))
    for u in range(Hc, U):
        settle_z(1, u)
        begin(gather_p(u))
    ct[...] = cb[...].reshape(T, D).T
    a1t[:D] = a1[...].reshape(T, D).T
    a1t[D:] = jnp.ones((16, T), BF16)
    a2t[D:] = jnp.ones((16, T), BF16)
    for u in range(Hc):
        settle_c(1, u)
    loop(1, H // 2, fwd, 0)
    wot[...] = jnp.concatenate([wa[hh][:, 3 * E:] for hh in range(H)], axis=1)
    for hh in range(H):
        wotp[:, hh * 2 * E:(hh + 1) * 2 * E] = jnp.concatenate([wa[hh][:, 3 * E:], jnp.zeros((D, E), BF16)], axis=1)
    settle_p(1, Hc)
    begin(gather_c(Hc))

    G = 2 if NI % 2 == 0 else 1
    GT, B = G * SP, 16
    tiles = [(lo, min(B, SP - lo)) for lo in range(0, SP, B)]

    if True:
        ms = [mm(o[0], wot[...], 1, 1)]
        for i in range(NI):
            if i + 1 < NI:
                ms.append(mm(o[i + 1], wot[...], 1, 1))
            for lo, n in tiles:
                rs = slice(lo, lo + n)
                hid = h[i, rs] + ms[i][rs] + vec[2:3, :]
                h[i, rs] = hid
                xh, rstd = norm_parts(hid)
                xh2[i, rs] = xh
                rs2[i, rs] = rstd
                a2[i, rs] = (xh * vec[3:4, :] + vec[4:5, :]).astype(BF16)
                yacc[i, rs] = hid + vec[5:6, :]
    a2t[:D] = a2[...].reshape(T, D).T

    ax = (dp, row, col)
    redf = [Reduce((rows, split), ax, fbuf[i], rsem.at[i], True) for i in range(nc)]
    redt = [Reduce((rows, split), ax, tbuf[j], rsem.at[nc + j], False) for j in range(Hc)]

    plan = {("f", 2): [(0, "q")], "mid": [(1, "q"), (2, "p"), (0, "z")], (0, 1): [(1, "z")], (1, 0): [(2, "q")],
            (2, 0): [(0, "a")], (2, 1): [(2, "z"), (3, "z")], "last": [(4, "z"), (1, "a")],
            "end": [(5, "z"), (2, "a"), (3, "a")], "end2": [(4, "a")], "end3": [(5, "a")]}
    reds = redf + redt
    if (nc, Hc, C) != (3, 3, 2):
        plan = {"mid": [(nc - 1, "p")], "last": [(u, "q") for u in range(nc + Hc)] + [(u, "z") for u in range(nc + Hc)],
                "end": [(u, "a") for u in range(nc + Hc)]}

    def step(at):
        for u, what in plan.get(at, ()):
            getattr(reds[u], "start_" + what)()

    def ff(half, lo, w, first):
        w1, w2 = wup.at[half, :, lo:lo + w], wdn.at[half, :, lo:lo + w]
        bias = uball[half, :, lo:lo + w]

        halves = [(k, min(256, w - k)) for k in range(0, w, 256)]
        todo = [(slice(i, i + G), k, m) for i in range(0, NI, G) for k, m in halves]

        def dots(n):
            im, k, m = todo[n]
            return (mm(a2[im].reshape(GT, D), w1[:, k:k + m], 1, 0), mm(cb[im].reshape(GT, D), w2[:, k:k + m], 1, 0))

        def down(im):
            dd = mm(du[im, :, :w].reshape(GT, w), w1[...], 1, 1).reshape(G, SP, D)
            dacc[im] = dd if first else dacc[im] + dd

        if True:
            ahead = [dots(0)]
            for n, (im, k, m) in enumerate(todo):
                if n + 1 < len(todo):
                    ahead.append(dots(n + 1))
                u, dd = ahead[n]
                act, slope = gelu_parts(u + bias[:, k:k + m])
                gb[half, im, :, lo + k:lo + k + m] = act.astype(BF16).reshape(G, SP, m)
                du[im, :, k:k + m] = (dd * slope).astype(BF16).reshape(G, SP, m)
                if k == 0 and n:
                    down(todo[n - 1][0])
            down(todo[-1][0])
        gu = mm(a2t[...], du[:, :, :w].reshape(T, w), 1, 0)
        dubs[half, :, lo:lo + w] = gu[D:D + 1]
        return gu[:D], mm(ct[...], gb[half, :, :, lo:lo + w].reshape(T, w), 1, 0)

    for i, (lo, w) in enumerate(chunks):
        for a, v in enumerate(ff(c, lo, w, i == 0)):
            redf[i].put(C - 1, a, v)
        if i:
            redf[i - 1].start_p()
        step(("f", i))
        if i + 1 < nc:
            settle_p(1, Hc + i + 1)
            begin(gather_c(Hc + i + 1))
        settle_c(1, Hc + i)
        for k in col.ks():
            for a, v in enumerate(ff(col.up(k), lo, w, False)):
                redf[i].put(k - 1, a, v)
            redf[i].c(k).start()

    z = jnp.zeros((8, D), F32)
    def dout_of(i):
        dd = mm(a2[i], wotp[...], 1, 0).astype(BF16)
        for hh in range(H):
            dout[hh, i] = dd[:, hh * 2 * E:(hh + 1) * 2 * E]

    sums = [z, z, z, z]
    for i in range(NI):
        for lo, n in tiles:
            rs = slice(lo, lo + n)
            cf = cb[i, rs].astype(F32)
            da = dacc[i, rs]
            xh = xh2[i, rs]
            dh = cf + norm_back(da, vec[3:4, :], xh, rs2[i, rs])
            h[i, rs] = dh
            a2[i, rs] = dh.astype(BF16)
            sums = [t + fold(v) for t, v in zip(sums, (cf, da * xh, da, dh))]
        if i:
            dout_of(i - 1)
    dout_of(NI - 1)
    s_db, s_g2, s_b2, s_ob = (rsum(v) for v in sums)
    step("mid")
    ct[...] = a2[...].reshape(T, D).T
    dwo_all = mm(ct[...], o[...].reshape(T, D), 1, 0)
    for hh in range(H):
        dwo[hh] = jnp.concatenate([jnp.zeros((D, E), F32), dwo_all[:, hh * E:(hh + 1) * E]], axis=1)

    def back(hh):
        if True:
            def dprob(i):
                return mm(qkv[hh, i, :, 2 * E:] * (1.0 / math.sqrt(E)), dout[hh, i], 1, 1)

            def turned(i):
                return qkv[hh, i, :, :2 * E].T, dout[hh, i].T[:E]

            def grads(i, p, ds, kqt, dot):
                dq, dk, dv = mm(kqt[:E], ds, 1, 0), mm(kqt[E:], ds, 1, 1), mm(dot, p, 1, 1)
                qkv[hh, i, :, :2 * E] = jnp.concatenate([dq, dk], axis=0).astype(BF16).T
                qkv[hh, i, :, 2 * E:] = jnp.concatenate([dv, jnp.zeros((E, SP), F32)], axis=0).astype(BF16).T

            ahead, done = [], []
            for n in range(-DEEP[2], NI + 1):
                if 0 <= n + DEEP[2] < NI:
                    ahead.append((dprob(n + DEEP[2]), turned(n + DEEP[2])))
                if 0 <= n < NI:
                    dpr, ts = ahead[n]
                    p = pt[hh, n]
                    pf = p.astype(F32)
                    delta = rsum(pf * dpr)
                    done.append((n, p, (pf * (dpr - delta)).astype(BF16), *ts))
                if n >= 1:
                    grads(*done[n - 1])
        g = mm(a1t[...], qkv[hh].reshape(T, W4), 1, 0)
        dqvs[hh] = g[D:D + 1]
        return jnp.concatenate([g[:D, :2 * E], g[:D, 2 * E:] + dwo[hh]], axis=1)

    for j in range(Hc):
        def pair(s, carry):
            redt[j].put(s, 0, back(lax.rem(c + 1 + s, C) * Hc + j))

            @pl.when(s < C - 1)
            def _():
                redt[j].c(s + 1).start()
                step((j, 0))

            return carry

        lax.fori_loop(0, C, pair, 0)
        redt[j].start_p()
        step((j, 1))

    def da1(i):
        t = mm(qkv[0, i], wa[0], 1, 1)
        for hh in range(1, H):
            t = t + mm(qkv[hh, i], wa[hh], 1, 1)
        return t

    sums, ds = [z, z], [da1(0)]
    for i in range(NI):
        if i + 1 < NI:
            ds.append(da1(i + 1))
        for lo, n in tiles:
            rs = slice(lo, lo + n)
            da = ds[i][rs]
            xh = xh1[i, rs]
            dx = h[i, rs] + norm_back(da, vec[0:1, :], xh, rs1[i, rs])
            keep = min(n, SEQ - lo)
            dxb[i, lo:lo + keep] = dx[:keep]
            sums = [t + fold(v) for t, v in zip(sums, (da * xh, da))]
    s_g1, s_b1 = (rsum(v) for v in sums)
    dx_cp = pltpu.make_async_copy(dxb, dx_o, osem.at[1])
    dx_cp.start()

    six = jnp.concatenate([s_g1, s_b1, s_ob, s_g2, s_b2, s_db], axis=0)
    nf = FH // 128
    for cc in range(C):
        tail = [jnp.concatenate([dqvs[cc * Hc + j][:, :E], dqvs[cc * Hc + j][:, 2 * E:3 * E]], axis=1) for j in range(Hc)]
        tail += [dubs[cc][:, j * 128:(j + 1) * 128] for j in range(nf)]
        tail = jnp.concatenate(tail, axis=0)
        for rr in range(R):
            sgs[cc, rr, 0:6, 0:rows] = six[:, rr * rows:(rr + 1) * rows]
            sgs[cc, rr, 6:6 + Hc + nf, 0:128] = tail
    sgc[c] = sgs[c]
    gc = [remote(sgs.at[col.up(k)], sgc.at[c], vsem.at[0, 3], vsem.at[1, 3], "col", col.up(k)) for k in col.ks()]
    for cp in gc:
        cp.start()
    step("last")
    settle_g(1, 0)
    s = sgc[0]
    for k in range(1, C):
        s = s + sgc[k]
    sgz[...] = s
    sgr[r] = sgz[r]
    gz = [remote(sgz.at[row.up(k)], sgr.at[r], vsem.at[0, 5], vsem.at[1, 5], "row", row.up(k)) for k in row.ks()]
    for cp in gz:
        cp.start()
    step("end")
    for i in range(NI):
        t = yacc[i]
        for k in range(C):
            t = t + mm(gb[k, i], wdn[k], 1, 1)
        xin[i] = t[:SEQ].astype(BF16)
    y_cp = pltpu.make_async_copy(xin, y_o, osem.at[0])
    y_cp.start()
    settle_g(1, 2)
    s = sgr[0]
    for k in range(1, R):
        s = s + sgr[k]
    sgp[d] = s
    gp = [remote(sgp.at[d], sgp.at[d], vsem.at[0, 4], vsem.at[1, 4], "dp", dp.up(k)) for k in dp.ks()]
    for cp in gp:
        cp.start()

    outs = [y_cp, dx_cp]
    step("end2")
    for i in range(nc):
        redf[i].finish()
        outs.append(pltpu.make_async_copy(redf[i].fin, ff_o[i], osem.at[3 + i]))
        outs[-1].start()
    step("end3")
    settle_g(1, 1)
    s = sgp[0]
    for k in range(1, DP):
        s = s + sgp[k]
    sgf[...] = s
    outs.append(pltpu.make_async_copy(sgf, sg_o, osem.at[2]))
    outs[-1].start()
    for j in range(Hc):
        redt[j].finish()
        outs.append(pltpu.make_async_copy(redt[j].fin, ft_o.at[j], osem.at[3 + nc + j]))
        outs[-1].start()
    for red in redf + redt:
        red.drain()
    for u in range(U):
        settle_z(0, u)
        settle_p(0, u)
        settle_c(0, u)
    settle_v(0)
    for stage in range(3):
        settle_g(0, stage)
    for cp in outs:
        cp.wait()


def finish_kernel(cfg, *refs):
    rows, Hc, E, nf, (sr, sl), chunks = cfg
    nc = len(chunks)
    (y_i, dx_i, ft_i, sg_i), ff_i, refs = refs[:4], refs[4:4 + nc], refs[4 + nc:]
    (y_o, dx_o, dg1_o, db1_o, daw_o, dqvb_o, dob_o, dg2_o, db2_o, dup_o, dub_o, ddn_o, ddb_o) = refs[:13]
    (ybuf, xbuf, ft, sg, wf, wt, isem, osem), ff = refs[13:21], refs[21:]
    n = ybuf.shape[0]
    small = [pltpu.make_async_copy(i, v, isem.at[2 * n + k]) for k, (i, v) in enumerate(((sg_i, sg), (ft_i, ft), *zip(ff_i, ff)))]
    ins = [pltpu.make_async_copy(dx_i.at[k], xbuf.at[k], isem.at[k]) for k in range(n)]
    ins += [pltpu.make_async_copy(y_i.at[k], ybuf.at[k], isem.at[n + k]) for k in range(n)]
    outs = [pltpu.make_async_copy(xbuf.at[k], dx_o.at[k], osem.at[k]) for k in range(n)]
    outs += [pltpu.make_async_copy(ybuf.at[k], y_o.at[k], osem.at[n + k]) for k in range(n)]
    for cp in small + ins:
        cp.start()
    small[0].wait()
    s = sg[...]
    for i, ref in enumerate([dg1_o, db1_o, dob_o, dg2_o, db2_o, ddb_o]):
        ref[...] = s[i:i + 1, :rows].reshape(rows)
    for j in range(nf):
        dub_o[pl.ds(j * 128, 128)] = s[6 + Hc + j:7 + Hc + j, :128].reshape(128)
    for j in range(Hc):
        dqvb_o[0:1, j * E:(j + 1) * E] = s[6 + j:7 + j, :E]
        dqvb_o[1:2, j * E:(j + 1) * E] = s[6 + j:7 + j, E:2 * E]

    def lay(src, a, ref, lo):
        pr, pw = src.shape[-2:]
        for qr in range(sr):
            for ql in range(sl):
                ref[pl.ds(qr * pr, pr), pl.ds(lo + ql * pw, pw)] = src[qr * sl + ql, a].astype(F32)

    small[1].wait()
    for j in range(Hc):
        lay(ft.at[j], 0, wt.at[j], 0)
    for i, (lo, w) in enumerate(chunks):
        small[2 + i].wait()
        for a in range(2):
            lay(ff[i], a, wf.at[a], lo)
    big = [pltpu.make_async_copy(b, o, osem.at[2 * n + k]) for k, (b, o) in enumerate(((wf.at[0], dup_o), (wf.at[1], ddn_o), (wt, daw_o)))]
    for o in big:
        o.start()
    outs += big
    for i, o in zip(ins, outs):
        i.wait()
        o.start()
    for o in outs:
        o.wait()


def pick_split(n, rows, widths):
    for sr in range(1, n + 1):
        if n % sr == 0 and rows % (16 * sr) == 0 and all(w % (128 * (n // sr)) == 0 for w in widths):
            return sr, n // sr
    return 1, 1


def local(sizes, x, g1, b1, aw, qvb, ob, g2, b2, up, ub, dn, db, c):
    DP, R, C = sizes
    NI, SEQ, D = x.shape
    Hc, rows, W4 = aw.shape
    E, FH = W4 // 4, up.shape[1]
    H, SP = C * Hc, -(-SEQ // 16) * 16
    T = NI * SP
    chunks = tuple((lo, 256) for lo in range(0, FH, 256)) if FH % 256 == 0 else ((0, FH),)
    nc, wmax = len(chunks), max(w for _, w in chunks)
    split = pick_split(DP, rows, (W4,) + tuple(w for _, w in chunks))
    np_ = split[0] * split[1]
    pr, pw = rows // split[0], W4 // split[1]
    sd, vm = jax.ShapeDtypeStruct, pltpu.VMEM
    dma = pltpu.SemaphoreType.DMA
    nf, VW = FH // 128, -(-rows // 128) * 128
    S = -(-(6 + Hc + nf) // 8) * 8
    cfg = (DP, R, C, NI, SEQ, SP, D, Hc, E, FH, rows, split, chunks)

    def red(A, L):
        pw = L // split[1]
        return [vm((C, np_, A, R, pr, pw), BF16), vm((max(C - 1, 1), np_, A, R, pr, pw), BF16), vm((DP, A, R, pr, pw), BF16),
                vm((R, A, pr, pw), BF16), vm((R, A, pr, pw), BF16), vm((np_, A, pr, pw), BF16)]

    scratch = sum([red(2, w) for _, w in chunks] + [red(1, W4)] * Hc, []) + [
        vm((H, D, W4), BF16), vm((C, D, FH), BF16), vm((C, D, FH), BF16), vm((R, 8, VW), F32),
        vm((C, 2, Hc * E), F32), vm((C, 1, FH), F32), vm((8, D), F32), vm((H, 1, W4), F32),
        vm((NI, SEQ, D), BF16), vm((NI, SEQ, D), BF16), vm((NI, SP, D), BF16), vm((NI, SP, D), F32), vm((NI, SP, 1), F32),
        vm((NI, SP, D), BF16), vm((H, NI, SP, W4), BF16), vm((H, NI, SP, SP), BF16), vm((NI, SP, D), BF16),
        vm((NI, SP, D), F32), vm((NI, SP, D), F32), vm((NI, SP, 1), F32), vm((NI, SP, D), BF16), vm((D, D), BF16),
        vm((D, 2 * D), BF16),
        vm((C, NI, SP, FH), BF16), vm((NI, SP, wmax), BF16), vm((NI, SP, D), F32), vm((NI, SP, D), F32),
        vm((H, NI, SP, 2 * E), BF16), vm((D + 16, T), BF16), vm((D, T), BF16), vm((D + 16, T), BF16),
        vm((H, D, 2 * E), F32), vm((NI, SEQ, D), F32), vm((C, 1, FH), F32), vm((H, 1, W4), F32),
        vm((C, R, S, VW), F32), vm((C, R, S, VW), F32), vm((DP, S, VW), F32), vm((R, S, VW), F32),
        vm((R, S, VW), F32), vm((S, VW), F32),
        dma((5,)), dma((3 + nc + Hc,)), dma((2, 2, Hc + nc)), dma((2, Hc + 2 * nc, max(C - 1, 1))), dma((nc + Hc, 2, 5)), dma((2, 6)),
    ]
    any_ = pl.BlockSpec(memory_space=pl.ANY)
    vm_ = pl.BlockSpec(memory_space=pltpu.VMEM)
    v = lambda a: sd(a.shape, F32)
    y, dx, ft, sg, *ff = pl.pallas_call(
        functools.partial(kernel, cfg),
        out_shape=(sd(x.shape, BF16), v(x), sd((Hc, np_, 1, pr, pw), BF16), sd((S, VW), F32),
                   *[sd((np_, 2, pr, w // split[1]), BF16) for _, w in chunks]),
        in_specs=[any_, vm_, vm_, any_, vm_, vm_, vm_, vm_, any_, vm_, any_, vm_, any_],
        out_specs=[any_] * (4 + nc),
        scratch_shapes=scratch,
        compiler_params=pltpu.CompilerParams(vmem_limit_bytes=67043328, collective_id=0, has_side_effects=True),
    )(x, g1, b1, aw, qvb, ob, g2, b2, up, ub, dn, db, c)
    return tuple(pl.pallas_call(
        functools.partial(finish_kernel, (rows, Hc, E, nf, split, chunks)),
        out_shape=(sd(x.shape, BF16), v(x), v(g1), v(b1), v(aw), v(qvb), v(ob), v(g2), v(b2), v(up), v(ub), v(dn), v(db)),
        in_specs=[any_] * (4 + nc),
        out_specs=[any_, any_, vm_, vm_, any_, vm_, vm_, vm_, vm_, any_, vm_, any_, vm_],
        scratch_shapes=[vm(x.shape, BF16), vm(x.shape, F32), vm(ft.shape, BF16), vm(sg.shape, F32),
                        vm((2, rows, FH), F32), vm(aw.shape, F32), dma((2 * NI + 2 + nc,)), dma((2 * NI + 3,)),
                        *[vm(f.shape, BF16) for f in ff]],
        compiler_params=pltpu.CompilerParams(vmem_limit_bytes=67043328),
    )(y, dx, ft, sg, *ff))


def solution(mesh):
    sizes = tuple(mesh.shape[a] for a in ("dp", "row", "col"))
    placed = (
        P(("dp", "row", "col"), None, None),
        P("row"),
        P("row"),
        P("col", "row", None),
        P(None, "col"),
        P("row"),
        P("row"),
        P("row"),
        P("row", "col"),
        P("col"),
        P("row", "col"),
        P("row"),
        P(("dp", "row", "col"), None, None),
    )
    return jax.shard_map(
        functools.partial(local, sizes),
        mesh=mesh,
        in_specs=placed,
        out_specs=(
            P(("dp", "row", "col"), None, None),
            P(("dp", "row", "col"), None, None),
            P("row"),
            P("row"),
            P("col", "row", None),
            P(None, "col"),
            P("row"),
            P("row"),
            P("row"),
            P("row", "col"),
            P("col"),
            P("row", "col"),
            P("row"),
        ),
        check_vma=False,
    )
```

```python
import functools
import math

import jax
import jax.numpy as jnp
from jax import lax
from jax.experimental import pallas as pl
from jax.experimental.pallas import tpu as pltpu
from jax.sharding import PartitionSpec as P

EPS = 1e-06
ROOT_HALF = 0.7071067811865476
INV_ROOT_TWO_PI = 0.3989422804014327
LOG2E = 1.4426950408889634
F32, BF16 = jnp.float32, jnp.bfloat16
MESH = pl.DeviceIdType.MESH


def mm(a, b, ca, cb):
    return lax.dot_general(a, b, (((ca,), (cb,)), ((), ())), preferred_element_type=F32)


def norm_parts(v):
    mean = jnp.mean(v, -1, keepdims=True)
    cen = v - mean
    rstd = lax.rsqrt(jnp.mean(cen * cen, -1, keepdims=True) + EPS)
    return cen * rstd, rstd


def norm_back(g, gain, xhat, rstd):
    gx = g * gain
    return rstd * (gx - jnp.mean(gx, -1, keepdims=True) - xhat * jnp.mean(gx * xhat, -1, keepdims=True))


def gelu_parts(u):
    w = u * ROOT_HALF
    cdf = 0.5 + 0.5 * lax.erf(w)
    bell = jnp.exp2((w * w) * -LOG2E)
    return u * cdf, cdf + (w * bell) * (INV_ROOT_TWO_PI / ROOT_HALF)


DEEP = (3, 2, 3)


def loop(lo, hi, body, init):
    return lax.fori_loop(lo, hi, body, init)


def rsum(v):
    return jnp.sum(v, 0, keepdims=True)


def fold(v):
    t = v[:8]
    for lo in range(8, v.shape[0], 8):
        t = t + v[lo:lo + 8]
    return t


class Shift:
    def __init__(self, axis, n):
        self.axis, self.n, self.me = axis, n, lax.axis_index(axis)

    def up(self, k):
        return lax.rem(self.me + k, self.n)

    def down(self, k):
        return lax.rem(self.me + self.n - k, self.n)

    def ks(self):
        return range(1, self.n)


def remote(src, dst, ssem, rsem, axis, to):
    return pltpu.make_async_remote_copy(
        src_ref=src, dst_ref=dst, send_sem=ssem, recv_sem=rsem, device_id={axis: to}, device_id_type=MESH)


def settle(sem, region):
    pltpu.make_async_copy(region, region, sem).wait()


class Reduce:
    def __init__(self, cfg, ax, bufs, sems, halve):
        self.rows, self.split = cfg
        self.dp, self.row, self.col = ax
        (self.sb, self.rc, self.rp, self.sz, self.rz, self.fin) = bufs
        self.sems = sems
        self.np = self.fin.shape[0]
        self.halve = halve and self.np == 4
        self.own = self.col.n - 1

    def put(self, slot, a, v):
        sr, sl = self.split
        pr, pw = self.fin.shape[-2:]
        for r in range(self.row.n):
            for qr in range(sr):
                for ql in range(sl):
                    lo = r * self.rows + qr * pr
                    self.sb[slot, qr * sl + ql, a, r] = v[lo:lo + pr, ql * pw:(ql + 1) * pw].astype(BF16)

    def copy(self, src, dst, stage, ax, to):
        return remote(src, dst, self.sems.at[0, stage], self.sems.at[1, stage], ax.axis, to)

    def c(self, k):
        return self.copy(self.sb.at[k - 1], self.rc.at[k - 1], 0, self.col, self.col.up(k))

    def wait(self, side, stage):
        n, m = self.dp.n - 1, self.row.n - 1
        live = (self.own, n, self.halve, m, n and self.np > 1)[stage]
        if live:
            region = (lambda: self.rc, lambda: self.rp.at[0:2 if self.halve else n], lambda: self.rp.at[2],
                      lambda: self.rz.at[0:m], lambda: self.fin.at[0:n])[stage]
            settle(self.sems.at[side, stage], region())

    def halves(self, a):
        lo, hi = lax.rem(self.dp.me, 2), self.dp.me // 2
        if a % 2 == 0:
            return lo, hi, lambda x, y: x + 2 * y, self.dp.me + 1 - 2 * lo, self.dp.me + 2 - 4 * hi
        return hi, lo, lambda x, y: 2 * x + y, self.dp.me + 2 - 4 * hi, self.dp.me + 1 - 2 * lo

    def arrays(self):
        return range(self.fin.shape[1])

    def ps(self):
        if not self.halve:
            return [self.copy(self.sb.at[self.own, self.dp.up(k) if self.np > 1 else 0], self.rp.at[self.dp.me], 1,
                              self.dp, self.dp.up(k)) for k in self.dp.ks()]
        out = []
        for a in self.arrays():
            bit, _, at, to, _ = self.halves(a)
            for i in range(2):
                out.append(self.copy(self.sb.at[self.own, at(1 - bit, i), a], self.rp.at[i, a], 1, self.dp, to))
        return out

    def qs(self):
        out = []
        for a in self.arrays() if self.halve else ():
            bit, other, at, _, to = self.halves(a)
            out.append(self.copy(self.sb.at[self.own, at(bit, 1 - other), a], self.rp.at[2, a], 2, self.dp, to))
        return out

    def zs(self):
        return [self.copy(self.sz.at[self.row.up(k)], self.rz.at[self.row.me], 3, self.row, self.row.up(k))
                for k in self.row.ks()]

    def as_(self):
        if self.np == 1:
            return []
        mine = self.fin.at[self.dp.me]
        return [self.copy(mine, mine, 4, self.dp, self.dp.up(k)) for k in self.dp.ks()]

    def start_p(self):
        if self.own:
            self.wait(1, 0)
            t = self.sb[self.own].astype(F32)
            for k in self.col.ks():
                t = t + self.rc[k - 1].astype(F32)
            self.sb[self.own] = t.astype(BF16)
        if self.np == 1:
            self.rp[self.dp.me] = self.sb[self.own, 0]
        for cp in self.ps():
            cp.start()

    def start_q(self):
        if self.halve:
            self.wait(1, 1)
            for a in self.arrays():
                bit, other, at, _, _ = self.halves(a)
                q = at(bit, 1 - other)
                t = self.sb[self.own, q, a].astype(F32) + self.rp[1 - other, a].astype(F32)
                self.sb[self.own, q, a] = t.astype(BF16)
            for cp in self.qs():
                cp.start()

    def start_z(self):
        self.wait(1, 2 if self.halve else 1)
        for a in self.arrays():
            if self.halve:
                _, other, _, _, _ = self.halves(a)
                t = self.sb[self.own, self.dp.me, a].astype(F32) + self.rp[other, a].astype(F32) + self.rp[2, a].astype(F32)
            elif self.np > 1:
                t = self.sb[self.own, self.dp.me, a].astype(F32)
                for k in self.dp.ks():
                    t = t + self.rp[self.dp.up(k), a].astype(F32)
            else:
                t = self.rp[0, a].astype(F32)
                for q in range(1, self.dp.n):
                    t = t + self.rp[q, a].astype(F32)
            self.sz[:, a] = t.astype(BF16)
        for cp in self.zs():
            cp.start()

    def start_a(self):
        self.wait(1, 3)
        t = self.sz[self.row.me].astype(F32)
        for k in self.row.ks():
            t = t + self.rz[self.row.up(k)].astype(F32)
        self.fin[self.dp.me if self.np > 1 else 0] = t.astype(BF16)
        for cp in self.as_():
            cp.start()

    def finish(self):
        self.wait(1, 4)

    def drain(self):
        for stage in range(5):
            self.wait(0, stage)


def kernel(cfg, *refs):
    (DP, R, C, NI, SEQ, SP, D, Hc, E, FH, rows, split, chunks) = cfg
    (x_hbm, g1_h, b1_h, aw_h, qvb_h, ob_h, g2_h, b2_h, up_h, ub_h, dn_h, db_h, c_hbm) = refs[:13]
    nc = len(chunks)
    (y_o, dx_o, ft_o, sg_o), ff_o = refs[13:17], refs[17:17 + nc]
    refs = refs[17 + nc:]
    fbuf = [refs[6 * i:6 * i + 6] for i in range(nc)]
    tbuf = [refs[6 * (nc + j):6 * (nc + j) + 6] for j in range(Hc)]
    (wa, wup, wdn, vall, qvall, uball, vec, bias3, xin, cin, cb, xh1, rs1, a1, qkv, pt, o, h, xh2, rs2, a2, wot, wotp,
     gb, du, yacc, dacc, dout, a2t, ct, a1t, dwo, dxb, dubs, dqvs,
     sgs, sgc, sgp, sgz, sgr, sgf,
     lsem, osem, wsem, csem, rsem, vsem) = refs[6 * (nc + Hc):]
    H, T, W4 = C * Hc, NI * SP, 4 * E
    dp, row, col = Shift("dp", DP), Shift("row", R), Shift("col", C)
    d, r, c = dp.me, row.me, col.me
    sr, sl = split
    np_ = sr * sl
    part = np_ > 1

    loads = [pltpu.make_async_copy(x_hbm, xin, lsem.at[0]), pltpu.make_async_copy(c_hbm, cin, lsem.at[1])]
    own = pl.ds(pl.multiple_of(r * rows, rows), rows)
    heads = pl.ds(c * Hc, Hc)
    wloads = [pltpu.make_async_copy(aw_h, wa.at[heads, own, :], lsem.at[2]),
              pltpu.make_async_copy(up_h, wup.at[c, own, :], lsem.at[3]),
              pltpu.make_async_copy(dn_h, wdn.at[c, own, :], lsem.at[4])]
    for cp in loads + wloads:
        cp.start()
    for i, v in enumerate([g1_h, b1_h, ob_h, g2_h, b2_h, db_h]):
        vall[r, i:i + 1, 0:rows] = v[...].reshape(1, rows)
    qvall[c] = qvb_h[...]
    uball[c] = ub_h[...].reshape(1, FH)

    barrier = pltpu.get_barrier_semaphore()
    for ax in (dp, row, col):
        for k in ax.ks():
            pl.semaphore_signal(barrier, inc=1, device_id={ax.axis: ax.up(k)}, device_id_type=MESH)

    xh1[:, SP - 16:, :] = jnp.zeros((NI, 16, D), F32)
    h[:, SP - 16:, :] = jnp.zeros((NI, 16, D), F32)
    yacc[:, SP - 16:, :] = jnp.zeros((NI, 16, D), F32)
    rs1[:, SP - 16:, :] = jnp.zeros((NI, 16, 1), F32)
    sgs[...] = jnp.zeros(sgs.shape, F32)
    pl.semaphore_wait(barrier, (DP - 1) + (R - 1) + (C - 1))

    piece = d if part else 0
    off = lax.rem(c * Hc, 2)
    order = [lax.rem(off + e, Hc) for e in range(Hc)]
    units = [[(aw_h.at[j], wa.at[c * Hc + j])] for j in order]
    for lo, w in chunks:
        cut = (slice(None), pl.ds(lo, w))
        units.append([(up_h.at[cut], wup.at[(c,) + cut]), (dn_h.at[cut], wdn.at[(c,) + cut])])

    def cut_of(ref, rr, q):
        pr, pw = rows // sr, ref.shape[1] // sl
        return ref.at[pl.ds(pl.multiple_of(rr * rows + (q // sl) * pr, pr), pr),
                      pl.ds(pl.multiple_of(lax.rem(q, sl) * pw, pw), pw)]

    def gather_z(u):
        return [remote(cut_of(src, 0, piece), cut_of(dst, r, piece), wsem.at[0, 0, u], wsem.at[1, 0, u], "row", row.up(k))
                for src, dst in units[u] for k in row.ks()]

    def gather_p(u):
        out = []
        for _, dst in units[u] if part else ():
            for k in row.ks():
                b = cut_of(dst, row.down(k), piece)
                out += [remote(b, b, wsem.at[0, 1, u], wsem.at[1, 1, u], "dp", dp.up(kd)) for kd in dp.ks()]
        return out

    def gather_c(u):
        at = u if u < Hc else Hc + 2 * (u - Hc)
        return [remote(dst, dst, csem.at[0, at + i, k - 1], csem.at[1, at + i, k - 1], "col", col.up(k))
                for i, (_, dst) in enumerate(units[u]) for k in col.ks()]

    def settle_z(side, u):
        sb = (tbuf[u] if u < Hc else fbuf[u - Hc])[0]
        if R > 1:
            settle(wsem.at[side, 0, u], sb.at[0, 0, :, 0:R - 1])

    def settle_p(side, u):
        sb = (tbuf[u] if u < Hc else fbuf[u - Hc])[0]
        if R > 1 and part:
            settle(wsem.at[side, 1, u], sb.at[0, 0:DP - 1, :, 0:R - 1])

    def settle_c(side, u):
        for cp in gather_c(u):
            cp.wait_recv() if side else cp.wait_send()

    def begin(copies):
        for cp in copies:
            cp.start()

    U = Hc + nc
    for u in range(Hc):
        begin(gather_z(u))
    vz = [remote(vall.at[r], vall.at[r], vsem.at[0, 0], vsem.at[1, 0], "row", row.up(k)) for k in row.ks()]
    vc = [remote(qvall.at[c], qvall.at[c], vsem.at[0, 1], vsem.at[1, 1], "col", col.up(k)) for k in col.ks()]
    vc += [remote(uball.at[c], uball.at[c], vsem.at[0, 2], vsem.at[1, 2], "col", col.up(k)) for k in col.ks()]

    def settle_v(side):
        if R > 1:
            settle(vsem.at[side, 0], vall.at[0:R - 1])
        if C > 1:
            settle(vsem.at[side, 1], qvall.at[0:C - 1])
            settle(vsem.at[side, 2], uball.at[0:C - 1])

    def settle_g(side, stage):
        n, ref = ((C - 1, sgc), (DP - 1, sgp), (R - 1, sgr))[stage]
        if n:
            settle(vsem.at[side, 3 + stage], ref.at[0:n])

    begin(vz + vc)
    loads[0].wait()

    def norm1(i, carry):
        xf = xin[i].astype(F32)
        xh, rstd = norm_parts(xf)
        xh1[i, :SEQ] = xh
        rs1[i, :SEQ] = rstd
        h[i, :SEQ] = xf
        return carry

    loop(0, NI, norm1, 0)
    for u in range(Hc):
        settle_z(1, u)
        begin(gather_p(u))
    for u in range(Hc, U):
        begin(gather_z(u))
    loads[1].wait()

    def prep(i, carry):
        yacc[i, :SEQ] = cin[i].astype(F32)
        cb[i] = yacc[i].astype(BF16)
        return carry

    loop(0, NI, prep, 0)
    settle_v(1)
    vec[...] = jnp.concatenate([vall[rr][:, :rows] for rr in range(R)], axis=1)
    for hh in range(H):
        qb = qvall[hh // Hc][:, (hh % Hc) * E:(hh % Hc + 1) * E]
        zz = jnp.zeros((1, E), F32)
        bias3[hh] = jnp.concatenate([zz, qb[0:1], qb[1:2], zz], axis=1)

    def act1(i, carry):
        a1[i] = (xh1[i] * vec[0:1, :] + vec[1:2, :]).astype(BF16)
        return carry

    loop(0, NI, act1, 0)
    for cp in wloads:
        cp.wait()
    first = min(2, Hc)
    for u in range(first):
        settle_p(1, u)
        begin(gather_c(u))

    live = SEQ // 16 * 16
    key_ok = lax.broadcasted_iota(jnp.int32, (SP - live, SP), 0) < SEQ - live

    def logits(t):
        return mm(t[:, :E], t[:, E:2 * E], 1, 1)

    def attend(s, t):
        s = jnp.concatenate([s[:live], jnp.where(key_ok, s[live:], -1e30)], axis=0)
        top = jnp.max(s, 0, keepdims=True)
        e = jnp.exp2((s - top) * (LOG2E / math.sqrt(E)))
        return (e * (1.0 / rsum(e))).astype(BF16)

    def weigh(p, t):
        return mm(t[:, 2 * E:].T[:E], p, 1, 0)

    def fwd(it, carry):
        pr = lax.rem((c * Hc + 1) // 2 + it, H // 2)
        todo = [(i, j) for i in range(NI) for j in range(2)]
        N, ts, vts, ahead, probs, outs = len(todo), [], [], [], [], []

        def project(n):
            i, j = todo[n]
            w = wa[2 * pr + j]
            w = jnp.concatenate([w[:, E:2 * E], w[:, :E], w[:, 2 * E:]], axis=1)
            t = (mm(a1[i], w, 1, 0) + bias3[2 * pr + j]).astype(BF16)
            qkv[2 * pr + j, i] = t
            ts.append(t)
            vts.append(t[:, 2 * E:].T[:E])

        def out(n):
            i, j = todo[n]
            outs.append(mm(vts[n], probs[n], 1, 0))
            if j == 1:
                o[i, :, pl.ds(pl.multiple_of(pr * 2 * E, 2 * E), 2 * E)] = jnp.concatenate(outs[-2:], axis=0).astype(BF16).T

        for n in range(-DEEP[0], N + 1):
            if 0 <= n + DEEP[0] < N:
                project(n + DEEP[0])
            if 0 <= n + DEEP[1] < N:
                ahead.append(logits(ts[n + DEEP[1]]))
            if 0 <= n < N:
                probs.append(attend(ahead[n], ts[n]))
                pt[2 * pr + todo[n][1], todo[n][0]] = probs[n]
            if n >= 1:
                out(n - 1)
        return carry

    loop(0, 1, fwd, 0)
    for u in range(first, Hc):
        settle_p(1, u)
        begin(gather_c(u))
    for u in range(Hc, U):
        settle_z(1, u)
        begin(gather_p(u))
    ct[...] = cb[...].reshape(T, D).T
    a1t[:D] = a1[...].reshape(T, D).T
    a1t[D:] = jnp.ones((16, T), BF16)
    a2t[D:] = jnp.ones((16, T), BF16)
    for u in range(Hc):
        settle_c(1, u)
    loop(1, H // 2, fwd, 0)
    wot[...] = jnp.concatenate([wa[hh][:, 3 * E:] for hh in range(H)], axis=1)
    for hh in range(H):
        wotp[:, hh * 2 * E:(hh + 1) * 2 * E] = jnp.concatenate([wa[hh][:, 3 * E:], jnp.zeros((D, E), BF16)], axis=1)
    settle_p(1, Hc)
    begin(gather_c(Hc))

    G = 2 if NI % 2 == 0 else 1
    GT, B = G * SP, 16
    tiles = [(lo, min(B, SP - lo)) for lo in range(0, SP, B)]

    if True:
        ms = [mm(o[0], wot[...], 1, 1)]
        for i in range(NI):
            if i + 1 < NI:
                ms.append(mm(o[i + 1], wot[...], 1, 1))
            for lo, n in tiles:
                rs = slice(lo, lo + n)
                hid = h[i, rs] + ms[i][rs] + vec[2:3, :]
                h[i, rs] = hid
                xh, rstd = norm_parts(hid)
                xh2[i, rs] = xh
                rs2[i, rs] = rstd
                a2[i, rs] = (xh * vec[3:4, :] + vec[4:5, :]).astype(BF16)
                yacc[i, rs] = hid + vec[5:6, :]
    a2t[:D] = a2[...].reshape(T, D).T

    ax = (dp, row, col)
    redf = [Reduce((rows, split), ax, fbuf[i], rsem.at[i], True) for i in range(nc)]
    redt = [Reduce((rows, split), ax, tbuf[j], rsem.at[nc + j], False) for j in range(Hc)]

    plan = {("f", 2): [(0, "q")], "mid": [(1, "q"), (2, "p"), (0, "z")], (0, 1): [(1, "z")], (1, 0): [(2, "q")],
            (2, 0): [(0, "a")], (2, 1): [(2, "z"), (3, "z")], "last": [(4, "z"), (1, "a")],
            "end": [(5, "z"), (2, "a"), (3, "a")], "end2": [(4, "a")], "end3": [(5, "a")]}
    reds = redf + redt
    if (nc, Hc, C) != (3, 3, 2):
        plan = {"mid": [(nc - 1, "p")], "last": [(u, "q") for u in range(nc + Hc)] + [(u, "z") for u in range(nc + Hc)],
                "end": [(u, "a") for u in range(nc + Hc)]}

    def step(at):
        for u, what in plan.get(at, ()):
            getattr(reds[u], "start_" + what)()

    def ff(half, lo, w, first):
        w1, w2 = wup.at[half, :, lo:lo + w], wdn.at[half, :, lo:lo + w]
        bias = uball[half, :, lo:lo + w]

        halves = [(k, min(256, w - k)) for k in range(0, w, 256)]
        todo = [(slice(i, i + G), k, m) for i in range(0, NI, G) for k, m in halves]

        def dots(n):
            im, k, m = todo[n]
            return (mm(a2[im].reshape(GT, D), w1[:, k:k + m], 1, 0), mm(cb[im].reshape(GT, D), w2[:, k:k + m], 1, 0))

        def down(im):
            dd = mm(du[im, :, :w].reshape(GT, w), w1[...], 1, 1).reshape(G, SP, D)
            dacc[im] = dd if first else dacc[im] + dd

        if True:
            ahead = [dots(0)]
            for n, (im, k, m) in enumerate(todo):
                if n + 1 < len(todo):
                    ahead.append(dots(n + 1))
                u, dd = ahead[n]
                act, slope = gelu_parts(u + bias[:, k:k + m])
                gb[half, im, :, lo + k:lo + k + m] = act.astype(BF16).reshape(G, SP, m)
                du[im, :, k:k + m] = (dd * slope).astype(BF16).reshape(G, SP, m)
                if k == 0 and n:
                    down(todo[n - 1][0])
            down(todo[-1][0])
        gu = mm(a2t[...], du[:, :, :w].reshape(T, w), 1, 0)
        dubs[half, :, lo:lo + w] = gu[D:D + 1]
        return gu[:D], mm(ct[...], gb[half, :, :, lo:lo + w].reshape(T, w), 1, 0)

    for i, (lo, w) in enumerate(chunks):
        for a, v in enumerate(ff(c, lo, w, i == 0)):
            redf[i].put(C - 1, a, v)
        if i:
            redf[i - 1].start_p()
        step(("f", i))
        if i + 1 < nc:
            settle_p(1, Hc + i + 1)
            begin(gather_c(Hc + i + 1))
        settle_c(1, Hc + i)
        for k in col.ks():
            for a, v in enumerate(ff(col.up(k), lo, w, False)):
                redf[i].put(k - 1, a, v)
            redf[i].c(k).start()

    z = jnp.zeros((8, D), F32)
    def dout_of(i):
        dd = mm(a2[i], wotp[...], 1, 0).astype(BF16)
        for hh in range(H):
            dout[hh, i] = dd[:, hh * 2 * E:(hh + 1) * 2 * E]

    sums = [z, z, z, z]
    for i in range(NI):
        for lo, n in tiles:
            rs = slice(lo, lo + n)
            cf = cb[i, rs].astype(F32)
            da = dacc[i, rs]
            xh = xh2[i, rs]
            dh = cf + norm_back(da, vec[3:4, :], xh, rs2[i, rs])
            h[i, rs] = dh
            a2[i, rs] = dh.astype(BF16)
            sums = [t + fold(v) for t, v in zip(sums, (cf, da * xh, da, dh))]
        if i:
            dout_of(i - 1)
    dout_of(NI - 1)
    s_db, s_g2, s_b2, s_ob = (rsum(v) for v in sums)
    step("mid")
    ct[...] = a2[...].reshape(T, D).T
    dwo_all = mm(ct[...], o[...].reshape(T, D), 1, 0)
    for hh in range(H):
        dwo[hh] = jnp.concatenate([jnp.zeros((D, E), F32), dwo_all[:, hh * E:(hh + 1) * E]], axis=1)

    def back(hh):
        if True:
            def dprob(i):
                return mm(qkv[hh, i, :, 2 * E:] * (1.0 / math.sqrt(E)), dout[hh, i], 1, 1)

            def turned(i):
                return qkv[hh, i, :, :2 * E].T, dout[hh, i].T[:E]

            def grads(i, p, ds, kqt, dot):
                dq, dk, dv = mm(kqt[:E], ds, 1, 0), mm(kqt[E:], ds, 1, 1), mm(dot, p, 1, 1)
                qkv[hh, i, :, :2 * E] = jnp.concatenate([dq, dk], axis=0).astype(BF16).T
                qkv[hh, i, :, 2 * E:] = jnp.concatenate([dv, jnp.zeros((E, SP), F32)], axis=0).astype(BF16).T

            ahead, done = [], []
            for n in range(-DEEP[2], NI + 1):
                if 0 <= n + DEEP[2] < NI:
                    ahead.append((dprob(n + DEEP[2]), turned(n + DEEP[2])))
                if 0 <= n < NI:
                    dpr, ts = ahead[n]
                    p = pt[hh, n]
                    pf = p.astype(F32)
                    delta = rsum(pf * dpr)
                    done.append((n, p, (pf * (dpr - delta)).astype(BF16), *ts))
                if n >= 1:
                    grads(*done[n - 1])
        g = mm(a1t[...], qkv[hh].reshape(T, W4), 1, 0)
        dqvs[hh] = g[D:D + 1]
        return jnp.concatenate([g[:D, :2 * E], g[:D, 2 * E:] + dwo[hh]], axis=1)

    for j in range(Hc):
        def pair(s, carry):
            redt[j].put(s, 0, back(lax.rem(c + 1 + s, C) * Hc + j))

            @pl.when(s < C - 1)
            def _():
                redt[j].c(s + 1).start()
                step((j, 0))

            return carry

        lax.fori_loop(0, C, pair, 0)
        redt[j].start_p()
        step((j, 1))

    def da1(i):
        t = mm(qkv[0, i], wa[0], 1, 1)
        for hh in range(1, H):
            t = t + mm(qkv[hh, i], wa[hh], 1, 1)
        return t

    sums, ds = [z, z], [da1(0)]
    for i in range(NI):
        if i + 1 < NI:
            ds.append(da1(i + 1))
        for lo, n in tiles:
            rs = slice(lo, lo + n)
            da = ds[i][rs]
            xh = xh1[i, rs]
            dx = h[i, rs] + norm_back(da, vec[0:1, :], xh, rs1[i, rs])
            keep = min(n, SEQ - lo)
            dxb[i, lo:lo + keep] = dx[:keep]
            sums = [t + fold(v) for t, v in zip(sums, (da * xh, da))]
    s_g1, s_b1 = (rsum(v) for v in sums)
    dx_cp = pltpu.make_async_copy(dxb, dx_o, osem.at[1])
    dx_cp.start()

    six = jnp.concatenate([s_g1, s_b1, s_ob, s_g2, s_b2, s_db], axis=0)
    nf = FH // 128
    for cc in range(C):
        tail = [jnp.concatenate([dqvs[cc * Hc + j][:, :E], dqvs[cc * Hc + j][:, 2 * E:3 * E]], axis=1) for j in range(Hc)]
        tail += [dubs[cc][:, j * 128:(j + 1) * 128] for j in range(nf)]
        tail = jnp.concatenate(tail, axis=0)
        for rr in range(R):
            sgs[cc, rr, 0:6, 0:rows] = six[:, rr * rows:(rr + 1) * rows]
            sgs[cc, rr, 6:6 + Hc + nf, 0:128] = tail
    sgc[c] = sgs[c]
    gc = [remote(sgs.at[col.up(k)], sgc.at[c], vsem.at[0, 3], vsem.at[1, 3], "col", col.up(k)) for k in col.ks()]
    for cp in gc:
        cp.start()
    step("last")
    settle_g(1, 0)
    s = sgc[0]
    for k in range(1, C):
        s = s + sgc[k]
    sgz[...] = s
    sgr[r] = sgz[r]
    gz = [remote(sgz.at[row.up(k)], sgr.at[r], vsem.at[0, 5], vsem.at[1, 5], "row", row.up(k)) for k in row.ks()]
    for cp in gz:
        cp.start()
    step("end")
    for i in range(NI):
        t = yacc[i]
        for k in range(C):
            t = t + mm(gb[k, i], wdn[k], 1, 1)
        xin[i] = t[:SEQ].astype(BF16)
    y_cp = pltpu.make_async_copy(xin, y_o, osem.at[0])
    y_cp.start()
    settle_g(1, 2)
    s = sgr[0]
    for k in range(1, R):
        s = s + sgr[k]
    sgp[d] = s
    gp = [remote(sgp.at[d], sgp.at[d], vsem.at[0, 4], vsem.at[1, 4], "dp", dp.up(k)) for k in dp.ks()]
    for cp in gp:
        cp.start()

    outs = [y_cp, dx_cp]
    step("end2")
    for i in range(nc):
        redf[i].finish()
        outs.append(pltpu.make_async_copy(redf[i].fin, ff_o[i], osem.at[3 + i]))
        outs[-1].start()
    step("end3")
    settle_g(1, 1)
    s = sgp[0]
    for k in range(1, DP):
        s = s + sgp[k]
    sgf[...] = s
    outs.append(pltpu.make_async_copy(sgf, sg_o, osem.at[2]))
    outs[-1].start()
    for j in range(Hc):
        redt[j].finish()
        outs.append(pltpu.make_async_copy(redt[j].fin, ft_o.at[j], osem.at[3 + nc + j]))
        outs[-1].start()
    for red in redf + redt:
        red.drain()
    for u in range(U):
        settle_z(0, u)
        settle_p(0, u)
        settle_c(0, u)
    settle_v(0)
    for stage in range(3):
        settle_g(0, stage)
    for cp in outs:
        cp.wait()


def finish_kernel(cfg, *refs):
    rows, Hc, E, nf, (sr, sl), chunks = cfg
    nc = len(chunks)
    (y_i, dx_i, ft_i, sg_i), ff_i, refs = refs[:4], refs[4:4 + nc], refs[4 + nc:]
    (y_o, dx_o, dg1_o, db1_o, daw_o, dqvb_o, dob_o, dg2_o, db2_o, dup_o, dub_o, ddn_o, ddb_o) = refs[:13]
    (ybuf, xbuf, ft, sg, wf, wt, isem, osem), ff = refs[13:21], refs[21:]
    n = ybuf.shape[0]
    small = [pltpu.make_async_copy(i, v, isem.at[2 * n + k]) for k, (i, v) in enumerate(((sg_i, sg), (ft_i, ft), *zip(ff_i, ff)))]
    ins = [pltpu.make_async_copy(dx_i.at[k], xbuf.at[k], isem.at[k]) for k in range(n)]
    ins += [pltpu.make_async_copy(y_i.at[k], ybuf.at[k], isem.at[n + k]) for k in range(n)]
    outs = [pltpu.make_async_copy(xbuf.at[k], dx_o.at[k], osem.at[k]) for k in range(n)]
    outs += [pltpu.make_async_copy(ybuf.at[k], y_o.at[k], osem.at[n + k]) for k in range(n)]
    for cp in ins + small:
        cp.start()
    for i, o in zip(ins, outs):
        i.wait()
        o.start()
    small[0].wait()
    s = sg[...]
    for i, ref in enumerate([dg1_o, db1_o, dob_o, dg2_o, db2_o, ddb_o]):
        ref[...] = s[i:i + 1, :rows].reshape(rows)
    for j in range(nf):
        dub_o[pl.ds(j * 128, 128)] = s[6 + Hc + j:7 + Hc + j, :128].reshape(128)
    for j in range(Hc):
        dqvb_o[0:1, j * E:(j + 1) * E] = s[6 + j:7 + j, :E]
        dqvb_o[1:2, j * E:(j + 1) * E] = s[6 + j:7 + j, E:2 * E]

    def lay(src, a, ref, lo):
        pr, pw = src.shape[-2:]
        for qr in range(sr):
            for ql in range(sl):
                ref[pl.ds(qr * pr, pr), pl.ds(lo + ql * pw, pw)] = src[qr * sl + ql, a].astype(F32)

    small[1].wait()
    for j in range(Hc):
        lay(ft.at[j], 0, wt.at[j], 0)
    for i, (lo, w) in enumerate(chunks):
        small[2 + i].wait()
        for a in range(2):
            lay(ff[i], a, wf.at[a], lo)
    big = [pltpu.make_async_copy(b, o, osem.at[2 * n + k]) for k, (b, o) in enumerate(((wf.at[0], dup_o), (wf.at[1], ddn_o), (wt, daw_o)))]
    for o in big:
        o.start()
    outs += big
    for o in outs:
        o.wait()


def pick_split(n, rows, widths):
    for sr in range(1, n + 1):
        if n % sr == 0 and rows % (16 * sr) == 0 and all(w % (128 * (n // sr)) == 0 for w in widths):
            return sr, n // sr
    return 1, 1


def local(sizes, x, g1, b1, aw, qvb, ob, g2, b2, up, ub, dn, db, c):
    DP, R, C = sizes
    NI, SEQ, D = x.shape
    Hc, rows, W4 = aw.shape
    E, FH = W4 // 4, up.shape[1]
    H, SP = C * Hc, -(-SEQ // 16) * 16
    T = NI * SP
    chunks = tuple((lo, 256) for lo in range(0, FH, 256)) if FH % 256 == 0 else ((0, FH),)
    nc, wmax = len(chunks), max(w for _, w in chunks)
    split = pick_split(DP, rows, (W4,) + tuple(w for _, w in chunks))
    np_ = split[0] * split[1]
    pr, pw = rows // split[0], W4 // split[1]
    sd, vm = jax.ShapeDtypeStruct, pltpu.VMEM
    dma = pltpu.SemaphoreType.DMA
    nf, VW = FH // 128, -(-rows // 128) * 128
    S = -(-(6 + Hc + nf) // 8) * 8
    cfg = (DP, R, C, NI, SEQ, SP, D, Hc, E, FH, rows, split, chunks)

    def red(A, L):
        pw = L // split[1]
        return [vm((C, np_, A, R, pr, pw), BF16), vm((max(C - 1, 1), np_, A, R, pr, pw), BF16), vm((DP, A, R, pr, pw), BF16),
                vm((R, A, pr, pw), BF16), vm((R, A, pr, pw), BF16), vm((np_, A, pr, pw), BF16)]

    scratch = sum([red(2, w) for _, w in chunks] + [red(1, W4)] * Hc, []) + [
        vm((H, D, W4), BF16), vm((C, D, FH), BF16), vm((C, D, FH), BF16), vm((R, 8, VW), F32),
        vm((C, 2, Hc * E), F32), vm((C, 1, FH), F32), vm((8, D), F32), vm((H, 1, W4), F32),
        vm((NI, SEQ, D), BF16), vm((NI, SEQ, D), BF16), vm((NI, SP, D), BF16), vm((NI, SP, D), F32), vm((NI, SP, 1), F32),
        vm((NI, SP, D), BF16), vm((H, NI, SP, W4), BF16), vm((H, NI, SP, SP), BF16), vm((NI, SP, D), BF16),
        vm((NI, SP, D), F32), vm((NI, SP, D), F32), vm((NI, SP, 1), F32), vm((NI, SP, D), BF16), vm((D, D), BF16),
        vm((D, 2 * D), BF16),
        vm((C, NI, SP, FH), BF16), vm((NI, SP, wmax), BF16), vm((NI, SP, D), F32), vm((NI, SP, D), F32),
        vm((H, NI, SP, 2 * E), BF16), vm((D + 16, T), BF16), vm((D, T), BF16), vm((D + 16, T), BF16),
        vm((H, D, 2 * E), F32), vm((NI, SEQ, D), F32), vm((C, 1, FH), F32), vm((H, 1, W4), F32),
        vm((C, R, S, VW), F32), vm((C, R, S, VW), F32), vm((DP, S, VW), F32), vm((R, S, VW), F32),
        vm((R, S, VW), F32), vm((S, VW), F32),
        dma((5,)), dma((3 + nc + Hc,)), dma((2, 2, Hc + nc)), dma((2, Hc + 2 * nc, max(C - 1, 1))), dma((nc + Hc, 2, 5)), dma((2, 6)),
    ]
    any_ = pl.BlockSpec(memory_space=pl.ANY)
    vm_ = pl.BlockSpec(memory_space=pltpu.VMEM)
    v = lambda a: sd(a.shape, F32)
    y, dx, ft, sg, *ff = pl.pallas_call(
        functools.partial(kernel, cfg),
        out_shape=(sd(x.shape, BF16), v(x), sd((Hc, np_, 1, pr, pw), BF16), sd((S, VW), F32),
                   *[sd((np_, 2, pr, w // split[1]), BF16) for _, w in chunks]),
        in_specs=[any_, vm_, vm_, any_, vm_, vm_, vm_, vm_, any_, vm_, any_, vm_, any_],
        out_specs=[any_] * (4 + nc),
        scratch_shapes=scratch,
        compiler_params=pltpu.CompilerParams(vmem_limit_bytes=67043328, collective_id=0, has_side_effects=True),
    )(x, g1, b1, aw, qvb, ob, g2, b2, up, ub, dn, db, c)
    return tuple(pl.pallas_call(
        functools.partial(finish_kernel, (rows, Hc, E, nf, split, chunks)),
        out_shape=(sd(x.shape, BF16), v(x), v(g1), v(b1), v(aw), v(qvb), v(ob), v(g2), v(b2), v(up), v(ub), v(dn), v(db)),
        in_specs=[any_] * (4 + nc),
        out_specs=[any_, any_, vm_, vm_, any_, vm_, vm_, vm_, vm_, any_, vm_, any_, vm_],
        scratch_shapes=[vm(x.shape, BF16), vm(x.shape, F32), vm(ft.shape, BF16), vm(sg.shape, F32),
                        vm((2, rows, FH), F32), vm(aw.shape, F32), dma((2 * NI + 2 + nc,)), dma((2 * NI + 3,)),
                        *[vm(f.shape, BF16) for f in ff]],
        compiler_params=pltpu.CompilerParams(vmem_limit_bytes=67043328),
    )(y, dx, ft, sg, *ff))


def solution(mesh):
    sizes = tuple(mesh.shape[a] for a in ("dp", "row", "col"))
    placed = (
        P(("dp", "row", "col"), None, None),
        P("row"),
        P("row"),
        P("col", "row", None),
        P(None, "col"),
        P("row"),
        P("row"),
        P("row"),
        P("row", "col"),
        P("col"),
        P("row", "col"),
        P("row"),
        P(("dp", "row", "col"), None, None),
    )
    return jax.shard_map(
        functools.partial(local, sizes),
        mesh=mesh,
        in_specs=placed,
        out_specs=(
            P(("dp", "row", "col"), None, None),
            P(("dp", "row", "col"), None, None),
            P("row"),
            P("row"),
            P("col", "row", None),
            P(None, "col"),
            P("row"),
            P("row"),
            P("row"),
            P("row", "col"),
            P("col"),
            P("row", "col"),
            P("row"),
        ),
        check_vma=False,
    )
```
